128 devices in a mesh: bl: 8 (over x, y_lo), freq: 16 (over z, y_hi, core).
Axes of the slice: x: 4, y: 4 (y_hi: 2, y_lo: 2; y = y_hi * 2 + y_lo), z: 4, core: 2. Of those that a mesh axis runs over, the one named last changes fastest.
Arguments:
- visibilities: float32 [2, 2, 256, 16384], P(None, None, 'freq', 'bl'), may hold values from -8 to 8
- sample_flag_weight: int32 [2, 256, 16384], P(None, 'freq', 'bl'), may hold values from 0 to 4
- baseline_station_pair: int32 [2, 16384], P(None, 'bl'), may hold values from 0 to 511, as said below
- baseline_spatial_coords: float32 [2, 2, 16384], P(None, None, 'bl'), may hold values from -6 to 6
- directions: float32 [2, 8], replicated, may hold values from -0.5 to 0.5
- source_flux: float32 [8, 256], P(None, 'freq'), may hold values from 0.5 to 2
- channel_ratio: float32 [256], P('freq'), may hold values from 0.7 to 1.4
- jones_gains: float32 [2, 8, 256, 512], P(None, None, 'freq'), may hold values from -4 to 4
- scaled_dual: float32 [2, 8, 256, 512], P(None, None, 'freq'), may hold values from -2 to 2
- consensus: float32 [2, 3, 8, 512], replicated, may hold values from -3 to 3
- penalty: float32 [8], replicated, may hold values from 0.3 to 3
Outputs:
- new_gains: float32 [2, 8, 256, 512], P(None, None, 'freq')
- new_consensus: float32 [2, 3, 8, 512], replicated
- new_dual: float32 [2, 8, 256, 512], P(None, None, 'freq')
- residuals: float32 [2, 2, 256, 16384], P(None, None, 'freq', 'bl')
The draws below stay inside these ranges and needn't reach their ends.
Inputs may be any that keep to these rules, and one draw needn't show every extreme that they name: `baseline_station_pair`: the two stations of every baseline differ.
All inputs are finite; a program needn't handle non-finite values.
Results may differ from the reference program's by a relative error of at most 0.00016.
Values sent between devices are 32-bit elements; how exact they have to be, the bound alone decides.
No kernel may reach another device: no remote copies, remote signals or barrier semaphores. Data moves between devices by JAX's collectives and lax.ppermute only.
A program may use at most 64 MiB of HBM per device.

```python
import math
import jax
import jax.numpy as jnp
from jax import lax

STATION_TOTAL = 512
DIRS = 8
NPOLY = 3
ITERS = 3
TIME_SLOT_TOTAL = 2
BASELINE_TOTAL = 16384
CHANNEL_TOTAL = 256


def draw_baseline_station_pair(key, part):
    leading_dims = jax.random.randint(jax.random.fold_in(key, 11), (BASELINE_TOTAL,), 0, STATION_TOTAL)
    update_step_length = jax.random.randint(jax.random.fold_in(key, 12), (BASELINE_TOTAL,), 1, STATION_TOTAL)
    return jnp.stack([leading_dims, (leading_dims + update_step_length) % STATION_TOTAL]).astype(jnp.int32)


def set_ends(result, own_key, low, high):
    spot = [jax.random.randint(jax.random.fold_in(own_key, axis), (), 0, length) for axis, length in enumerate(result.shape)]
    widest = result.shape.index(max(result.shape))
    neighbour = spot[:widest] + [(spot[widest] + 1) % result.shape[widest]] + spot[widest + 1:]
    return result.at[tuple(spot)].set(low).at[tuple(neighbour)].set(high)


def level_of(key, dims, cuts, low, top_value):
    gain = 1.0
    for dim, shards_of in cuts:
        draws = jax.random.uniform(jax.random.fold_in(jax.random.fold_in(key, 6), dim), (shards_of,), jnp.float32, low / len(cuts), top_value / len(cuts))
        gain = gain * jnp.repeat(jnp.exp(draws), dims[dim] // shards_of).reshape((-1,) + (1,) * (len(dims) - 1 - dim))
    return gain


def gaussian(own_key, dims, spread, reach, cuts=(), held_as=jnp.bfloat16):
    values = jax.random.normal(own_key, dims, jnp.float32) * spread
    if len(cuts) > 0:
        values = level_of(own_key, dims, cuts, -0.22, 0.18) * values
    return jnp.clip(values, min=-reach, max=reach).astype(held_as)


def setup_inputs(seed: int = 0) -> dict:
    arg_keys = jax.random.split(jax.random.key(seed), 12)
    return {
        "visibilities": gaussian(arg_keys[0], (2, TIME_SLOT_TOTAL, CHANNEL_TOTAL, BASELINE_TOTAL), 1.0, 8.0, ((2, 16), (3, 8)), jnp.float32),
        "sample_flag_weight": set_ends(jax.random.randint(arg_keys[1], (TIME_SLOT_TOTAL, CHANNEL_TOTAL, BASELINE_TOTAL), 0, 5), jax.random.fold_in(arg_keys[1], 1), 0, 4).astype(jnp.int32),
        "baseline_station_pair": draw_baseline_station_pair(jax.random.fold_in(arg_keys[11], 71), 0),
        "baseline_spatial_coords": gaussian(arg_keys[3], (2, TIME_SLOT_TOTAL, BASELINE_TOTAL), 1.0, 6.0, ((2, 8),), jnp.float32),
        "directions": jnp.clip(jax.random.uniform(arg_keys[4], (2, DIRS), jnp.float32, -0.5, 0.5), -0.5, 0.5),
        "source_flux": jnp.clip(jnp.exp(math.log(2.0) - 1.3862944 * jax.random.uniform(arg_keys[5], (DIRS, CHANNEL_TOTAL), jnp.float32) ** level_of(arg_keys[5], (DIRS, CHANNEL_TOTAL), ((1, 16),), -0.2, 0.2)), 0.5, 2.0),
        "channel_ratio": jnp.clip(jnp.exp(math.log(1.4) - 0.6931472 * jax.random.uniform(arg_keys[6], (CHANNEL_TOTAL,), jnp.float32) ** level_of(arg_keys[6], (CHANNEL_TOTAL,), ((0, 16),), -0.2, 0.2)), 0.7, 1.4),
        "jones_gains": gaussian(arg_keys[7], (2, DIRS, CHANNEL_TOTAL, STATION_TOTAL), 0.8, 4.0, ((2, 16),), jnp.float32),
        "scaled_dual": gaussian(arg_keys[8], (2, DIRS, CHANNEL_TOTAL, STATION_TOTAL), 0.3, 2.0, ((2, 16),), jnp.float32),
        "consensus": gaussian(arg_keys[9], (2, NPOLY, DIRS, STATION_TOTAL), 0.5, 3.0, (), jnp.float32),
        "penalty": jnp.clip(jnp.exp(jax.random.uniform(arg_keys[10], (DIRS,), jnp.float32, math.log(0.3), math.log(3.0))), 0.3, 3.0),
    }


robust_dof = 2.0
small_term = 1e-06
two_pi = 2.0 * math.pi

def legendre(ratios):
    scaled = (ratios - 1.05) / 0.35
    values = [jnp.ones_like(scaled), scaled]
    for degree in range(1, NPOLY - 1):
        values.append(((2 * degree + 1) * scaled * values[degree] - degree * values[degree - 1]) / (degree + 1))
    return jnp.stack(values[:NPOLY])

def coherency(coords, sky_dirs, fluxes, ratios):
    project = sky_dirs[0][:, None, None] * coords[0][None] + sky_dirs[1][:, None, None] * coords[1][None]
    phases = two_pi * project[:, :, None, :] * ratios[None, None, :, None]
    amplitude = fluxes[:, None, :, None]
    return (amplitude * jnp.cos(phases), amplitude * jnp.sin(phases))

def predict(gain_re, gain_im, pair_index, sky_re, sky_im):
    left_re = jnp.take(gain_re, pair_index[0], axis=2)
    left_im = jnp.take(gain_im, pair_index[0], axis=2)
    right_re = jnp.take(gain_re, pair_index[1], axis=2)
    right_im = jnp.take(gain_im, pair_index[1], axis=2)
    pair_re = left_re * right_re + left_im * right_im
    pair_im = left_im * right_re - left_re * right_im
    model_re = pair_re[:, None] * sky_re - pair_im[:, None] * sky_im
    model_im = pair_re[:, None] * sky_im + pair_im[:, None] * sky_re
    return ((left_re, left_im, right_re, right_im), model_re, model_im)

def residual_of(observed, model_re, model_im):
    return (observed[0] - jnp.sum(model_re, axis=0), observed[1] - jnp.sum(model_im, axis=0))

def robust_weights(flagged, error_re, error_im, sigma_sq):
    return flagged * (robust_dof + 1.0) / (robust_dof + (error_re * error_re + error_im * error_im) / sigma_sq)

def normal_terms(error_re, error_im, model_re, model_im, weights, sky_re, sky_im, side_gains, pair_index, station_list):
    target_re = error_re[None] + model_re
    target_im = error_im[None] + model_im
    cross_re = sky_re * target_re + sky_im * target_im
    cross_im = sky_re * target_im - sky_im * target_re
    weight_wide = weights[None]
    summed_re = jnp.sum(weight_wide * cross_re, axis=1)
    summed_im = jnp.sum(weight_wide * cross_im, axis=1)
    powers = jnp.sum(weight_wide * (sky_re * sky_re + sky_im * sky_im), axis=1)
    left_re, left_im, right_re, right_im = side_gains
    first_re = right_re * summed_re - right_im * summed_im
    first_im = right_re * summed_im + right_im * summed_re
    second_re = left_re * summed_re + left_im * summed_im
    second_im = left_im * summed_re - left_re * summed_im
    first_norm = (right_re * right_re + right_im * right_im) * powers
    second_norm = (left_re * left_re + left_im * left_im) * powers
    stacked_first = jnp.stack([first_re, first_im, first_norm])
    stacked_second = jnp.stack([second_re, second_im, second_norm])
    zeroed = jnp.zeros(stacked_first.shape[:3] + (station_list,), stacked_first.dtype)
    return zeroed.at[:, :, :, pair_index[0]].add(stacked_first).at[:, :, :, pair_index[1]].add(stacked_second)

def update_gains(gain_re, gain_im, normal_sums, anchor_re, anchor_im, effective_penalty):
    penalty_wide = effective_penalty[:, None, None]
    divisor = normal_sums[2] + penalty_wide
    solved_re = (normal_sums[0] + penalty_wide * anchor_re) / divisor
    solved_im = (normal_sums[1] + penalty_wide * anchor_im) / divisor
    return (0.5 * (gain_re + solved_re), 0.5 * (gain_im + solved_im))

def cholesky_solve(gram_total, flat_rhs):
    factor = jnp.linalg.cholesky(gram_total)
    matrix_order = gram_total.shape[0]
    forward = []
    for row_index in range(matrix_order):
        running = flat_rhs[row_index]
        for col_index in range(row_index):
            running = running - factor[row_index, col_index] * forward[col_index]
        forward.append(running / factor[row_index, row_index])
    backward = [None] * matrix_order
    for row_index in reversed(range(matrix_order)):
        running = forward[row_index]
        for col_index in range(row_index + 1, matrix_order):
            running = running - factor[col_index, row_index] * backward[col_index]
        backward[row_index] = running / factor[row_index, row_index]
    return jnp.stack(backward)

def solve_consensus(gram_total, rhs_total):
    matrix_order = gram_total.shape[0]
    flat_rhs = jnp.moveaxis(rhs_total, 1, 0).reshape(matrix_order, -1)
    solved = cholesky_solve(gram_total, flat_rhs)
    return jnp.moveaxis(solved.reshape((matrix_order, rhs_total.shape[0]) + rhs_total.shape[2:]), 0, 1)

def reference(visibilities, sample_flag_weight, baseline_station_pair, baseline_spatial_coords, directions, source_flux, channel_ratio, jones_gains, scaled_dual, consensus, penalty):
    chan_block = math.gcd(CHANNEL_TOTAL, 8)
    blocks = CHANNEL_TOTAL // chan_block

    def split_axis(tensor, position):
        old_shape = tensor.shape
        reshaped = tensor.reshape(old_shape[:position] + (blocks, chan_block) + old_shape[position + 1:])
        return jnp.moveaxis(reshaped, position, 0)

    def join_axis(tensor, position):
        moved_axes = jnp.moveaxis(tensor, 0, position)
        old_shape = moved_axes.shape
        return moved_axes.reshape(old_shape[:position] + (blocks * chan_block,) + old_shape[position + 2:])
    effective_penalty = penalty * (2.0 * BASELINE_TOTAL * TIME_SLOT_TOTAL / STATION_TOTAL)
    poly_basis = legendre(channel_ratio)
    anchor = jnp.einsum('jc,xjks->xkcs', poly_basis, consensus, precision=lax.Precision.HIGHEST) - scaled_dual
    flagged = sample_flag_weight.astype(jnp.float32)
    weight_count = jnp.sum(flagged)
    vis_blocks = split_axis(visibilities, 2)
    flag_blocks = split_axis(flagged, 1)
    flux_blocks = split_axis(source_flux, 1)
    ratio_blocks = channel_ratio.reshape(blocks, chan_block)
    anchor_blocks = split_axis(anchor, 2)

    def block_model(gain_block, flux_block, ratio_block):
        sky_re, sky_im = coherency(baseline_spatial_coords, directions, flux_block, ratio_block)
        side_gains, model_re, model_im = predict(gain_block[0], gain_block[1], baseline_station_pair, sky_re, sky_im)
        return (sky_re, sky_im, side_gains, model_re, model_im)
    gain_state = jones_gains
    for iteration in range(ITERS):
        gain_blocks = split_axis(gain_state, 2)

        def misfit_block(block_items):
            vis_block, flag_block, flux_block, ratio_block, gain_block = block_items
            sky_re, sky_im, side_gains, model_re, model_im = block_model(gain_block, flux_block, ratio_block)
            error_re, error_im = residual_of(vis_block, model_re, model_im)
            return jnp.sum(flag_block * (error_re * error_re + error_im * error_im))
        squares = jnp.sum(lax.map(misfit_block, (vis_blocks, flag_blocks, flux_blocks, ratio_blocks, gain_blocks)))
        sigma_sq = squares / (weight_count + 1.0) + small_term

        def update_block(block_items):
            vis_block, flag_block, flux_block, ratio_block, gain_block, anchor_block = block_items
            sky_re, sky_im, side_gains, model_re, model_im = block_model(gain_block, flux_block, ratio_block)
            error_re, error_im = residual_of(vis_block, model_re, model_im)
            weights = robust_weights(flag_block, error_re, error_im, sigma_sq)
            normal_sums = normal_terms(error_re, error_im, model_re, model_im, weights, sky_re, sky_im, side_gains, baseline_station_pair, STATION_TOTAL)
            new_re, new_im = update_gains(gain_block[0], gain_block[1], normal_sums, anchor_block[0], anchor_block[1], effective_penalty)
            return jnp.stack([new_re, new_im])
        gain_state = join_axis(lax.map(update_block, (vis_blocks, flag_blocks, flux_blocks, ratio_blocks, gain_blocks, anchor_blocks)), 2)
    final_blocks = split_axis(gain_state, 2)

    def residual_block(block_items):
        vis_block, flux_block, ratio_block, gain_block = block_items
        sky_re, sky_im, side_gains, model_re, model_im = block_model(gain_block, flux_block, ratio_block)
        error_re, error_im = residual_of(vis_block, model_re, model_im)
        return jnp.stack([error_re, error_im])
    residuals = join_axis(lax.map(residual_block, (vis_blocks, flux_blocks, ratio_blocks, final_blocks)), 2)
    gram_total = jnp.dot(poly_basis, poly_basis.T, precision=lax.Precision.HIGHEST)
    rhs_total = jnp.einsum('jc,xkcs->xjks', poly_basis, gain_state + scaled_dual, precision=lax.Precision.HIGHEST)
    new_consensus = solve_consensus(gram_total, rhs_total)
    new_dual = scaled_dual + gain_state - jnp.einsum('jc,xjks->xkcs', poly_basis, new_consensus, precision=lax.Precision.HIGHEST)
    return (gain_state, new_consensus, new_dual, residuals)
```

```python
import functools

import jax
import jax.numpy as jnp
from jax import lax
from jax.experimental import pallas as pl
from jax.experimental.pallas import tpu as pltpu
from jax.sharding import Mesh
from jax.sharding import PartitionSpec as P

NPOLY = 3
ITERS = 3
BL = ("bl_0", "bl_1")
FREQ = ("freq_0", "freq_1", "freq_2")
ALL = BL + FREQ

STATIONS = 512
DIRS = 8
TIMES = 2
BASELINES = 16384
PARTS = 8
FEW = 2
LOCAL = BASELINES // PARTS
SUB = 256

robust_dof = 2.0
small_term = 1e-06

SIN_TERMS = (
    3.1415926401307086,
    -5.167710083507905,
    2.5500775232148403,
    -0.5982912856219295,
    0.07765766030867731,
)
COS_TERMS = (
    0.9999999997799046,
    -4.934802137078821,
    4.058709159556128,
    -1.3352120030477381,
    0.23493731380150681,
    -0.024396324323359975,
)

F32 = jnp.float32
BF16 = jnp.bfloat16


def horner(terms, w):
    value = jnp.full_like(w, terms[-1])
    for term in terms[-2::-1]:
        value = value * w + term
    return value


def turn_parts(turns):
    f = turns - jnp.floor(turns + 0.5)
    w = f * f
    half_sin = f * horner(SIN_TERMS, w)
    half_cos = horner(COS_TERMS, w)
    twice = half_sin + half_sin
    return 1.0 - twice * half_sin, twice * half_cos


def two_parts(value):
    high = value.astype(BF16)
    low = (value - high.astype(F32)).astype(BF16)
    return high, low


def wide_kernel(
    gains_ref,
    vis_ref,
    flag_ref,
    pair_ref,
    coord_ref,
    dirs_ref,
    flux_ref,
    ratio_ref,
    *rest,
    residual_out,
    channels,
    block,
):
    outs, (high_ref, low_ref, left_ref, right_ref) = rest[:-4], rest[-4:]
    step = pl.program_id(0)

    @pl.when(step == 0)
    def _():
        high, low = two_parts(gains_ref[...])
        high_ref[...] = high
        low_ref[...] = low

    stations = lax.broadcasted_iota(jnp.int32, (STATIONS, block), 0)
    for row, target in ((0, left_ref), (1, right_ref)):
        hot = (stations == pair_ref[row : row + 1, :]).astype(F32).astype(BF16)
        target[...] = jnp.dot(high_ref[...], hot, preferred_element_type=F32) + jnp.dot(
            low_ref[...], hot, preferred_element_type=F32
        )
    ratio = ratio_ref[:, :1]
    total = [[None, None] for _ in range(TIMES)]
    for k in range(DIRS):
        re = pl.ds(k * channels, channels)
        im = pl.ds((DIRS + k) * channels, channels)
        left_re, left_im = left_ref[re, :], left_ref[im, :]
        right_re, right_im = right_ref[re, :], right_ref[im, :]
        flux = flux_ref[re, :1]
        pair_re = (left_re * right_re + left_im * right_im) * flux
        pair_im = (left_im * right_re - left_re * right_im) * flux
        for t in range(TIMES):
            project = (
                dirs_ref[0, k] * coord_ref[t : t + 1, :]
                + dirs_ref[1, k] * coord_ref[TIMES + t : TIMES + t + 1, :]
            )
            sky_re, sky_im = turn_parts(project * ratio)
            model_re = pair_re * sky_re - pair_im * sky_im
            model_im = pair_re * sky_im + pair_im * sky_re
            if k == 0:
                total[t] = [model_re, model_im]
            else:
                total[t] = [total[t][0] + model_re, total[t][1] + model_im]
    if residual_out:
        (residual_ref,) = outs
        for t in range(TIMES):
            residual_ref[0, t] = vis_ref[0, t] - total[t][0]
            residual_ref[1, t] = vis_ref[1, t] - total[t][1]
    else:
        (sums_ref,) = outs
        misfit = jnp.zeros((8, 128), F32)
        count = jnp.zeros((8, 128), F32)
        for t in range(TIMES):
            error_re = vis_ref[0, t] - total[t][0]
            error_im = vis_ref[1, t] - total[t][1]
            flagged = flag_ref[t].astype(F32)
            part = flagged * (error_re * error_re + error_im * error_im)
            for r in range(0, channels, 8):
                for c in range(0, block, 128):
                    misfit += part[r : r + 8, c : c + 128]
                    count += flagged[r : r + 8, c : c + 128]
        sums = jnp.concatenate(
            [jnp.sum(misfit, axis=0, keepdims=True), jnp.sum(count, axis=0, keepdims=True)], axis=1
        )

        @pl.when(step == 0)
        def _():
            sums_ref[...] = sums

        @pl.when(step > 0)
        def _():
            sums_ref[...] += sums


def wide_model(gains, vis, flags, pairs, coords, directions, flux, ratio, residual_out):
    channels = vis.shape[2]
    count = vis.shape[3]
    block = SUB
    rows = 2 * DIRS * channels
    whole = lambda shape: pl.BlockSpec(shape, lambda i: (0,) * len(shape))
    vis_spec = pl.BlockSpec((2, TIMES, channels, block), lambda i: (0, 0, 0, i))
    if residual_out:
        out_shape = jax.ShapeDtypeStruct(vis.shape, F32)
        out_spec = vis_spec
    else:
        out_shape = jax.ShapeDtypeStruct((1, 256), F32)
        out_spec = whole((1, 256))
    return pl.pallas_call(
        functools.partial(
            wide_kernel, residual_out=residual_out, channels=channels, block=block
        ),
        grid=(count // block,),
        in_specs=[
            whole((rows, STATIONS)),
            vis_spec,
            pl.BlockSpec((TIMES, channels, block), lambda i: (0, 0, i)),
            pl.BlockSpec((2, block), lambda i: (0, i)),
            pl.BlockSpec((2 * TIMES, block), lambda i: (0, i)),
            pl.BlockSpec(memory_space=pltpu.SMEM),
            whole((DIRS * channels, 1)),
            whole((channels, 1)),
        ],
        out_specs=out_spec,
        out_shape=out_shape,
        scratch_shapes=[
            pltpu.VMEM((rows, STATIONS), BF16),
            pltpu.VMEM((rows, STATIONS), BF16),
            pltpu.VMEM((rows, block), F32),
            pltpu.VMEM((rows, block), F32),
        ],
        name="wide_residual" if residual_out else "wide_misfit",
    )(gains, vis, flags, pairs, coords, directions, flux.reshape(-1, 1), ratio.reshape(-1, 1))


def swap_sum(rows):
    place = lax.broadcasted_iota(jnp.int32, rows[0].shape, 0)
    for bit in (4, 2, 1):
        mine = (place & bit) == 0
        merged = []
        for i in range(len(rows) // 2):
            a, b = rows[i], rows[i + len(rows) // 2]
            low = a + pltpu.roll(a, 8 - bit, axis=0)
            high = b + pltpu.roll(b, bit, axis=0)
            merged.append(jnp.where(mine, low, high))
        rows = merged
    return rows[0]


def model_block(data_ref, table_ref, sky_in, geo, outs, at, misfit):
    left_out, right_out, error_out, sky_out = outs
    lanes = pl.ds(at, SUB)
    place = lax.broadcasted_iota(jnp.int32, (128, SUB), 0)
    picked = []
    for row in (16, 17):
        station = data_ref[0, row : row + 1, lanes].astype(jnp.int32)
        hot = (place == (station & 127)).astype(F32).astype(BF16)
        got = jnp.dot(
            table_ref[...], jnp.concatenate([hot, hot], axis=0), preferred_element_type=F32
        )
        quarter = jnp.broadcast_to(station >> 7, (32, SUB))
        picked.append(
            jnp.where(
                quarter < 2,
                jnp.where(quarter == 0, got[0:32], got[32:64]),
                jnp.where(quarter == 2, got[64:96], got[96:128]),
            )
        )
    left, right = picked
    left_out[0, :, lanes] = left
    right_out[0, :, lanes] = right
    pieces = [None] * 8
    for f in range(FEW):
        lr, li = left[16 * f : 16 * f + 8], left[16 * f + 8 : 16 * f + 16]
        rr, ri = right[16 * f : 16 * f + 8], right[16 * f + 8 : 16 * f + 16]
        pair_re = lr * rr + li * ri
        pair_im = li * rr - lr * ri
        for t in range(TIMES):
            if sky_in is None:
                dirs, flux, ratio = geo
                project = dirs[0] * data_ref[0, 12 + t : 13 + t, lanes] + dirs[1] * data_ref[
                    0, 14 + t : 15 + t, lanes
                ]
                sky_re, sky_im = turn_parts(project * ratio[f])
                sky_re = sky_re * flux[f]
                sky_im = sky_im * flux[f]
                sky_out[0, t, f, 0, :, lanes] = sky_re
                sky_out[0, t, f, 1, :, lanes] = sky_im
            else:
                sky_re = sky_in[0, t, f, 0, :, lanes]
                sky_im = sky_in[0, t, f, 1, :, lanes]
            pieces[2 * t + f] = pair_re * sky_re - pair_im * sky_im
            pieces[4 + 2 * t + f] = pair_re * sky_im + pair_im * sky_re
    error = data_ref[0, 0:8, lanes] - swap_sum(pieces)
    error_out[0, :, lanes] = error
    flagged = data_ref[0, 8:12, lanes]
    part = jnp.concatenate([flagged, flagged], axis=0) * (error * error)
    return misfit + part


def build_table(table_ref, gains):
    high, low = two_parts(gains)
    for q in range(4):
        table_ref[32 * q : 32 * q + 32, 0:128] = high[:, 128 * q : 128 * q + 128]
        table_ref[32 * q : 32 * q + 32, 128:256] = low[:, 128 * q : 128 * q + 128]


def first_kernel(
    data_ref, gains_ref, geo_ref, left_out, right_out, error_out, sky_out, table_ref
):
    @pl.when(pl.program_id(0) == 0)
    def _():
        build_table(table_ref, gains_ref[...])

    col = lambda i: geo_ref[:, i : i + 1]
    geo = ((col(0), col(1)), (col(2), col(3)), (col(4), col(5)))

    def run(i, carry):
        at = pl.multiple_of(i * SUB, SUB)
        model_block(
            data_ref, table_ref, None, geo, (left_out, right_out, error_out, sky_out), at,
            jnp.zeros((8, SUB), F32),
        )
        return carry

    lax.fori_loop(0, LOCAL // SUB, run, 0)


def normal_block(data_ref, left_ref, right_ref, error_ref, sky_ref, total_ref, at, inverse):
    lanes = pl.ds(at, SUB)
    error = error_ref[0, :, lanes]
    square = error * error
    square = square + pltpu.roll(square, 4, axis=0)
    flagged = data_ref[0, 8:12, lanes]
    flagged = jnp.concatenate([flagged, flagged], axis=0)
    weight = flagged * (robust_dof + 1.0) / (robust_dof + square * inverse)
    scaled = weight * error
    left = left_ref[0, :, lanes]
    right = right_ref[0, :, lanes]
    first, second = [], []
    wide = lambda row: jnp.broadcast_to(row, (DIRS, SUB))
    for f in range(FEW):
        z_re, z_im = None, None
        for t in range(TIMES):
            i = 2 * t + f
            y_re, y_im = wide(scaled[i : i + 1]), wide(scaled[4 + i : 5 + i])
            sky_re = sky_ref[0, t, f, 0, :, lanes]
            sky_im = sky_ref[0, t, f, 1, :, lanes]
            a = sky_re * y_re + sky_im * y_im
            b = sky_re * y_im - sky_im * y_re
            z_re, z_im = (a, b) if t == 0 else (z_re + a, z_im + b)
        power = wide(weight[f : f + 1] + weight[2 + f : 3 + f])
        lr, li = left[16 * f : 16 * f + 8], left[16 * f + 8 : 16 * f + 16]
        rr, ri = right[16 * f : 16 * f + 8], right[16 * f + 8 : 16 * f + 16]
        first += [rr * z_re - ri * z_im, rr * z_im + ri * z_re, (rr * rr + ri * ri) * power]
        second += [lr * z_re + li * z_im, li * z_re - lr * z_im, (lr * lr + li * li) * power]
    place = lax.broadcasted_iota(jnp.int32, (256, SUB), 0)
    total = None
    for row, pieces in ((16, first), (17, second)):
        station = data_ref[0, row : row + 1, lanes].astype(jnp.int32)
        hot = (place == (station & 255)).astype(F32).astype(BF16)
        values = jnp.concatenate(pieces, axis=0)
        upper = jnp.broadcast_to(station, (48, SUB)) >= 256
        parts = []
        for half in (jnp.where(upper, 0.0, values), jnp.where(upper, values, 0.0)):
            parts += list(two_parts(half))
        got = lax.dot_general(
            jnp.concatenate(parts, axis=0),
            hot,
            (((1,), (1,)), ((), ())),
            preferred_element_type=F32,
        )
        total = got if total is None else total + got
    total_ref[...] += total


def renew_gains(gains, anchor, total, columns):
    halves = [total[0:48] + total[48:96], total[96:144] + total[144:192]]
    sums = jnp.concatenate(halves, axis=1)
    rows = []
    for f in range(FEW):
        flux = columns[:, 2 + f : 3 + f]
        rho = columns[:, 6:7]
        norm = sums[24 * f + 16 : 24 * f + 24] * (flux * flux)
        divisor = norm + rho
        for c in range(2):
            g = gains[16 * f + 8 * c : 16 * f + 8 * c + 8]
            a = anchor[16 * f + 8 * c : 16 * f + 8 * c + 8]
            n = sums[24 * f + 8 * c : 24 * f + 8 * c + 8] + g * norm
            rows.append(0.5 * (g + (n + rho * a) / divisor))
    return jnp.concatenate(rows, axis=0)


def middle_kernel(
    sigma_ref,
    data_ref,
    left_ref,
    right_ref,
    error_ref,
    sky_ref,
    gains_ref,
    anchor_ref,
    geo_ref,
    gains_out,
    left_out,
    right_out,
    error_out,
    misfit_out,
    table_ref,
    total_ref,
):
    phase, step = pl.program_id(0), pl.program_id(1)
    last = pl.num_programs(1) - 1

    @pl.when((phase == 0) & (step == 0))
    def _():
        total_ref[...] = jnp.zeros_like(total_ref)

    @pl.when(phase == 0)
    def _():
        inverse = sigma_ref[0, 0]

        def run(i, carry):
            at = pl.multiple_of(i * SUB, SUB)
            normal_block(
                data_ref, left_ref, right_ref, error_ref, sky_ref, total_ref, at, inverse
            )
            return carry

        lax.fori_loop(0, LOCAL // SUB, run, 0)

    @pl.when((phase == 0) & (step == last))
    def _():
        gains = renew_gains(gains_ref[...], anchor_ref[...], total_ref[...], geo_ref[...])
        gains_out[...] = gains
        build_table(table_ref, gains)

    @pl.when(phase == 1)
    def _():
        def run(i, misfit):
            at = pl.multiple_of(i * SUB, SUB)
            return model_block(
                data_ref, table_ref, sky_ref, None, (left_out, right_out, error_out, None), at,
                misfit,
            )

        misfit = lax.fori_loop(0, LOCAL // SUB, run, jnp.zeros((8, SUB), F32))
        misfit = jnp.sum(misfit[:, :128] + misfit[:, 128:], axis=0, keepdims=True)

        @pl.when(step == 0)
        def _():
            misfit_out[...] = misfit

        @pl.when(step > 0)
        def _():
            misfit_out[...] += misfit


def last_kernel(
    sigma_ref,
    data_ref,
    left_ref,
    right_ref,
    error_ref,
    sky_ref,
    gains_ref,
    anchor_ref,
    geo_ref,
    gains_out,
    total_ref,
):
    step = pl.program_id(0)

    @pl.when(step == 0)
    def _():
        total_ref[...] = jnp.zeros_like(total_ref)

    inverse = sigma_ref[0, 0]

    def run(i, carry):
        at = pl.multiple_of(i * SUB, SUB)
        normal_block(data_ref, left_ref, right_ref, error_ref, sky_ref, total_ref, at, inverse)
        return carry

    lax.fori_loop(0, LOCAL // SUB, run, 0)

    @pl.when(step == pl.num_programs(0) - 1)
    def _():
        gains_out[...] = renew_gains(
            gains_ref[...], anchor_ref[...], total_ref[...], geo_ref[...]
        )


ROWS = 18
GAIN_ROWS = 2 * FEW * DIRS
SKY = (TIMES, FEW, 2, DIRS)


def shapes_of(rows):
    return jax.ShapeDtypeStruct((PARTS, rows, LOCAL), F32)


def first_call(data, gains, geo):
    at = lambda i: (i, 0, 0)
    return pl.pallas_call(
        first_kernel,
        grid=(PARTS,),
        in_specs=[
            pl.BlockSpec((1, ROWS, LOCAL), at),
            pl.BlockSpec((GAIN_ROWS, STATIONS), lambda i: (0, 0)),
            pl.BlockSpec((DIRS, 8), lambda i: (0, 0)),
        ],
        out_specs=[
            pl.BlockSpec((1, GAIN_ROWS, LOCAL), at),
            pl.BlockSpec((1, GAIN_ROWS, LOCAL), at),
            pl.BlockSpec((1, 8, LOCAL), at),
            pl.BlockSpec((1,) + SKY + (LOCAL,), lambda i: (i, 0, 0, 0, 0, 0)),
        ],
        out_shape=[
            shapes_of(GAIN_ROWS),
            shapes_of(GAIN_ROWS),
            shapes_of(8),
            jax.ShapeDtypeStruct((PARTS,) + SKY + (LOCAL,), F32),
        ],
        scratch_shapes=[pltpu.VMEM((128, 256), BF16)],
        name="first_model",
    )(data, gains, geo)


def middle_call(sigma, data, left, right, error, sky, gains, anchor, geo):
    at = lambda p, i: (i, 0, 0)
    held = lambda p, i: ((1 - p) * i + p * (PARTS - 1), 0, 0)
    made = lambda p, i: (p * i, 0, 0)
    small = lambda p, i: (0, 0)
    return pl.pallas_call(
        middle_kernel,
        grid=(2, PARTS),
        in_specs=[
            pl.BlockSpec(memory_space=pltpu.SMEM),
            pl.BlockSpec((1, ROWS, LOCAL), at),
            pl.BlockSpec((1, GAIN_ROWS, LOCAL), held),
            pl.BlockSpec((1, GAIN_ROWS, LOCAL), held),
            pl.BlockSpec((1, 8, LOCAL), held),
            pl.BlockSpec((1,) + SKY + (LOCAL,), lambda p, i: (i, 0, 0, 0, 0, 0)),
            pl.BlockSpec((GAIN_ROWS, STATIONS), small),
            pl.BlockSpec((GAIN_ROWS, STATIONS), small),
            pl.BlockSpec((DIRS, 8), small),
        ],
        out_specs=[
            pl.BlockSpec((GAIN_ROWS, STATIONS), small),
            pl.BlockSpec((1, GAIN_ROWS, LOCAL), made),
            pl.BlockSpec((1, GAIN_ROWS, LOCAL), made),
            pl.BlockSpec((1, 8, LOCAL), made),
            pl.BlockSpec((1, 128), small),
        ],
        out_shape=[
            jax.ShapeDtypeStruct((GAIN_ROWS, STATIONS), F32),
            shapes_of(GAIN_ROWS),
            shapes_of(GAIN_ROWS),
            shapes_of(8),
            jax.ShapeDtypeStruct((1, 128), F32),
        ],
        scratch_shapes=[pltpu.VMEM((128, 256), BF16), pltpu.VMEM((192, 256), F32)],
        name="normal_and_model",
    )(sigma, data, left, right, error, sky, gains, anchor, geo)


def last_call(sigma, data, left, right, error, sky, gains, anchor, geo):
    at = lambda i: (i, 0, 0)
    small = lambda i: (0, 0)
    return pl.pallas_call(
        last_kernel,
        grid=(PARTS,),
        in_specs=[
            pl.BlockSpec(memory_space=pltpu.SMEM),
            pl.BlockSpec((1, ROWS, LOCAL), at),
            pl.BlockSpec((1, GAIN_ROWS, LOCAL), at),
            pl.BlockSpec((1, GAIN_ROWS, LOCAL), at),
            pl.BlockSpec((1, 8, LOCAL), at),
            pl.BlockSpec((1,) + SKY + (LOCAL,), lambda i: (i, 0, 0, 0, 0, 0)),
            pl.BlockSpec((GAIN_ROWS, STATIONS), small),
            pl.BlockSpec((GAIN_ROWS, STATIONS), small),
            pl.BlockSpec((DIRS, 8), small),
        ],
        out_specs=pl.BlockSpec((GAIN_ROWS, STATIONS), small),
        out_shape=jax.ShapeDtypeStruct((GAIN_ROWS, STATIONS), F32),
        scratch_shapes=[pltpu.VMEM((192, 256), F32)],
        name="normal_last",
    )(sigma, data, left, right, error, sky, gains, anchor, geo)


def legendre(ratios):
    scaled = (ratios - 1.05) / 0.35
    values = [jnp.ones_like(scaled), scaled]
    values.append((3 * scaled * values[1] - 1 * values[0]) / 2)
    return jnp.stack(values[:NPOLY])


def sent_to_all(array, axes):
    count = lax.axis_size(axes)
    return lax.all_to_all(
        jnp.broadcast_to(array[None], (count, *array.shape)), axes, 0, 0, tiled=True
    )


def cholesky_solve(gram, rhs):
    order = len(rhs)
    factor = [[None] * order for _ in range(order)]
    for i in range(order):
        for j in range(i + 1):
            value = gram[i, j]
            for m in range(j):
                value = value - factor[i][m] * factor[j][m]
            factor[i][j] = jnp.sqrt(value) if i == j else value / factor[j][j]
    forward = []
    for i in range(order):
        running = rhs[i]
        for j in range(i):
            running = running - factor[i][j] * forward[j]
        forward.append(running / factor[i][i])
    backward = [None] * order
    for i in reversed(range(order)):
        running = forward[i]
        for j in range(i + 1, order):
            running = running - factor[j][i] * backward[j]
        backward[i] = running / factor[i][i]
    return backward


def own_channels(array, axis, own):
    return lax.dynamic_slice_in_dim(array, own * FEW, FEW, axis)


def packed(vis, flags, pairs, coords):
    vis = vis.reshape(4, PARTS, FEW, LOCAL).transpose(1, 0, 2, 3).reshape(PARTS, 8, LOCAL)
    flags = flags.astype(F32).reshape(TIMES, PARTS, FEW, LOCAL).transpose(1, 0, 2, 3)
    flags = flags.reshape(PARTS, 4, LOCAL)
    coords = jnp.broadcast_to(coords.reshape(1, 4, LOCAL), (PARTS, 4, LOCAL))
    pairs = jnp.broadcast_to(pairs.astype(F32)[None], (PARTS, 2, LOCAL))
    return jnp.concatenate([vis, flags, coords, pairs], axis=1)


def body(
    visibilities,
    sample_flag_weight,
    baseline_station_pair,
    baseline_spatial_coords,
    directions,
    source_flux,
    channel_ratio,
    jones_gains,
    scaled_dual,
    consensus,
    penalty,
):
    devices = lax.axis_size(ALL)
    own = lax.axis_index(BL)
    channels = channel_ratio.shape[0]
    rho = penalty * (2.0 * BASELINES * TIMES / STATIONS)

    send = packed(
        visibilities, sample_flag_weight, baseline_station_pair, baseline_spatial_coords
    )
    send = send.reshape(PARTS, ROWS * LOCAL // 128, 128)
    data = lax.all_to_all(send, BL, 0, 0, tiled=True).reshape(PARTS, ROWS, LOCAL)

    coords = baseline_spatial_coords.reshape(2 * TIMES, LOCAL)
    wide = functools.partial(
        wide_model,
        vis=visibilities,
        flags=sample_flag_weight,
        pairs=baseline_station_pair,
        coords=coords,
        directions=directions,
        flux=source_flux,
        ratio=channel_ratio,
    )
    sums = wide(jones_gains.reshape(-1, STATIONS), residual_out=False)

    ratio = own_channels(channel_ratio, 0, own)
    flux = own_channels(source_flux, 1, own)
    basis = legendre(ratio)
    gram_own = (basis[:, None, :] * basis[None, :, :]).sum(-1)
    payload = jnp.concatenate([sums, jnp.pad(gram_own.reshape(1, 9), ((0, 0), (0, 119)))], axis=1)
    arrived = sent_to_all(payload, ALL)
    arrived = arrived.sum(axis=0)[0]
    squares, weight_count = arrived[:128].sum(), arrived[128:256].sum()
    gram = arrived[256:265].reshape(3, 3)

    def inverse_sigma(squares):
        return (1.0 / (squares / (weight_count + 1.0) + small_term)).reshape(1, 1)

    def rows_of(array):
        part = own_channels(array, 2, own)
        return part.transpose(2, 0, 1, 3)

    dual = rows_of(scaled_dual)
    anchor = (
        sum(
            basis[j][:, None, None, None] * consensus[:, j][None] for j in range(NPOLY)
        )
        - dual
    ).reshape(GAIN_ROWS, STATIONS)
    gains = rows_of(jones_gains).reshape(GAIN_ROWS, STATIONS)
    geo = jnp.concatenate(
        [
            directions.T,
            flux,
            jnp.broadcast_to(ratio[None], (DIRS, FEW)),
            rho[:, None],
            jnp.zeros((DIRS, 1), F32),
        ],
        axis=1,
    )

    left, right, error, sky = first_call(data, gains, geo)
    sigma = inverse_sigma(squares)
    for iteration in range(ITERS - 1):
        gains, left, right, error, misfit = middle_call(
            sigma, data, left, right, error, sky, gains, anchor, geo
        )
        sigma = inverse_sigma(sent_to_all(misfit, ALL).sum())
    gains = last_call(sigma, data, left, right, error, sky, gains, anchor, geo)

    new_rows = gains.reshape(FEW, 2, DIRS, STATIONS)
    lifted = new_rows + dual
    part = 2 * DIRS * STATIONS // devices
    rhs = (basis[:, :, None] * lifted.reshape(1, FEW, -1)).sum(axis=1)
    rhs = rhs.reshape(NPOLY, devices, part).transpose(1, 0, 2)
    rhs = lax.all_to_all(rhs, ALL, 0, 0, tiled=True).sum(axis=0)
    solved = jnp.stack(cholesky_solve(gram, [rhs[j] for j in range(NPOLY)]))
    everyone = sent_to_all(solved, ALL)
    new_consensus = (
        everyone.transpose(1, 0, 2).reshape(NPOLY, 2, DIRS, STATIONS).transpose(1, 0, 2, 3)
    )

    gathered = sent_to_all(gains.reshape(GAIN_ROWS * STATIONS // 128, 128), BL)
    new_gains = (
        gathered.reshape(PARTS * FEW, 2, DIRS, STATIONS).transpose(1, 2, 0, 3)
    )
    residuals = wide(new_gains.reshape(-1, STATIONS), residual_out=True)

    all_basis = legendre(channel_ratio)
    fitted = sum(
        all_basis[j][None, None, :, None] * new_consensus[:, j][:, :, None, :]
        for j in range(NPOLY)
    )
    new_dual = scaled_dual + new_gains - fitted
    return (new_gains, new_consensus, new_dual, residuals)


def solution(mesh):
    split = Mesh(
        mesh.devices.reshape(4, 2, 4, 2, 2), ("bl_0", "bl_1", "freq_0", "freq_1", "freq_2")
    )
    in_specs = (
        P(None, None, FREQ, BL),
        P(None, FREQ, BL),
        P(None, BL),
        P(None, None, BL),
        P(),
        P(None, FREQ),
        P(FREQ),
        P(None, None, FREQ, None),
        P(None, None, FREQ, None),
        P(),
        P(),
    )
    out_specs = (P(None, None, FREQ, None), P(), P(None, None, FREQ, None), P(None, None, FREQ, BL))
    return jax.shard_map(body, mesh=split, in_specs=in_specs, out_specs=out_specs, check_vma=False)
```

```python
import functools

import jax
import jax.numpy as jnp
from jax import lax
from jax.experimental import pallas as pl
from jax.experimental.pallas import tpu as pltpu
from jax.sharding import Mesh
from jax.sharding import PartitionSpec as P

NPOLY = 3
ITERS = 3
BL = ("bl_0", "bl_1")
FREQ = ("freq_0", "freq_1", "freq_2")
ALL = BL + FREQ

STATIONS = 512
DIRS = 8
TIMES = 2
BASELINES = 16384
PARTS = 8
FEW = 2
LOCAL = BASELINES // PARTS
SUB = 256
MODEL_RUNS = 4
NORMAL_RUNS = 4

robust_dof = 2.0
small_term = 1e-06

SIN_TERMS = (
    3.1415926401307086,
    -5.167710083507905,
    2.5500775232148403,
    -0.5982912856219295,
    0.07765766030867731,
)
COS_TERMS = (
    0.9999999997799046,
    -4.934802137078821,
    4.058709159556128,
    -1.3352120030477381,
    0.23493731380150681,
    -0.024396324323359975,
)

F32 = jnp.float32
PER_US = 4.0e6


def lasts(microseconds):
    return pl.CostEstimate(
        flops=int(microseconds * PER_US), transcendentals=0, bytes_accessed=1 << 20
    )


BF16 = jnp.bfloat16


def horner(terms, w):
    value = jnp.full_like(w, terms[-1])
    for term in terms[-2::-1]:
        value = value * w + term
    return value


def turn_parts(turns):
    f = turns - jnp.floor(turns + 0.5)
    w = f * f
    half_sin = f * horner(SIN_TERMS, w)
    half_cos = horner(COS_TERMS, w)
    twice = half_sin + half_sin
    return 1.0 - twice * half_sin, twice * half_cos


def two_parts(value):
    high = value.astype(BF16)
    low = (value - high.astype(F32)).astype(BF16)
    return high, low


def wide_kernel(
    gains_ref,
    vis_ref,
    flag_ref,
    pair_ref,
    coord_ref,
    dirs_ref,
    flux_ref,
    ratio_ref,
    *rest,
    residual_out,
    channels,
    block,
):
    outs, (high_ref, low_ref, left_ref, right_ref, column_ref) = rest[:-5], rest[-5:]
    step = pl.program_id(0)

    @pl.when(step == 0)
    def _():
        own = lax.broadcasted_iota(jnp.int32, (channels, channels), 0)
        own = own == lax.broadcasted_iota(jnp.int32, (channels, channels), 1)
        for k in range(DIRS + 1):
            row = flux_ref[k : k + 1, :] if k < DIRS else ratio_ref[...]
            column = jnp.where(own, jnp.broadcast_to(row, (channels, channels)), 0.0)
            column_ref[k * channels : (k + 1) * channels, :] = jnp.broadcast_to(
                jnp.sum(column, axis=1, keepdims=True), (channels, 128)
            )
        high, low = two_parts(gains_ref[...])
        high_ref[...] = high
        low_ref[...] = low

    stations = lax.broadcasted_iota(jnp.int32, (STATIONS, block), 0)
    for row, target in ((0, left_ref), (1, right_ref)):
        hot = (stations == pair_ref[row : row + 1, :]).astype(F32).astype(BF16)
        target[...] = jnp.dot(high_ref[...], hot, preferred_element_type=F32) + jnp.dot(
            low_ref[...], hot, preferred_element_type=F32
        )
    ratio = column_ref[DIRS * channels :, :1]
    total = [[None, None] for _ in range(TIMES)]
    for k in range(DIRS):
        re = pl.ds(k * channels, channels)
        im = pl.ds((DIRS + k) * channels, channels)
        left_re, left_im = left_ref[re, :], left_ref[im, :]
        right_re, right_im = right_ref[re, :], right_ref[im, :]
        flux = column_ref[re, :1]
        pair_re = (left_re * right_re + left_im * right_im) * flux
        pair_im = (left_im * right_re - left_re * right_im) * flux
        for t in range(TIMES):
            project = (
                dirs_ref[0, k] * coord_ref[0, t : t + 1, :]
                + dirs_ref[1, k] * coord_ref[1, t : t + 1, :]
            )
            sky_re, sky_im = turn_parts(project * ratio)
            model_re = pair_re * sky_re - pair_im * sky_im
            model_im = pair_re * sky_im + pair_im * sky_re
            if k == 0:
                total[t] = [model_re, model_im]
            else:
                total[t] = [total[t][0] + model_re, total[t][1] + model_im]
    if residual_out:
        (residual_ref,) = outs
        for t in range(TIMES):
            residual_ref[0, t] = vis_ref[0, t] - total[t][0]
            residual_ref[1, t] = vis_ref[1, t] - total[t][1]
    else:
        (sums_ref,) = outs
        misfit = jnp.zeros((8, 128), F32)
        count = jnp.zeros((8, 128), F32)
        for t in range(TIMES):
            error_re = vis_ref[0, t] - total[t][0]
            error_im = vis_ref[1, t] - total[t][1]
            flagged = flag_ref[t].astype(F32)
            part = flagged * (error_re * error_re + error_im * error_im)
            for r in range(0, channels, 8):
                for c in range(0, block, 128):
                    misfit += part[r : r + 8, c : c + 128]
                    count += flagged[r : r + 8, c : c + 128]
        sums = jnp.concatenate(
            [jnp.sum(misfit, axis=0, keepdims=True), jnp.sum(count, axis=0, keepdims=True)], axis=1
        )

        @pl.when(step == 0)
        def _():
            sums_ref[...] = sums

        @pl.when(step > 0)
        def _():
            sums_ref[...] += sums


def wide_model(gains, vis, flags, pairs, coords, directions, flux, ratio, residual_out):
    channels = vis.shape[2]
    count = vis.shape[3]
    block = SUB
    rows = 2 * DIRS * channels
    whole = lambda shape: pl.BlockSpec(shape, lambda i: (0,) * len(shape))
    vis_spec = pl.BlockSpec((2, TIMES, channels, block), lambda i: (0, 0, 0, i))
    if residual_out:
        out_shape = jax.ShapeDtypeStruct(vis.shape, F32)
        out_spec = vis_spec
    else:
        out_shape = jax.ShapeDtypeStruct((1, 256), F32)
        out_spec = whole((1, 256))
    return pl.pallas_call(
        functools.partial(
            wide_kernel, residual_out=residual_out, channels=channels, block=block
        ),
        grid=(count // block,),
        in_specs=[
            whole((rows, STATIONS)),
            vis_spec,
            pl.BlockSpec((TIMES, channels, block), lambda i: (0, 0, i)),
            pl.BlockSpec((2, block), lambda i: (0, i)),
            pl.BlockSpec((2, TIMES, block), lambda i: (0, 0, i)),
            pl.BlockSpec(memory_space=pltpu.SMEM),
            whole((DIRS, channels)),
            whole((1, channels)),
        ],
        out_specs=out_spec,
        out_shape=out_shape,
        scratch_shapes=[
            pltpu.VMEM((rows, STATIONS), BF16),
            pltpu.VMEM((rows, STATIONS), BF16),
            pltpu.VMEM((rows, block), F32),
            pltpu.VMEM((rows, block), F32),
            pltpu.VMEM(((DIRS + 1) * channels, 128), F32),
        ],
        cost_estimate=lasts(8),
        name="wide_residual" if residual_out else "wide_misfit",
    )(gains, vis, flags, pairs, coords, directions, flux, ratio.reshape(1, -1))


def swap_sum(rows):
    place = lax.broadcasted_iota(jnp.int32, rows[0].shape, 0)
    for bit in (4, 2, 1):
        mine = (place & bit) == 0
        merged = []
        for i in range(len(rows) // 2):
            a, b = rows[i], rows[i + len(rows) // 2]
            low = a + pltpu.roll(a, 8 - bit, axis=0)
            high = b + pltpu.roll(b, bit, axis=0)
            merged.append(jnp.where(mine, low, high))
        rows = merged
    return rows[0]


def one_hot(places, count):
    row = jnp.concatenate([places, places], axis=0).astype(BF16)
    lanes = places.shape[1]
    base = lax.broadcasted_iota(jnp.int32, (16, lanes), 0).astype(F32)
    one = jnp.ones((16, lanes), BF16)
    none = jnp.zeros((16, lanes), BF16)
    return jnp.concatenate(
        [jnp.where(row == (base + float(i)).astype(BF16), one, none) for i in range(0, count, 16)],
        axis=0,
    )


def model_block(data_ref, table_ref, sky_in, geo, outs, at, misfit):
    left_out, right_out, error_out, sky_out = outs
    lanes = pl.ds(at, SUB)
    picked = []
    for row in (16, 17):
        station = jnp.broadcast_to(data_ref[0, row : row + 1, lanes], (8, SUB))
        quarter = jnp.floor(station * (1.0 / 128.0))
        hot = one_hot(station - 128.0 * quarter, 128)
        got = jnp.dot(
            table_ref[...], jnp.concatenate([hot, hot], axis=0), preferred_element_type=F32
        )
        first, second, upper = quarter == 0.0, quarter == 2.0, quarter < 2.0
        picked.append(
            jnp.concatenate(
                [
                    jnp.where(
                        upper,
                        jnp.where(first, got[i : i + 8], got[32 + i : 40 + i]),
                        jnp.where(second, got[64 + i : 72 + i], got[96 + i : 104 + i]),
                    )
                    for i in range(0, 32, 8)
                ],
                axis=0,
            )
        )
    left, right = picked
    left_out[0, :, lanes] = left
    right_out[0, :, lanes] = right
    pieces = [None] * 8
    for f in range(FEW):
        lr, li = left[16 * f : 16 * f + 8], left[16 * f + 8 : 16 * f + 16]
        rr, ri = right[16 * f : 16 * f + 8], right[16 * f + 8 : 16 * f + 16]
        pair_re = lr * rr + li * ri
        pair_im = li * rr - lr * ri
        for t in range(TIMES):
            if sky_in is None:
                dirs, flux, ratio = geo
                project = dirs[0] * data_ref[0, 12 + t : 13 + t, lanes] + dirs[1] * data_ref[
                    0, 14 + t : 15 + t, lanes
                ]
                sky_re, sky_im = turn_parts(project * ratio[f])
                sky_re = sky_re * flux[f]
                sky_im = sky_im * flux[f]
                sky_out[0, t, f, 0, :, lanes] = sky_re
                sky_out[0, t, f, 1, :, lanes] = sky_im
            else:
                sky_re = sky_in[0, t, f, 0, :, lanes]
                sky_im = sky_in[0, t, f, 1, :, lanes]
            pieces[2 * t + f] = pair_re * sky_re - pair_im * sky_im
            pieces[4 + 2 * t + f] = pair_re * sky_im + pair_im * sky_re
    error = data_ref[0, 0:8, lanes] - swap_sum(pieces)
    error_out[0, :, lanes] = error
    flagged = data_ref[0, 8:12, lanes]
    part = jnp.concatenate([flagged, flagged], axis=0) * (error * error)
    return misfit + part


def model_runs(data_ref, table_ref, sky_in, geo, outs):
    def run(i, misfit):
        for j in range(MODEL_RUNS):
            at = pl.multiple_of((i * MODEL_RUNS + j) * SUB, SUB)
            misfit = model_block(data_ref, table_ref, sky_in, geo, outs, at, misfit)
        return misfit

    return lax.fori_loop(0, LOCAL // SUB // MODEL_RUNS, run, jnp.zeros((8, SUB), F32))


def build_table(table_ref, gains):
    high, low = two_parts(gains)
    for q in range(4):
        table_ref[32 * q : 32 * q + 32, 0:128] = high[:, 128 * q : 128 * q + 128]
        table_ref[32 * q : 32 * q + 32, 128:256] = low[:, 128 * q : 128 * q + 128]


def first_kernel(
    data_ref, gains_ref, geo_ref, left_out, right_out, error_out, sky_out, table_ref
):
    @pl.when(pl.program_id(0) == 0)
    def _():
        build_table(table_ref, gains_ref[...])

    col = lambda i: geo_ref[:, i : i + 1]
    geo = ((col(0), col(1)), (col(2), col(3)), (col(4), col(5)))

    model_runs(data_ref, table_ref, None, geo, (left_out, right_out, error_out, sky_out))


def normal_block(data_ref, left_ref, right_ref, error_ref, sky_ref, at, inverse):
    lanes = pl.ds(at, SUB)
    error = error_ref[0, :, lanes]
    square = error * error
    square = square + pltpu.roll(square, 4, axis=0)
    flagged = data_ref[0, 8:12, lanes]
    flagged = jnp.concatenate([flagged, flagged], axis=0)
    weight = flagged * (robust_dof + 1.0) / (robust_dof + square * inverse)
    scaled = weight * error
    left = left_ref[0, :, lanes]
    right = right_ref[0, :, lanes]
    first, second = [], []
    wide = lambda row: jnp.broadcast_to(row, (DIRS, SUB))
    for f in range(FEW):
        z_re, z_im = None, None
        for t in range(TIMES):
            i = 2 * t + f
            y_re, y_im = wide(scaled[i : i + 1]), wide(scaled[4 + i : 5 + i])
            sky_re = sky_ref[0, t, f, 0, :, lanes]
            sky_im = sky_ref[0, t, f, 1, :, lanes]
            a = sky_re * y_re + sky_im * y_im
            b = sky_re * y_im - sky_im * y_re
            z_re, z_im = (a, b) if t == 0 else (z_re + a, z_im + b)
        power = wide(weight[f : f + 1] + weight[2 + f : 3 + f])
        lr, li = left[16 * f : 16 * f + 8], left[16 * f + 8 : 16 * f + 16]
        rr, ri = right[16 * f : 16 * f + 8], right[16 * f + 8 : 16 * f + 16]
        first += [rr * z_re - ri * z_im, rr * z_im + ri * z_re, (rr * rr + ri * ri) * power]
        second += [lr * z_re + li * z_im, li * z_re - lr * z_im, (lr * lr + li * li) * power]
    made = []
    for row, pieces in ((16, first), (17, second)):
        station = jnp.broadcast_to(data_ref[0, row : row + 1, lanes], (8, SUB))
        half = jnp.where(station >= 256.0, 1.0, 0.0)
        hot = one_hot(station - 256.0 * half, 256)
        high = jnp.concatenate([half, half], axis=0).astype(BF16)
        values = jnp.concatenate(pieces, axis=0)
        parts = two_parts(values)
        upper = [part[i : i + 16] * high for part in parts for i in (0, 16, 32)]
        made.append((jnp.concatenate(list(parts) + upper, axis=0), hot))
    return made


def normal_runs(data_ref, left_ref, right_ref, error_ref, sky_ref, total_ref, inverse):
    def run(i, carry):
        made = []
        for j in range(NORMAL_RUNS):
            at = pl.multiple_of((i * NORMAL_RUNS + j) * SUB, SUB)
            made += normal_block(data_ref, left_ref, right_ref, error_ref, sky_ref, at, inverse)
        total_ref[...] += lax.dot_general(
            jnp.concatenate([m[0] for m in made], axis=1),
            jnp.concatenate([m[1] for m in made], axis=1),
            (((1,), (1,)), ((), ())),
            preferred_element_type=F32,
        )
        return carry

    lax.fori_loop(0, LOCAL // SUB // NORMAL_RUNS, run, 0)


def renew_gains(gains, anchor, total, columns):
    both, upper = total[0:48] + total[48:96], total[96:144] + total[144:192]
    sums = jnp.concatenate([both - upper, upper], axis=1)
    rows = []
    for f in range(FEW):
        flux = columns[:, 2 + f : 3 + f]
        rho = columns[:, 6:7]
        norm = sums[24 * f + 16 : 24 * f + 24] * (flux * flux)
        divisor = norm + rho
        for c in range(2):
            g = gains[16 * f + 8 * c : 16 * f + 8 * c + 8]
            a = anchor[16 * f + 8 * c : 16 * f + 8 * c + 8]
            n = sums[24 * f + 8 * c : 24 * f + 8 * c + 8] + g * norm
            rows.append(0.5 * (g + (n + rho * a) / divisor))
    return jnp.concatenate(rows, axis=0)


def inverse_of(squares_ref, count_ref):
    squares = jnp.sum(jnp.sum(squares_ref[...], axis=0, keepdims=True), axis=1, keepdims=True)
    count = jnp.sum(count_ref[...], axis=1, keepdims=True)
    return 1.0 / (squares / (count + 1.0) + small_term)


def middle_kernel(
    squares_ref,
    count_ref,
    data_ref,
    left_ref,
    right_ref,
    error_ref,
    sky_ref,
    gains_ref,
    anchor_ref,
    geo_ref,
    gains_out,
    left_out,
    right_out,
    error_out,
    misfit_out,
    table_ref,
    total_ref,
    misfit_ref,
):
    phase, step = pl.program_id(0), pl.program_id(1)
    last = pl.num_programs(1) - 1

    @pl.when((phase == 0) & (step == 0))
    def _():
        total_ref[...] = jnp.zeros_like(total_ref)

    @pl.when(phase == 0)
    def _():
        normal_runs(
            data_ref, left_ref, right_ref, error_ref, sky_ref, total_ref,
            inverse_of(squares_ref, count_ref),
        )

    @pl.when((phase == 0) & (step == last))
    def _():
        gains = renew_gains(gains_ref[...], anchor_ref[...], total_ref[...], geo_ref[...])
        gains_out[...] = gains
        build_table(table_ref, gains)

    @pl.when(phase == 1)
    def _():
        misfit = model_runs(
            data_ref, table_ref, sky_ref, None, (left_out, right_out, error_out, None)
        )
        misfit = jnp.sum(misfit[:, :128] + misfit[:, 128:], axis=0, keepdims=True)

        @pl.when(step == 0)
        def _():
            misfit_ref[...] = misfit

        @pl.when(step > 0)
        def _():
            misfit_ref[...] += misfit

        @pl.when(step == last)
        def _():
            misfit_out[...] = jnp.broadcast_to(misfit_ref[...], misfit_out.shape)


def last_kernel(
    squares_ref,
    count_ref,
    data_ref,
    left_ref,
    right_ref,
    error_ref,
    sky_ref,
    gains_ref,
    anchor_ref,
    geo_ref,
    gains_out,
    total_ref,
):
    step = pl.program_id(0)

    @pl.when(step == 0)
    def _():
        total_ref[...] = jnp.zeros_like(total_ref)

    normal_runs(
        data_ref, left_ref, right_ref, error_ref, sky_ref, total_ref,
        inverse_of(squares_ref, count_ref),
    )

    @pl.when(step == pl.num_programs(0) - 1)
    def _():
        gains_out[...] = renew_gains(
            gains_ref[...], anchor_ref[...], total_ref[...], geo_ref[...]
        )


ROWS = 18
GAIN_ROWS = 2 * FEW * DIRS
SKY = (TIMES, FEW, 2, DIRS)


def shapes_of(rows):
    return jax.ShapeDtypeStruct((PARTS, rows, LOCAL), F32)


def first_call(data, gains, geo):
    at = lambda i: (i, 0, 0)
    return pl.pallas_call(
        first_kernel,
        grid=(PARTS,),
        in_specs=[
            pl.BlockSpec((1, ROWS, LOCAL), at),
            pl.BlockSpec((GAIN_ROWS, STATIONS), lambda i: (0, 0)),
            pl.BlockSpec((DIRS, 8), lambda i: (0, 0)),
        ],
        out_specs=[
            pl.BlockSpec((1, GAIN_ROWS, LOCAL), at),
            pl.BlockSpec((1, GAIN_ROWS, LOCAL), at),
            pl.BlockSpec((1, 8, LOCAL), at),
            pl.BlockSpec((1,) + SKY + (LOCAL,), lambda i: (i, 0, 0, 0, 0, 0)),
        ],
        out_shape=[
            shapes_of(GAIN_ROWS),
            shapes_of(GAIN_ROWS),
            shapes_of(8),
            jax.ShapeDtypeStruct((PARTS,) + SKY + (LOCAL,), F32),
        ],
        scratch_shapes=[pltpu.VMEM((128, 256), BF16)],
        cost_estimate=lasts(10),
        name="first_model",
    )(data, gains, geo)


def middle_call(squares, count, data, left, right, error, sky, gains, anchor, geo, devices):
    at = lambda p, i: (i, 0, 0)
    held = lambda p, i: ((1 - p) * i + p * (PARTS - 1), 0, 0)
    made = lambda p, i: (p * i, 0, 0)
    small = lambda p, i: (0, 0)
    return pl.pallas_call(
        middle_kernel,
        grid=(2, PARTS),
        in_specs=[
            pl.BlockSpec(squares.shape, small),
            pl.BlockSpec((1, 128), small),
            pl.BlockSpec((1, ROWS, LOCAL), at),
            pl.BlockSpec((1, GAIN_ROWS, LOCAL), held),
            pl.BlockSpec((1, GAIN_ROWS, LOCAL), held),
            pl.BlockSpec((1, 8, LOCAL), held),
            pl.BlockSpec((1,) + SKY + (LOCAL,), lambda p, i: (i, 0, 0, 0, 0, 0)),
            pl.BlockSpec((GAIN_ROWS, STATIONS), small),
            pl.BlockSpec((GAIN_ROWS, STATIONS), small),
            pl.BlockSpec((DIRS, 8), small),
        ],
        out_specs=[
            pl.BlockSpec((GAIN_ROWS, STATIONS), small),
            pl.BlockSpec((1, GAIN_ROWS, LOCAL), made),
            pl.BlockSpec((1, GAIN_ROWS, LOCAL), made),
            pl.BlockSpec((1, 8, LOCAL), made),
            pl.BlockSpec((devices, 128), small),
        ],
        out_shape=[
            jax.ShapeDtypeStruct((GAIN_ROWS, STATIONS), F32),
            shapes_of(GAIN_ROWS),
            shapes_of(GAIN_ROWS),
            shapes_of(8),
            jax.ShapeDtypeStruct((devices, 128), F32),
        ],
        scratch_shapes=[
            pltpu.VMEM((128, 256), BF16),
            pltpu.VMEM((192, 256), F32),
            pltpu.VMEM((1, 128), F32),
        ],
        cost_estimate=lasts(20),
        name="normal_and_model",
    )(squares, count, data, left, right, error, sky, gains, anchor, geo)


def last_call(squares, count, data, left, right, error, sky, gains, anchor, geo):
    at = lambda i: (i, 0, 0)
    small = lambda i: (0, 0)
    return pl.pallas_call(
        last_kernel,
        grid=(PARTS,),
        in_specs=[
            pl.BlockSpec(squares.shape, small),
            pl.BlockSpec((1, 128), small),
            pl.BlockSpec((1, ROWS, LOCAL), at),
            pl.BlockSpec((1, GAIN_ROWS, LOCAL), at),
            pl.BlockSpec((1, GAIN_ROWS, LOCAL), at),
            pl.BlockSpec((1, 8, LOCAL), at),
            pl.BlockSpec((1,) + SKY + (LOCAL,), lambda i: (i, 0, 0, 0, 0, 0)),
            pl.BlockSpec((GAIN_ROWS, STATIONS), small),
            pl.BlockSpec((GAIN_ROWS, STATIONS), small),
            pl.BlockSpec((DIRS, 8), small),
        ],
        out_specs=pl.BlockSpec((GAIN_ROWS, STATIONS), small),
        out_shape=jax.ShapeDtypeStruct((GAIN_ROWS, STATIONS), F32),
        scratch_shapes=[pltpu.VMEM((192, 256), F32)],
        cost_estimate=lasts(11),
        name="normal_last",
    )(squares, count, data, left, right, error, sky, gains, anchor, geo)


def legendre(ratios):
    scaled = (ratios - 1.05) / 0.35
    values = [jnp.ones_like(scaled), scaled]
    values.append((3 * scaled * values[1] - 1 * values[0]) / 2)
    return jnp.stack(values[:NPOLY])


def sent_to_all(array, axes):
    count = lax.axis_size(axes)
    return lax.all_to_all(
        jnp.broadcast_to(array[None], (count, *array.shape)), axes, 0, 0, tiled=True
    )


def cholesky_solve(gram, rhs):
    order = len(rhs)
    factor = [[None] * order for _ in range(order)]
    for i in range(order):
        for j in range(i + 1):
            value = gram[i, j]
            for m in range(j):
                value = value - factor[i][m] * factor[j][m]
            factor[i][j] = jnp.sqrt(value) if i == j else value / factor[j][j]
    forward = []
    for i in range(order):
        running = rhs[i]
        for j in range(i):
            running = running - factor[i][j] * forward[j]
        forward.append(running / factor[i][i])
    backward = [None] * order
    for i in reversed(range(order)):
        running = forward[i]
        for j in range(i + 1, order):
            running = running - factor[j][i] * backward[j]
        backward[i] = running / factor[i][i]
    return backward


def own_channels(array, axis, own):
    return lax.dynamic_slice_in_dim(array, own * FEW, FEW, axis)


def packed(vis, flags, pairs, coords):
    vis = vis.reshape(4, PARTS, FEW, LOCAL).transpose(1, 0, 2, 3).reshape(PARTS, 8, LOCAL)
    flags = flags.astype(F32).reshape(TIMES, PARTS, FEW, LOCAL).transpose(1, 0, 2, 3)
    flags = flags.reshape(PARTS, 4, LOCAL)
    coords = jnp.broadcast_to(coords.reshape(1, 4, LOCAL), (PARTS, 4, LOCAL))
    pairs = jnp.broadcast_to(pairs.astype(F32)[None], (PARTS, 2, LOCAL))
    return jnp.concatenate([vis, flags, coords, pairs], axis=1)


def body(
    visibilities,
    sample_flag_weight,
    baseline_station_pair,
    baseline_spatial_coords,
    directions,
    source_flux,
    channel_ratio,
    jones_gains,
    scaled_dual,
    consensus,
    penalty,
):
    devices = lax.axis_size(ALL)
    own = lax.axis_index(BL)
    channels = channel_ratio.shape[0]
    rho = penalty * (2.0 * BASELINES * TIMES / STATIONS)

    send = packed(
        visibilities, sample_flag_weight, baseline_station_pair, baseline_spatial_coords
    )
    send = send.reshape(PARTS, ROWS * LOCAL // 128, 128)
    data = lax.all_to_all(send, BL, 0, 0, tiled=True).reshape(PARTS, ROWS, LOCAL)

    wide = functools.partial(
        wide_model,
        vis=visibilities,
        flags=sample_flag_weight,
        pairs=baseline_station_pair,
        coords=baseline_spatial_coords,
        directions=directions,
        flux=source_flux,
        ratio=channel_ratio,
    )
    sums = wide(jones_gains.reshape(-1, STATIONS), residual_out=False)

    ratio = own_channels(channel_ratio, 0, own)
    flux = own_channels(source_flux, 1, own)
    basis = legendre(ratio)
    gram_own = (basis[:, None, :] * basis[None, :, :]).sum(-1)
    sums, data = lax.optimization_barrier((sums, data))
    payload = jnp.concatenate([sums, jnp.pad(gram_own.reshape(1, 9), ((0, 0), (0, 119)))], axis=1)
    arrived = sent_to_all(payload, ALL)
    arrived = arrived.sum(axis=0)
    squares, count = arrived[:, :128], arrived[:, 128:256]
    gram = arrived[0, 256:265].reshape(3, 3)

    def rows_of(array):
        part = own_channels(array, 2, own)
        return part.transpose(2, 0, 1, 3)

    dual = rows_of(scaled_dual)
    anchor = (
        sum(
            basis[j][:, None, None, None] * consensus[:, j][None] for j in range(NPOLY)
        )
        - dual
    ).reshape(GAIN_ROWS, STATIONS)
    gains = rows_of(jones_gains).reshape(GAIN_ROWS, STATIONS)
    geo = jnp.concatenate(
        [
            directions.T,
            flux,
            jnp.broadcast_to(ratio[None], (DIRS, FEW)),
            rho[:, None],
            jnp.zeros((DIRS, 1), F32),
        ],
        axis=1,
    )

    left, right, error, sky = first_call(data, gains, geo)
    for iteration in range(ITERS - 1):
        gains, left, right, error, misfit = middle_call(
            squares, count, data, left, right, error, sky, gains, anchor, geo, devices
        )
        squares = lax.all_to_all(misfit[:, None], ALL, 0, 0, tiled=True)[:, 0]
    gains = last_call(squares, count, data, left, right, error, sky, gains, anchor, geo)

    gathered = sent_to_all(gains.reshape(GAIN_ROWS * STATIONS // 128, 128), BL)
    new_gains = (
        gathered.reshape(PARTS * FEW, 2, DIRS, STATIONS).transpose(1, 2, 0, 3)
    )
    new_gains = lax.optimization_barrier(new_gains)
    residuals = wide(new_gains.reshape(-1, STATIONS), residual_out=True)

    all_basis = legendre(channel_ratio)
    lifted = new_gains + scaled_dual
    rhs = jnp.stack(
        [
            (all_basis[j][None, None, :, None] * lifted).sum(axis=2).reshape(-1, STATIONS)
            for j in range(NPOLY)
        ],
        axis=1,
    )
    rhs = lax.all_to_all(rhs, FREQ, 0, 0, tiled=True)
    rhs = rhs.sum(axis=0)
    solved = jnp.stack(cholesky_solve(gram, [rhs[j] for j in range(NPOLY)]))
    everyone = sent_to_all(solved, FREQ)
    new_consensus = everyone.reshape(2, DIRS, NPOLY, STATIONS).transpose(0, 2, 1, 3)
    fitted = sum(
        all_basis[j][None, None, :, None] * new_consensus[:, j][:, :, None, :]
        for j in range(NPOLY)
    )
    new_dual = lifted - fitted
    return (new_gains, new_consensus, new_dual, residuals)


def solution(mesh):
    split = Mesh(
        mesh.devices.reshape(4, 2, 4, 2, 2), ("bl_0", "bl_1", "freq_0", "freq_1", "freq_2")
    )
    in_specs = (
        P(None, None, FREQ, BL),
        P(None, FREQ, BL),
        P(None, BL),
        P(None, None, BL),
        P(),
        P(None, FREQ),
        P(FREQ),
        P(None, None, FREQ, None),
        P(None, None, FREQ, None),
        P(),
        P(),
    )
    out_specs = (P(None, None, FREQ, None), P(), P(None, None, FREQ, None), P(None, None, FREQ, BL))
    return jax.shard_map(body, mesh=split, in_specs=in_specs, out_specs=out_specs, check_vma=False)
```

```python
import functools

import jax
import jax.numpy as jnp
from jax import lax
from jax.experimental import pallas as pl
from jax.experimental.pallas import tpu as pltpu
from jax.sharding import Mesh
from jax.sharding import PartitionSpec as P

NPOLY = 3
ITERS = 3
BL = ("bl_0", "bl_1")
FREQ = ("freq_0", "freq_1", "freq_2")
ALL = BL + FREQ

STATIONS = 512
DIRS = 8
TIMES = 2
BASELINES = 16384
PARTS = 8
FEW = 2
LOCAL = BASELINES // PARTS
SUB = 256
MODEL_RUNS = 8
NORMAL_RUNS = 4

robust_dof = 2.0
small_term = 1e-06

SIN_TERMS = (
    3.1415926401307086,
    -5.167710083507905,
    2.5500775232148403,
    -0.5982912856219295,
    0.07765766030867731,
)
COS_TERMS = (
    0.9999999997799046,
    -4.934802137078821,
    4.058709159556128,
    -1.3352120030477381,
    0.23493731380150681,
    -0.024396324323359975,
)

F32 = jnp.float32
PER_US = 4.0e6


def lasts(microseconds):
    return pl.CostEstimate(
        flops=int(microseconds * PER_US), transcendentals=0, bytes_accessed=1 << 20
    )


BF16 = jnp.bfloat16


def horner(terms, w):
    value = jnp.full_like(w, terms[-1])
    for term in terms[-2::-1]:
        value = value * w + term
    return value


def turn_parts(turns):
    f = turns - jnp.floor(turns + 0.5)
    w = f * f
    half_sin = f * horner(SIN_TERMS, w)
    half_cos = horner(COS_TERMS, w)
    twice = half_sin + half_sin
    return 1.0 - twice * half_sin, twice * half_cos


def two_parts(value):
    high = value.astype(BF16)
    low = (value - high.astype(F32)).astype(BF16)
    return high, low


def wide_kernel(
    gains_ref,
    vis_ref,
    flag_ref,
    pair_ref,
    coord_ref,
    dirs_ref,
    flux_ref,
    ratio_ref,
    *rest,
    residual_out,
    channels,
    block,
):
    outs, (high_ref, low_ref, left_ref, right_ref, column_ref) = rest[:-5], rest[-5:]
    step = pl.program_id(0)

    @pl.when(step == 0)
    def _():
        own = lax.broadcasted_iota(jnp.int32, (channels, channels), 0)
        own = own == lax.broadcasted_iota(jnp.int32, (channels, channels), 1)
        for k in range(DIRS + 1):
            row = flux_ref[k : k + 1, :] if k < DIRS else ratio_ref[...]
            column = jnp.where(own, jnp.broadcast_to(row, (channels, channels)), 0.0)
            column_ref[k * channels : (k + 1) * channels, :] = jnp.broadcast_to(
                jnp.sum(column, axis=1, keepdims=True), (channels, 128)
            )
        high, low = two_parts(gains_ref[...])
        high_ref[...] = high
        low_ref[...] = low

    stations = lax.broadcasted_iota(jnp.int32, (STATIONS, block), 0)
    for row, target in ((0, left_ref), (1, right_ref)):
        hot = (stations == pair_ref[row : row + 1, :]).astype(F32).astype(BF16)
        target[...] = jnp.dot(high_ref[...], hot, preferred_element_type=F32) + jnp.dot(
            low_ref[...], hot, preferred_element_type=F32
        )
    ratio = column_ref[DIRS * channels :, :1]
    total = [[None, None] for _ in range(TIMES)]
    for k in range(DIRS):
        re = pl.ds(k * channels, channels)
        im = pl.ds((DIRS + k) * channels, channels)
        left_re, left_im = left_ref[re, :], left_ref[im, :]
        right_re, right_im = right_ref[re, :], right_ref[im, :]
        flux = column_ref[re, :1]
        pair_re = (left_re * right_re + left_im * right_im) * flux
        pair_im = (left_im * right_re - left_re * right_im) * flux
        for t in range(TIMES):
            project = (
                dirs_ref[0, k] * coord_ref[0, t : t + 1, :]
                + dirs_ref[1, k] * coord_ref[1, t : t + 1, :]
            )
            sky_re, sky_im = turn_parts(project * ratio)
            model_re = pair_re * sky_re - pair_im * sky_im
            model_im = pair_re * sky_im + pair_im * sky_re
            if k == 0:
                total[t] = [model_re, model_im]
            else:
                total[t] = [total[t][0] + model_re, total[t][1] + model_im]
    if residual_out:
        (residual_ref,) = outs
        for t in range(TIMES):
            residual_ref[0, t] = vis_ref[0, t] - total[t][0]
            residual_ref[1, t] = vis_ref[1, t] - total[t][1]
    else:
        (sums_ref,) = outs
        misfit = jnp.zeros((8, 128), F32)
        count = jnp.zeros((8, 128), F32)
        for t in range(TIMES):
            error_re = vis_ref[0, t] - total[t][0]
            error_im = vis_ref[1, t] - total[t][1]
            flagged = flag_ref[t].astype(F32)
            part = flagged * (error_re * error_re + error_im * error_im)
            for r in range(0, channels, 8):
                for c in range(0, block, 128):
                    misfit += part[r : r + 8, c : c + 128]
                    count += flagged[r : r + 8, c : c + 128]
        sums = jnp.concatenate(
            [jnp.sum(misfit, axis=0, keepdims=True), jnp.sum(count, axis=0, keepdims=True)], axis=1
        )

        @pl.when(step == 0)
        def _():
            sums_ref[...] = sums

        @pl.when(step > 0)
        def _():
            sums_ref[...] += sums


def wide_model(gains, vis, flags, pairs, coords, directions, flux, ratio, residual_out):
    channels = vis.shape[2]
    count = vis.shape[3]
    block = SUB
    rows = 2 * DIRS * channels
    whole = lambda shape: pl.BlockSpec(shape, lambda i: (0,) * len(shape))
    vis_spec = pl.BlockSpec((2, TIMES, channels, block), lambda i: (0, 0, 0, i))
    if residual_out:
        out_shape = jax.ShapeDtypeStruct(vis.shape, F32)
        out_spec = vis_spec
    else:
        out_shape = jax.ShapeDtypeStruct((1, 256), F32)
        out_spec = whole((1, 256))
    return pl.pallas_call(
        functools.partial(
            wide_kernel, residual_out=residual_out, channels=channels, block=block
        ),
        grid=(count // block,),
        in_specs=[
            whole((rows, STATIONS)),
            vis_spec,
            pl.BlockSpec((TIMES, channels, block), lambda i: (0, 0, i)),
            pl.BlockSpec((2, block), lambda i: (0, i)),
            pl.BlockSpec((2, TIMES, block), lambda i: (0, 0, i)),
            pl.BlockSpec(memory_space=pltpu.SMEM),
            whole((DIRS, channels)),
            whole((1, channels)),
        ],
        out_specs=out_spec,
        out_shape=out_shape,
        scratch_shapes=[
            pltpu.VMEM((rows, STATIONS), BF16),
            pltpu.VMEM((rows, STATIONS), BF16),
            pltpu.VMEM((rows, block), F32),
            pltpu.VMEM((rows, block), F32),
            pltpu.VMEM(((DIRS + 1) * channels, 128), F32),
        ],
        cost_estimate=lasts(8),
        compiler_params=pltpu.CompilerParams(vmem_limit_bytes=16 * 1024 * 1024),
        name="wide_residual" if residual_out else "wide_misfit",
    )(gains, vis, flags, pairs, coords, directions, flux, ratio.reshape(1, -1))


def swap_sum(rows):
    place = lax.broadcasted_iota(jnp.int32, rows[0].shape, 0)
    for bit in (4, 2, 1):
        mine = (place & bit) == 0
        merged = []
        for i in range(len(rows) // 2):
            a, b = rows[i], rows[i + len(rows) // 2]
            low = a + pltpu.roll(a, 8 - bit, axis=0)
            high = b + pltpu.roll(b, bit, axis=0)
            merged.append(jnp.where(mine, low, high))
        rows = merged
    return rows[0]


def one_hot(places, count):
    row = jnp.concatenate([places, places], axis=0).astype(BF16)
    lanes = places.shape[1]
    base = lax.broadcasted_iota(jnp.int32, (16, lanes), 0).astype(F32)
    one = jnp.ones((16, lanes), BF16)
    none = jnp.zeros((16, lanes), BF16)
    return jnp.concatenate(
        [jnp.where(row == (base + float(i)).astype(BF16), one, none) for i in range(0, count, 16)],
        axis=0,
    )


def model_block(part, at, data_ref, table_ref, sky_ref, outs, misfit, geo):
    left_out, right_out, error_out = outs
    lanes = pl.ds(at, SUB)
    picked = []
    for side in range(2):
        station = jnp.broadcast_to(data_ref[part, 16 + side : 17 + side, lanes], (8, SUB))
        quarter = jnp.floor(station * (1.0 / 128.0))
        hot = one_hot(station - 128.0 * quarter, 128)
        got = jnp.dot(
            table_ref[...], jnp.concatenate([hot, hot], axis=0), preferred_element_type=F32
        )
        first, second, lower = quarter == 0.0, quarter == 2.0, quarter < 2.0
        picked.append(
            jnp.concatenate(
                [
                    jnp.where(
                        lower,
                        jnp.where(first, got[i : i + 8], got[32 + i : 40 + i]),
                        jnp.where(second, got[64 + i : 72 + i], got[96 + i : 104 + i]),
                    )
                    for i in range(0, 32, 8)
                ],
                axis=0,
            )
        )
    left, right = picked
    left_out[part, :, lanes] = left
    right_out[part, :, lanes] = right
    pieces = [None] * 8
    for f in range(FEW):
        lr, li = left[16 * f : 16 * f + 8], left[16 * f + 8 : 16 * f + 16]
        rr, ri = right[16 * f : 16 * f + 8], right[16 * f + 8 : 16 * f + 16]
        pair_re = lr * rr + li * ri
        pair_im = li * rr - lr * ri
        for t in range(TIMES):
            if geo is not None:
                dirs, flux, ratio = geo
                project = dirs[0] * data_ref[part, 12 + t : 13 + t, lanes] + dirs[
                    1
                ] * data_ref[part, 14 + t : 15 + t, lanes]
                sky_re, sky_im = turn_parts(project * ratio[f])
                sky_re = sky_re * flux[f]
                sky_im = sky_im * flux[f]
                sky_ref[part, t, f, 0, :, lanes] = sky_re
                sky_ref[part, t, f, 1, :, lanes] = sky_im
            else:
                sky_re = sky_ref[part, t, f, 0, :, lanes]
                sky_im = sky_ref[part, t, f, 1, :, lanes]
            pieces[2 * t + f] = pair_re * sky_re - pair_im * sky_im
            pieces[4 + 2 * t + f] = pair_re * sky_im + pair_im * sky_re
    error = data_ref[part, 0:8, lanes] - swap_sum(pieces)
    error_out[part, :, lanes] = error
    flagged = data_ref[part, 8:12, lanes]
    return misfit + jnp.concatenate([flagged, flagged], axis=0) * (error * error)


def model_runs(data_ref, table_ref, sky_ref, outs, geo):
    steps = LOCAL // SUB // MODEL_RUNS

    def run(i, misfit):
        part, first = i // steps, (i % steps) * MODEL_RUNS
        for j in range(MODEL_RUNS):
            at = pl.multiple_of((first + j) * SUB, SUB)
            misfit = model_block(
                part, at, data_ref, table_ref, sky_ref, outs, misfit, geo
            )
        return misfit

    return lax.fori_loop(0, PARTS * steps, run, jnp.zeros((8, SUB), F32))


def build_table(table_ref, gains):
    for p, part in enumerate(two_parts(gains)):
        for q in range(4):
            table_ref[32 * q : 32 * q + 32, 128 * p : 128 * p + 128] = part[
                :, 128 * q : 128 * q + 128
            ]


def normal_block(part, at, data_ref, left_ref, right_ref, error_ref, sky_ref, inverse):
    lanes = pl.ds(at, SUB)
    error = error_ref[part, :, lanes]
    square = error * error
    square = square + pltpu.roll(square, 4, axis=0)
    flagged = data_ref[part, 8:12, lanes]
    flagged = jnp.concatenate([flagged, flagged], axis=0)
    weight = flagged * (robust_dof + 1.0) / (robust_dof + square * inverse)
    scaled = weight * error
    left = left_ref[part, :, lanes]
    right = right_ref[part, :, lanes]
    first, second = [], []
    wide = lambda row: jnp.broadcast_to(row, (DIRS, SUB))
    for f in range(FEW):
        z_re, z_im = None, None
        for t in range(TIMES):
            i = 2 * t + f
            y_re, y_im = wide(scaled[i : i + 1]), wide(scaled[4 + i : 5 + i])
            sky_re = sky_ref[part, t, f, 0, :, lanes]
            sky_im = sky_ref[part, t, f, 1, :, lanes]
            a = sky_re * y_re + sky_im * y_im
            b = sky_re * y_im - sky_im * y_re
            z_re, z_im = (a, b) if t == 0 else (z_re + a, z_im + b)
        power = wide(weight[f : f + 1] + weight[2 + f : 3 + f])
        lr, li = left[16 * f : 16 * f + 8], left[16 * f + 8 : 16 * f + 16]
        rr, ri = right[16 * f : 16 * f + 8], right[16 * f + 8 : 16 * f + 16]
        first += [rr * z_re - ri * z_im, rr * z_im + ri * z_re, (rr * rr + ri * ri) * power]
        second += [lr * z_re + li * z_im, li * z_re - lr * z_im, (lr * lr + li * li) * power]
    made = []
    for side, pieces in ((0, first), (1, second)):
        station = jnp.broadcast_to(data_ref[part, 16 + side : 17 + side, lanes], (8, SUB))
        half = jnp.where(station >= 256.0, 1.0, 0.0)
        high = jnp.concatenate([half, half], axis=0).astype(BF16)
        parts = two_parts(jnp.concatenate(pieces, axis=0))
        upper = [p[i : i + 16] * high for p in parts for i in (0, 16, 32)]
        hot = one_hot(station - 256.0 * half, 256)
        made.append((jnp.concatenate(list(parts) + upper, axis=0), hot))
    return made


def normal_runs(data_ref, left_ref, right_ref, error_ref, sky_ref, total_ref, inverse):
    steps = LOCAL // SUB // NORMAL_RUNS
    total_ref[...] = jnp.zeros_like(total_ref)

    def run(i, carry):
        part, first = i // steps, (i % steps) * NORMAL_RUNS
        made = []
        for j in range(NORMAL_RUNS):
            at = pl.multiple_of((first + j) * SUB, SUB)
            made += normal_block(
                part, at, data_ref, left_ref, right_ref, error_ref, sky_ref, inverse
            )
        total_ref[...] += lax.dot_general(
            jnp.concatenate([m[0] for m in made], axis=1),
            jnp.concatenate([m[1] for m in made], axis=1),
            (((1,), (1,)), ((), ())),
            preferred_element_type=F32,
        )
        return carry

    lax.fori_loop(0, PARTS * steps, run, 0)


def renew_gains(gains, anchor, total, columns):
    both, upper = total[0:48] + total[48:96], total[96:144] + total[144:192]
    sums = jnp.concatenate([both - upper, upper], axis=1)
    rows = []
    for f in range(FEW):
        flux = columns[:, 2 + f : 3 + f]
        rho = columns[:, 6:7]
        norm = sums[24 * f + 16 : 24 * f + 24] * (flux * flux)
        divisor = norm + rho
        for c in range(2):
            g = gains[16 * f + 8 * c : 16 * f + 8 * c + 8]
            a = anchor[16 * f + 8 * c : 16 * f + 8 * c + 8]
            n = sums[24 * f + 8 * c : 24 * f + 8 * c + 8] + g * norm
            rows.append(0.5 * (g + (n + rho * a) / divisor))
    return jnp.concatenate(rows, axis=0)


def inverse_of(squares_ref, count_ref):
    squares = jnp.sum(jnp.sum(squares_ref[...], axis=0, keepdims=True), axis=1, keepdims=True)
    count = jnp.sum(count_ref[...], axis=1, keepdims=True)
    return 1.0 / (squares / (count + 1.0) + small_term)


def renewed(squares_ref, count_ref, data_ref, held, gains_ref, anchor_ref, geo_ref, total_ref):
    normal_runs(data_ref, *held, total_ref, inverse_of(squares_ref, count_ref))
    return renew_gains(gains_ref[...], anchor_ref[...], total_ref[...], geo_ref[...])


def next_model(gains, data_ref, sky_ref, outs, misfit_out, table_ref):
    build_table(table_ref, gains)
    misfit = model_runs(data_ref, table_ref, sky_ref, outs, None)
    misfit = jnp.sum(misfit[:, :128] + misfit[:, 128:], axis=0, keepdims=True)
    misfit_out[...] = jnp.broadcast_to(misfit, misfit_out.shape)


def first_kernel(
    squares_ref,
    count_ref,
    data_ref,
    gains_ref,
    anchor_ref,
    geo_ref,
    gains_out,
    left_out,
    right_out,
    error_out,
    sky_out,
    misfit_out,
    table_ref,
    total_ref,
):
    build_table(table_ref, gains_ref[...])
    col = lambda i: geo_ref[:, i : i + 1]
    geo = ((col(0), col(1)), (col(2), col(3)), (col(4), col(5)))
    outs = (left_out, right_out, error_out)
    model_runs(data_ref, table_ref, sky_out, outs, geo)
    gains = renewed(
        squares_ref, count_ref, data_ref, (*outs, sky_out), gains_ref, anchor_ref, geo_ref, total_ref
    )
    gains_out[...] = gains
    next_model(gains, data_ref, sky_out, outs, misfit_out, table_ref)


def middle_kernel(
    squares_ref,
    count_ref,
    data_ref,
    left_ref,
    right_ref,
    error_ref,
    sky_ref,
    gains_ref,
    anchor_ref,
    geo_ref,
    gains_out,
    left_out,
    right_out,
    error_out,
    misfit_out,
    table_ref,
    total_ref,
):
    held = (left_ref, right_ref, error_ref, sky_ref)
    gains = renewed(
        squares_ref, count_ref, data_ref, held, gains_ref, anchor_ref, geo_ref, total_ref
    )
    gains_out[...] = gains
    next_model(
        gains, data_ref, sky_ref, (left_out, right_out, error_out), misfit_out, table_ref
    )


def last_kernel(
    squares_ref,
    count_ref,
    data_ref,
    left_ref,
    right_ref,
    error_ref,
    sky_ref,
    gains_ref,
    anchor_ref,
    geo_ref,
    gains_out,
    total_ref,
):
    held = (left_ref, right_ref, error_ref, sky_ref)
    gains_out[...] = renewed(
        squares_ref, count_ref, data_ref, held, gains_ref, anchor_ref, geo_ref, total_ref
    )


ROWS = 18
GAIN_ROWS = 2 * FEW * DIRS
SKY = (TIMES, FEW, 2, DIRS)
GRANT = pltpu.CompilerParams(vmem_limit_bytes=8 * 1024 * 1024)
ON_CHIP = pl.BlockSpec(memory_space=pltpu.VMEM)


def shapes_of(rows):
    return jax.ShapeDtypeStruct((PARTS, rows, LOCAL), F32)


def first_call(squares, count, data, gains, anchor, geo, devices):
    return pl.pallas_call(
        first_kernel,
        in_specs=[ON_CHIP] * 6,
        out_specs=[ON_CHIP] * 6,
        out_shape=[
            jax.ShapeDtypeStruct((GAIN_ROWS, STATIONS), F32),
            shapes_of(GAIN_ROWS),
            shapes_of(GAIN_ROWS),
            shapes_of(8),
            jax.ShapeDtypeStruct((PARTS,) + SKY + (LOCAL,), F32),
            jax.ShapeDtypeStruct((devices, 128), F32),
        ],
        scratch_shapes=[pltpu.VMEM((128, 256), BF16), pltpu.VMEM((192, 256), F32)],
        compiler_params=GRANT,
        cost_estimate=lasts(18),
        name="first_step",
    )(squares, count, data, gains, anchor, geo)


def middle_call(squares, count, data, held, gains, anchor, geo, devices):
    return pl.pallas_call(
        middle_kernel,
        in_specs=[ON_CHIP] * 10,
        out_specs=[ON_CHIP] * 5,
        out_shape=[
            jax.ShapeDtypeStruct((GAIN_ROWS, STATIONS), F32),
            shapes_of(GAIN_ROWS),
            shapes_of(GAIN_ROWS),
            shapes_of(8),
            jax.ShapeDtypeStruct((devices, 128), F32),
        ],
        scratch_shapes=[pltpu.VMEM((128, 256), BF16), pltpu.VMEM((192, 256), F32)],
        compiler_params=GRANT,
        cost_estimate=lasts(14),
        name="normal_and_model",
    )(squares, count, data, *held, gains, anchor, geo)


def last_call(squares, count, data, held, gains, anchor, geo):
    return pl.pallas_call(
        last_kernel,
        in_specs=[ON_CHIP] * 10,
        out_specs=ON_CHIP,
        out_shape=jax.ShapeDtypeStruct((GAIN_ROWS, STATIONS), F32),
        scratch_shapes=[pltpu.VMEM((192, 256), F32)],
        compiler_params=GRANT,
        cost_estimate=lasts(8),
        name="normal_last",
    )(squares, count, data, *held, gains, anchor, geo)


def legendre(ratios):
    scaled = (ratios - 1.05) / 0.35
    values = [jnp.ones_like(scaled), scaled]
    values.append((3 * scaled * values[1] - 1 * values[0]) / 2)
    return jnp.stack(values[:NPOLY])


def sent_to_all(array, axes):
    count = lax.axis_size(axes)
    return lax.all_to_all(
        jnp.broadcast_to(array[None], (count, *array.shape)), axes, 0, 0, tiled=True
    )


def cholesky_solve(gram, rhs):
    order = len(rhs)
    factor = [[None] * order for _ in range(order)]
    for i in range(order):
        for j in range(i + 1):
            value = gram[i, j]
            for m in range(j):
                value = value - factor[i][m] * factor[j][m]
            factor[i][j] = jnp.sqrt(value) if i == j else value / factor[j][j]
    forward = []
    for i in range(order):
        running = rhs[i]
        for j in range(i):
            running = running - factor[i][j] * forward[j]
        forward.append(running / factor[i][i])
    backward = [None] * order
    for i in reversed(range(order)):
        running = forward[i]
        for j in range(i + 1, order):
            running = running - factor[j][i] * backward[j]
        backward[i] = running / factor[i][i]
    return backward


def own_channels(array, axis, own):
    return lax.dynamic_slice_in_dim(array, own * FEW, FEW, axis)


def packed(vis, flags, pairs, coords):
    vis = vis.reshape(4, PARTS, FEW, LOCAL).transpose(1, 0, 2, 3).reshape(PARTS, 8, LOCAL)
    flags = flags.astype(F32).reshape(TIMES, PARTS, FEW, LOCAL).transpose(1, 0, 2, 3)
    flags = flags.reshape(PARTS, 4, LOCAL)
    coords = jnp.broadcast_to(coords.reshape(1, 4, LOCAL), (PARTS, 4, LOCAL))
    pairs = jnp.broadcast_to(pairs.astype(F32)[None], (PARTS, 2, LOCAL))
    return jnp.concatenate([vis, flags, coords, pairs], axis=1)


def body(
    visibilities,
    sample_flag_weight,
    baseline_station_pair,
    baseline_spatial_coords,
    directions,
    source_flux,
    channel_ratio,
    jones_gains,
    scaled_dual,
    consensus,
    penalty,
):
    devices = lax.axis_size(ALL)
    own = lax.axis_index(BL)
    channels = channel_ratio.shape[0]
    rho = penalty * (2.0 * BASELINES * TIMES / STATIONS)

    wide = functools.partial(
        wide_model,
        vis=visibilities,
        flags=sample_flag_weight,
        pairs=baseline_station_pair,
        coords=baseline_spatial_coords,
        directions=directions,
        flux=source_flux,
        ratio=channel_ratio,
    )
    sums = wide(jones_gains.reshape(-1, STATIONS), residual_out=False)

    ratio = own_channels(channel_ratio, 0, own)
    flux = own_channels(source_flux, 1, own)
    basis = legendre(ratio)
    gram_own = (basis[:, None, :] * basis[None, :, :]).sum(-1)
    payload = jnp.concatenate([sums, jnp.pad(gram_own.reshape(1, 9), ((0, 0), (0, 119)))], axis=1)
    arrived = sent_to_all(payload, ALL)
    send = packed(
        visibilities, sample_flag_weight, baseline_station_pair, baseline_spatial_coords
    )
    arrived, send = lax.optimization_barrier(
        (arrived, send.reshape(PARTS, ROWS * LOCAL // 128, 128))
    )
    data = lax.all_to_all(send, BL, 0, 0, tiled=True).reshape(PARTS, ROWS, LOCAL)
    arrived = arrived.sum(axis=0)
    squares, count = arrived[:, :128], arrived[:, 128:256]
    gram = arrived[0, 256:265].reshape(3, 3)

    def rows_of(array):
        part = own_channels(array, 2, own)
        return part.transpose(2, 0, 1, 3)

    dual = rows_of(scaled_dual)
    anchor = (
        sum(
            basis[j][:, None, None, None] * consensus[:, j][None] for j in range(NPOLY)
        )
        - dual
    ).reshape(GAIN_ROWS, STATIONS)
    gains = rows_of(jones_gains).reshape(GAIN_ROWS, STATIONS)
    geo = jnp.concatenate(
        [
            directions.T,
            flux,
            jnp.broadcast_to(ratio[None], (DIRS, FEW)),
            rho[:, None],
            jnp.zeros((DIRS, 1), F32),
        ],
        axis=1,
    )

    gains, left, right, error, sky, misfit = first_call(
        squares, count, data, gains, anchor, geo, devices
    )
    for iteration in range(1, ITERS):
        squares = lax.all_to_all(misfit[:, None], ALL, 0, 0, tiled=True)[:, 0]
        held = (left, right, error, sky)
        if iteration + 1 < ITERS:
            gains, left, right, error, misfit = middle_call(
                squares, count, data, held, gains, anchor, geo, devices
            )
        else:
            gains = last_call(squares, count, data, held, gains, anchor, geo)

    gathered = sent_to_all(gains.reshape(GAIN_ROWS * STATIONS // 128, 128), BL)
    new_gains = (
        gathered.reshape(PARTS * FEW, 2, DIRS, STATIONS).transpose(1, 2, 0, 3)
    )
    new_gains = lax.optimization_barrier(new_gains)
    residuals = wide(new_gains.reshape(-1, STATIONS), residual_out=True)

    all_basis = legendre(channel_ratio)
    lifted = new_gains + scaled_dual
    rhs = jnp.stack(
        [
            (all_basis[j][None, None, :, None] * lifted).sum(axis=2).reshape(-1, STATIONS)
            for j in range(NPOLY)
        ],
        axis=1,
    )
    rhs = lax.all_to_all(rhs, FREQ, 0, 0, tiled=True)
    rhs = rhs.sum(axis=0)
    solved = jnp.stack(cholesky_solve(gram, [rhs[j] for j in range(NPOLY)]))
    everyone = sent_to_all(solved, FREQ)
    new_consensus = everyone.reshape(2, DIRS, NPOLY, STATIONS).transpose(0, 2, 1, 3)
    fitted = sum(
        all_basis[j][None, None, :, None] * new_consensus[:, j][:, :, None, :]
        for j in range(NPOLY)
    )
    new_dual = lifted - fitted
    return (new_gains, new_consensus, new_dual, residuals)


def solution(mesh):
    split = Mesh(
        mesh.devices.reshape(4, 2, 4, 2, 2), ("bl_0", "bl_1", "freq_0", "freq_1", "freq_2")
    )
    in_specs = (
        P(None, None, FREQ, BL),
        P(None, FREQ, BL),
        P(None, BL),
        P(None, None, BL),
        P(),
        P(None, FREQ),
        P(FREQ),
        P(None, None, FREQ, None),
        P(None, None, FREQ, None),
        P(),
        P(),
    )
    out_specs = (P(None, None, FREQ, None), P(), P(None, None, FREQ, None), P(None, None, FREQ, BL))
    return jax.shard_map(body, mesh=split, in_specs=in_specs, out_specs=out_specs, check_vma=False)
```

```python
import functools

import jax
import jax.numpy as jnp
from jax import lax
from jax.experimental import pallas as pl
from jax.experimental.pallas import tpu as pltpu
from jax.sharding import Mesh
from jax.sharding import PartitionSpec as P

NPOLY = 3
ITERS = 3
BL = ("bl_0", "bl_1")
FREQ = ("freq_0", "freq_1", "freq_2")
ALL = BL + FREQ

STATIONS = 512
DIRS = 8
TIMES = 2
BASELINES = 16384
PARTS = 8
FEW = 2
LOCAL = BASELINES // PARTS
SUB = 256
MODEL_RUNS = 8
NORMAL_RUNS = 4

robust_dof = 2.0
small_term = 1e-06

SIN_TERMS = (
    3.1415926401307086,
    -5.167710083507905,
    2.5500775232148403,
    -0.5982912856219295,
    0.07765766030867731,
)
COS_TERMS = (
    0.9999999997799046,
    -4.934802137078821,
    4.058709159556128,
    -1.3352120030477381,
    0.23493731380150681,
    -0.024396324323359975,
)

F32 = jnp.float32
PER_US = 4.0e6


def lasts(microseconds):
    return pl.CostEstimate(
        flops=int(microseconds * PER_US), transcendentals=0, bytes_accessed=1 << 20
    )


BF16 = jnp.bfloat16


def legendre(ratios):
    scaled = (ratios - 1.05) / 0.35
    values = [jnp.ones_like(scaled), scaled]
    values.append((3 * scaled * values[1] - 1 * values[0]) / 2)
    return values[:NPOLY]


def horner(terms, w):
    value = jnp.full_like(w, terms[-1])
    for term in terms[-2::-1]:
        value = value * w + term
    return value


def turn_parts(turns):
    f = turns - jnp.floor(turns + 0.5)
    w = f * f
    half_sin = f * horner(SIN_TERMS, w)
    half_cos = horner(COS_TERMS, w)
    twice = half_sin + half_sin
    return 1.0 - twice * half_sin, twice * half_cos


def two_parts(value):
    high = value.astype(BF16)
    low = (value - high.astype(F32)).astype(BF16)
    return high, low


def wide_kernel(
    gains_ref,
    vis_ref,
    flag_ref,
    pair_ref,
    coord_ref,
    dirs_ref,
    flux_ref,
    ratio_ref,
    *rest,
    residual_out,
    channels,
    block,
):
    outs, rest = rest[:1], rest[1:]
    high_ref, low_ref, left_ref, right_ref, column_ref, held_ref = rest
    step = pl.program_id(0)

    @pl.when(step == 0)
    def _():
        own = lax.broadcasted_iota(jnp.int32, (channels, channels), 0)
        own = own == lax.broadcasted_iota(jnp.int32, (channels, channels), 1)
        for k in range(DIRS + 1):
            row = flux_ref[k : k + 1, :] if k < DIRS else ratio_ref[...]
            column = jnp.where(own, jnp.broadcast_to(row, (channels, channels)), 0.0)
            column_ref[k * channels : (k + 1) * channels, :] = jnp.broadcast_to(
                jnp.sum(column, axis=1, keepdims=True), (channels, 128)
            )
        high, low = two_parts(gains_ref[...])
        high_ref[...] = high
        low_ref[...] = low

    stations = lax.broadcasted_iota(jnp.int32, (STATIONS, block), 0)
    for row, target in ((0, left_ref), (1, right_ref)):
        hot = (stations == pair_ref[row : row + 1, :]).astype(F32).astype(BF16)
        target[...] = jnp.dot(high_ref[...], hot, preferred_element_type=F32) + jnp.dot(
            low_ref[...], hot, preferred_element_type=F32
        )
    ratio = column_ref[DIRS * channels :, :1]
    total = [[None, None] for _ in range(TIMES)]
    for k in range(DIRS):
        re = pl.ds(k * channels, channels)
        im = pl.ds((DIRS + k) * channels, channels)
        left_re, left_im = left_ref[re, :], left_ref[im, :]
        right_re, right_im = right_ref[re, :], right_ref[im, :]
        flux = column_ref[re, :1]
        pair_re = (left_re * right_re + left_im * right_im) * flux
        pair_im = (left_im * right_re - left_re * right_im) * flux
        for t in range(TIMES):
            project = (
                dirs_ref[0, k] * coord_ref[0, t : t + 1, :]
                + dirs_ref[1, k] * coord_ref[1, t : t + 1, :]
            )
            sky_re, sky_im = turn_parts(project * ratio)
            model_re = pair_re * sky_re - pair_im * sky_im
            model_im = pair_re * sky_im + pair_im * sky_re
            if k == 0:
                total[t] = [model_re, model_im]
            else:
                total[t] = [total[t][0] + model_re, total[t][1] + model_im]
    if residual_out:
        (residual_ref,) = outs
        for t in range(TIMES):
            residual_ref[0, t] = vis_ref[0, t] - total[t][0]
            residual_ref[1, t] = vis_ref[1, t] - total[t][1]
    else:
        (sums_ref,) = outs
        misfit = jnp.zeros((8, 128), F32)
        count = jnp.zeros((8, 128), F32)
        for t in range(TIMES):
            error_re = vis_ref[0, t] - total[t][0]
            error_im = vis_ref[1, t] - total[t][1]
            flagged = flag_ref[t].astype(F32)
            part = flagged * (error_re * error_re + error_im * error_im)
            for r in range(0, channels, 8):
                for c in range(0, block, 128):
                    misfit += part[r : r + 8, c : c + 128]
                    count += flagged[r : r + 8, c : c + 128]
        step_sums = jnp.concatenate([misfit, count], axis=0)

        @pl.when(step == 0)
        def _():
            held_ref[...] = step_sums

        @pl.when(step > 0)
        def _():
            held_ref[...] += step_sums

        @pl.when(step == pl.num_programs(0) - 1)
        def _():
            full = lambda x: jnp.sum(jnp.sum(x, axis=0, keepdims=True), axis=1, keepdims=True)
            basis = legendre(ratio_ref[...])
            entries = [full(held_ref[0:8, :]), full(held_ref[8:16, :])]
            entries += [full(basis[i] * basis[j]) for i in range(NPOLY) for j in range(i + 1)]
            lane = lax.broadcasted_iota(jnp.int32, (8, 128), 1)
            row = jnp.zeros((8, 128), F32)
            for i, entry in enumerate(entries):
                row = jnp.where(lane == i, jnp.broadcast_to(entry, (8, 128)), row)
            sums_ref[...] = jnp.broadcast_to(row[0:1], sums_ref.shape)


def wide_model(gains, vis, flags, pairs, coords, directions, flux, ratio, residual_out, devices=None):
    channels = vis.shape[2]
    count = vis.shape[3]
    block = SUB
    rows = 2 * DIRS * channels
    whole = lambda shape: pl.BlockSpec(shape, lambda i: (0,) * len(shape))
    vis_spec = pl.BlockSpec((2, TIMES, channels, block), lambda i: (0, 0, 0, i))
    if residual_out:
        out_shape = jax.ShapeDtypeStruct(vis.shape, F32)
        out_spec = vis_spec
    else:
        out_shape = jax.ShapeDtypeStruct((devices, 128), F32)
        out_spec = whole((devices, 128))
    return pl.pallas_call(
        functools.partial(
            wide_kernel, residual_out=residual_out, channels=channels, block=block
        ),
        grid=(count // block,),
        in_specs=[
            whole((rows, STATIONS)),
            vis_spec,
            pl.BlockSpec((TIMES, channels, block), lambda i: (0, 0, i)),
            pl.BlockSpec((2, block), lambda i: (0, i)),
            pl.BlockSpec((2, TIMES, block), lambda i: (0, 0, i)),
            pl.BlockSpec(memory_space=pltpu.SMEM),
            whole((DIRS, channels)),
            whole((1, channels)),
        ],
        out_specs=out_spec,
        out_shape=out_shape,
        scratch_shapes=[
            pltpu.VMEM((rows, STATIONS), BF16),
            pltpu.VMEM((rows, STATIONS), BF16),
            pltpu.VMEM((rows, block), F32),
            pltpu.VMEM((rows, block), F32),
            pltpu.VMEM(((DIRS + 1) * channels, 128), F32),
            pltpu.VMEM((16, 128), F32),
        ],
        cost_estimate=lasts(8),
        name="wide_residual" if residual_out else "wide_misfit",
    )(gains, vis, flags, pairs, coords, directions, flux, ratio.reshape(1, -1))


def swap_sum(rows):
    place = lax.broadcasted_iota(jnp.int32, rows[0].shape, 0)
    for bit in (4, 2, 1):
        mine = (place & bit) == 0
        merged = []
        for i in range(len(rows) // 2):
            a, b = rows[i], rows[i + len(rows) // 2]
            low = a + pltpu.roll(a, 8 - bit, axis=0)
            high = b + pltpu.roll(b, bit, axis=0)
            merged.append(jnp.where(mine, low, high))
        rows = merged
    return rows[0]


def one_hot(places, count):
    row = jnp.concatenate([places, places], axis=0).astype(BF16)
    lanes = places.shape[1]
    base = lax.broadcasted_iota(jnp.int32, (16, lanes), 0).astype(F32)
    one = jnp.ones((16, lanes), BF16)
    none = jnp.zeros((16, lanes), BF16)
    return jnp.concatenate(
        [jnp.where(row == (base + float(i)).astype(BF16), one, none) for i in range(0, count, 16)],
        axis=0,
    )


def model_block(part, at, data_ref, table_ref, sky_ref, outs, misfit, geo):
    left_out, right_out, error_out = outs
    lanes = pl.ds(at, SUB)
    picked = []
    for side in range(2):
        station = jnp.broadcast_to(data_ref[part, 16 + side : 17 + side, lanes], (8, SUB))
        quarter = jnp.floor(station * (1.0 / 128.0))
        hot = one_hot(station - 128.0 * quarter, 128)
        got = jnp.dot(
            table_ref[...], jnp.concatenate([hot, hot], axis=0), preferred_element_type=F32
        )
        first, second, lower = quarter == 0.0, quarter == 2.0, quarter < 2.0
        picked.append(
            jnp.concatenate(
                [
                    jnp.where(
                        lower,
                        jnp.where(first, got[i : i + 8], got[32 + i : 40 + i]),
                        jnp.where(second, got[64 + i : 72 + i], got[96 + i : 104 + i]),
                    )
                    for i in range(0, 32, 8)
                ],
                axis=0,
            )
        )
    left, right = picked
    left_out[part, :, lanes] = left
    right_out[part, :, lanes] = right
    pieces = [None] * 8
    for f in range(FEW):
        lr, li = left[16 * f : 16 * f + 8], left[16 * f + 8 : 16 * f + 16]
        rr, ri = right[16 * f : 16 * f + 8], right[16 * f + 8 : 16 * f + 16]
        pair_re = lr * rr + li * ri
        pair_im = li * rr - lr * ri
        for t in range(TIMES):
            if geo is not None:
                dirs, flux, ratio = geo
                project = dirs[0] * data_ref[part, 12 + t : 13 + t, lanes] + dirs[
                    1
                ] * data_ref[part, 14 + t : 15 + t, lanes]
                sky_re, sky_im = turn_parts(project * ratio[f])
                sky_re = sky_re * flux[f]
                sky_im = sky_im * flux[f]
                sky_ref[part, t, f, 0, :, lanes] = sky_re
                sky_ref[part, t, f, 1, :, lanes] = sky_im
            else:
                sky_re = sky_ref[part, t, f, 0, :, lanes]
                sky_im = sky_ref[part, t, f, 1, :, lanes]
            pieces[2 * t + f] = pair_re * sky_re - pair_im * sky_im
            pieces[4 + 2 * t + f] = pair_re * sky_im + pair_im * sky_re
    error = data_ref[part, 0:8, lanes] - swap_sum(pieces)
    error_out[part, :, lanes] = error
    flagged = data_ref[part, 8:12, lanes]
    return misfit + jnp.concatenate([flagged, flagged], axis=0) * (error * error)


def model_runs(data_ref, table_ref, sky_ref, outs, geo):
    steps = LOCAL // SUB // MODEL_RUNS

    def run(i, misfit):
        part, first = i // steps, (i % steps) * MODEL_RUNS
        for j in range(MODEL_RUNS):
            at = pl.multiple_of((first + j) * SUB, SUB)
            misfit = model_block(
                part, at, data_ref, table_ref, sky_ref, outs, misfit, geo
            )
        return misfit

    return lax.fori_loop(0, PARTS * steps, run, jnp.zeros((8, SUB), F32))


def build_table(table_ref, gains):
    for p, part in enumerate(two_parts(gains)):
        for q in range(4):
            table_ref[32 * q : 32 * q + 32, 128 * p : 128 * p + 128] = part[
                :, 128 * q : 128 * q + 128
            ]


def normal_block(part, at, data_ref, left_ref, right_ref, error_ref, sky_ref, inverse):
    lanes = pl.ds(at, SUB)
    error = error_ref[part, :, lanes]
    square = error * error
    square = square + pltpu.roll(square, 4, axis=0)
    flagged = data_ref[part, 8:12, lanes]
    flagged = jnp.concatenate([flagged, flagged], axis=0)
    weight = flagged * (robust_dof + 1.0) / (robust_dof + square * inverse)
    scaled = weight * error
    left = left_ref[part, :, lanes]
    right = right_ref[part, :, lanes]
    first, second = [], []
    wide = lambda row: jnp.broadcast_to(row, (DIRS, SUB))
    for f in range(FEW):
        z_re, z_im = None, None
        for t in range(TIMES):
            i = 2 * t + f
            y_re, y_im = wide(scaled[i : i + 1]), wide(scaled[4 + i : 5 + i])
            sky_re = sky_ref[part, t, f, 0, :, lanes]
            sky_im = sky_ref[part, t, f, 1, :, lanes]
            a = sky_re * y_re + sky_im * y_im
            b = sky_re * y_im - sky_im * y_re
            z_re, z_im = (a, b) if t == 0 else (z_re + a, z_im + b)
        power = wide(weight[f : f + 1] + weight[2 + f : 3 + f])
        lr, li = left[16 * f : 16 * f + 8], left[16 * f + 8 : 16 * f + 16]
        rr, ri = right[16 * f : 16 * f + 8], right[16 * f + 8 : 16 * f + 16]
        first += [rr * z_re - ri * z_im, rr * z_im + ri * z_re, (rr * rr + ri * ri) * power]
        second += [lr * z_re + li * z_im, li * z_re - lr * z_im, (lr * lr + li * li) * power]
    made = []
    for side, pieces in ((0, first), (1, second)):
        station = jnp.broadcast_to(data_ref[part, 16 + side : 17 + side, lanes], (8, SUB))
        half = jnp.where(station >= 256.0, 1.0, 0.0)
        high = jnp.concatenate([half, half], axis=0).astype(BF16)
        parts = two_parts(jnp.concatenate(pieces, axis=0))
        upper = [p[i : i + 16] * high for p in parts for i in (0, 16, 32)]
        hot = one_hot(station - 256.0 * half, 256)
        made.append((jnp.concatenate(list(parts) + upper, axis=0), hot))
    return made


def normal_runs(data_ref, left_ref, right_ref, error_ref, sky_ref, total_ref, inverse):
    steps = LOCAL // SUB // NORMAL_RUNS
    total_ref[...] = jnp.zeros_like(total_ref)

    def run(i, carry):
        part, first = i // steps, (i % steps) * NORMAL_RUNS
        made = []
        for j in range(NORMAL_RUNS):
            at = pl.multiple_of((first + j) * SUB, SUB)
            made += normal_block(
                part, at, data_ref, left_ref, right_ref, error_ref, sky_ref, inverse
            )
        total_ref[...] += lax.dot_general(
            jnp.concatenate([m[0] for m in made], axis=1),
            jnp.concatenate([m[1] for m in made], axis=1),
            (((1,), (1,)), ((), ())),
            preferred_element_type=F32,
        )
        return carry

    lax.fori_loop(0, PARTS * steps, run, 0)


def renew_gains(gains, anchor, total, columns):
    both, upper = total[0:48] + total[48:96], total[96:144] + total[144:192]
    sums = jnp.concatenate([both - upper, upper], axis=1)
    rows = []
    for f in range(FEW):
        flux = columns[:, 2 + f : 3 + f]
        rho = columns[:, 6:7]
        norm = sums[24 * f + 16 : 24 * f + 24] * (flux * flux)
        divisor = norm + rho
        for c in range(2):
            g = gains[16 * f + 8 * c : 16 * f + 8 * c + 8]
            a = anchor[16 * f + 8 * c : 16 * f + 8 * c + 8]
            n = sums[24 * f + 8 * c : 24 * f + 8 * c + 8] + g * norm
            rows.append(0.5 * (g + (n + rho * a) / divisor))
    return jnp.concatenate(rows, axis=0)


def inverse_of(squares_ref, count_ref):
    squares = jnp.sum(squares_ref[...], axis=0, keepdims=True)
    count = jnp.sum(count_ref[...], axis=0, keepdims=True)
    lane = lax.broadcasted_iota(jnp.int32, (1, 128), 1)
    pick = lambda row, i: jnp.sum(jnp.where(lane == i, row, 0.0), axis=1, keepdims=True)
    return 1.0 / (pick(squares, 0) / (pick(count, 1) + 1.0) + small_term)


def renewed(
    squares_ref, count_ref, data_ref, held, gains_ref, anchor_ref, geo_ref, total_ref
):
    normal_runs(data_ref, *held, total_ref, inverse_of(squares_ref, count_ref))
    return renew_gains(gains_ref[...], anchor_ref[...], total_ref[...], geo_ref[...])


def next_model(gains, data_ref, sky_ref, outs, misfit_out, table_ref):
    build_table(table_ref, gains)
    misfit = model_runs(data_ref, table_ref, sky_ref, outs, None)
    misfit = jnp.sum(misfit[:, :128] + misfit[:, 128:], axis=0, keepdims=True)
    misfit = jnp.sum(misfit, axis=1, keepdims=True)
    misfit_out[...] = jnp.broadcast_to(misfit, misfit_out.shape)


def first_kernel(
    data_ref, gains_ref, geo_ref, left_out, right_out, error_out, sky_out, table_ref
):
    build_table(table_ref, gains_ref[...])
    col = lambda i: geo_ref[:, i : i + 1]
    geo = ((col(0), col(1)), (col(2), col(3)), (col(4), col(5)))
    model_runs(data_ref, table_ref, sky_out, (left_out, right_out, error_out), geo)


def middle_kernel(
    squares_ref,
    count_ref,
    data_ref,
    left_ref,
    right_ref,
    error_ref,
    sky_ref,
    gains_ref,
    anchor_ref,
    geo_ref,
    gains_out,
    left_out,
    right_out,
    error_out,
    misfit_out,
    table_ref,
    total_ref,
):
    held = (left_ref, right_ref, error_ref, sky_ref)
    gains = renewed(
        squares_ref, count_ref, data_ref, held, gains_ref, anchor_ref, geo_ref, total_ref
    )
    gains_out[...] = gains
    next_model(
        gains, data_ref, sky_ref, (left_out, right_out, error_out), misfit_out, table_ref
    )


def last_kernel(
    squares_ref,
    count_ref,
    data_ref,
    left_ref,
    right_ref,
    error_ref,
    sky_ref,
    gains_ref,
    anchor_ref,
    geo_ref,
    gains_out,
    total_ref,
):
    held = (left_ref, right_ref, error_ref, sky_ref)
    gains_out[...] = renewed(
        squares_ref, count_ref, data_ref, held, gains_ref, anchor_ref, geo_ref, total_ref
    )


ROWS = 18
GAIN_ROWS = 2 * FEW * DIRS
SKY = (TIMES, FEW, 2, DIRS)
GRANT = pltpu.CompilerParams(vmem_limit_bytes=8 * 1024 * 1024)
ON_CHIP = pl.BlockSpec(memory_space=pltpu.VMEM)


def shapes_of(rows):
    return jax.ShapeDtypeStruct((PARTS, rows, LOCAL), F32)


def held_shapes():
    return [
        shapes_of(GAIN_ROWS),
        shapes_of(GAIN_ROWS),
        shapes_of(8),
        jax.ShapeDtypeStruct((PARTS,) + SKY + (LOCAL,), F32),
    ]


def first_call(data, gains, geo):
    return pl.pallas_call(
        first_kernel,
        in_specs=[ON_CHIP] * 3,
        out_specs=[ON_CHIP] * 4,
        out_shape=held_shapes(),
        scratch_shapes=[pltpu.VMEM((128, 256), BF16)],
        compiler_params=GRANT,
        cost_estimate=lasts(6),
        name="first_model",
    )(data, gains, geo)


def middle_call(squares, count, data, held, gains, anchor, geo, devices):
    return pl.pallas_call(
        middle_kernel,
        in_specs=[ON_CHIP] * 10,
        out_specs=[ON_CHIP] * 5,
        out_shape=[
            jax.ShapeDtypeStruct((GAIN_ROWS, STATIONS), F32),
            shapes_of(GAIN_ROWS),
            shapes_of(GAIN_ROWS),
            shapes_of(8),
            jax.ShapeDtypeStruct((devices, 128), F32),
        ],
        scratch_shapes=[pltpu.VMEM((128, 256), BF16), pltpu.VMEM((192, 256), F32)],
        compiler_params=GRANT,
        cost_estimate=lasts(14),
        name="normal_and_model",
    )(squares, count, data, *held, gains, anchor, geo)


def last_call(squares, count, data, held, gains, anchor, geo):
    return pl.pallas_call(
        last_kernel,
        in_specs=[ON_CHIP] * 10,
        out_specs=ON_CHIP,
        out_shape=jax.ShapeDtypeStruct((GAIN_ROWS, STATIONS), F32),
        scratch_shapes=[pltpu.VMEM((192, 256), F32)],
        compiler_params=GRANT,
        cost_estimate=lasts(8),
        name="normal_last",
    )(squares, count, data, *held, gains, anchor, geo)


def sent_to_all(array, axes):
    count = lax.axis_size(axes)
    return lax.all_to_all(
        jnp.broadcast_to(array[None], (count, *array.shape)), axes, 0, 0, tiled=True
    )


def cholesky_solve(gram, rhs):
    order = len(rhs)
    factor = [[None] * order for _ in range(order)]
    for i in range(order):
        for j in range(i + 1):
            value = gram[i][j]
            for m in range(j):
                value = value - factor[i][m] * factor[j][m]
            factor[i][j] = jnp.sqrt(value) if i == j else value / factor[j][j]
    forward = []
    for i in range(order):
        running = rhs[i]
        for j in range(i):
            running = running - factor[i][j] * forward[j]
        forward.append(running / factor[i][i])
    backward = [None] * order
    for i in reversed(range(order)):
        running = forward[i]
        for j in range(i + 1, order):
            running = running - factor[j][i] * backward[j]
        backward[i] = running / factor[i][i]
    return backward


def own_channels(array, axis, own):
    return lax.dynamic_slice_in_dim(array, own * FEW, FEW, axis)


def packed(vis, flags, pairs, coords):
    vis = vis.reshape(4, PARTS, FEW, LOCAL).transpose(1, 0, 2, 3).reshape(PARTS, 8, LOCAL)
    flags = flags.astype(F32).reshape(TIMES, PARTS, FEW, LOCAL).transpose(1, 0, 2, 3)
    flags = flags.reshape(PARTS, 4, LOCAL)
    coords = jnp.broadcast_to(coords.reshape(1, 4, LOCAL), (PARTS, 4, LOCAL))
    pairs = jnp.broadcast_to(pairs.astype(F32)[None], (PARTS, 2, LOCAL))
    return jnp.concatenate([vis, flags, coords, pairs], axis=1)


def body(
    visibilities,
    sample_flag_weight,
    baseline_station_pair,
    baseline_spatial_coords,
    directions,
    source_flux,
    channel_ratio,
    jones_gains,
    scaled_dual,
    consensus,
    penalty,
):
    devices = lax.axis_size(ALL)
    own = lax.axis_index(BL)
    channels = channel_ratio.shape[0]
    rho = penalty * (2.0 * BASELINES * TIMES / STATIONS)

    wide = functools.partial(
        wide_model,
        vis=visibilities,
        flags=sample_flag_weight,
        pairs=baseline_station_pair,
        coords=baseline_spatial_coords,
        directions=directions,
        flux=source_flux,
        ratio=channel_ratio,
    )
    payload = wide(jones_gains.reshape(-1, STATIONS), residual_out=False, devices=devices)
    send = packed(
        visibilities, sample_flag_weight, baseline_station_pair, baseline_spatial_coords
    )
    send = send.reshape(PARTS, ROWS * LOCAL // 128, 128)
    data = lax.all_to_all(send, BL, 0, 0, tiled=True).reshape(PARTS, ROWS, LOCAL)
    payload, data = lax.optimization_barrier((payload, data))
    arrived = lax.all_to_all(payload[:, None], ALL, 0, 0, tiled=True)[:, 0]

    ratio = own_channels(channel_ratio, 0, own)
    flux = own_channels(source_flux, 1, own)
    basis = legendre(ratio)
    sums = arrived.sum(axis=0) / lax.axis_size(BL)
    gram = [[sums[2 + i * (i + 1) // 2 + j] for j in range(i + 1)] for i in range(NPOLY)]

    def rows_of(array):
        part = own_channels(array, 2, own)
        return part.transpose(2, 0, 1, 3)

    dual = rows_of(scaled_dual)
    anchor = (
        sum(
            basis[j][:, None, None, None] * consensus[:, j][None] for j in range(NPOLY)
        )
        - dual
    ).reshape(GAIN_ROWS, STATIONS)
    gains = rows_of(jones_gains).reshape(GAIN_ROWS, STATIONS)
    geo = jnp.concatenate(
        [
            directions.T,
            flux,
            jnp.broadcast_to(ratio[None], (DIRS, FEW)),
            rho[:, None],
            jnp.zeros((DIRS, 1), F32),
        ],
        axis=1,
    )

    left, right, error, sky = first_call(data, gains, geo)
    squares = arrived
    for iteration in range(ITERS - 1):
        gains, left, right, error, misfit = middle_call(
            squares, arrived, data, (left, right, error, sky), gains, anchor, geo, devices
        )
        squares = lax.all_to_all(misfit[:, None], ALL, 0, 0, tiled=True)[:, 0]
    gains = last_call(squares, arrived, data, (left, right, error, sky), gains, anchor, geo)

    gathered = sent_to_all(gains.reshape(GAIN_ROWS * STATIONS // 128, 128), BL)
    new_gains = (
        gathered.reshape(PARTS * FEW, 2, DIRS, STATIONS).transpose(1, 2, 0, 3)
    )
    new_gains = lax.optimization_barrier(new_gains)
    residuals = wide(new_gains.reshape(-1, STATIONS), residual_out=True)

    all_basis = legendre(channel_ratio)
    lifted = new_gains + scaled_dual
    rhs = jnp.stack(
        [
            (all_basis[j][None, None, :, None] * lifted).sum(axis=2).reshape(-1, STATIONS)
            for j in range(NPOLY)
        ],
        axis=1,
    )
    rhs = lax.all_to_all(rhs, FREQ, 0, 0, tiled=True)
    rhs = rhs.sum(axis=0)
    solved = jnp.stack(cholesky_solve(gram, [rhs[j] for j in range(NPOLY)]))
    everyone = sent_to_all(solved, FREQ)
    new_consensus = everyone.reshape(2, DIRS, NPOLY, STATIONS).transpose(0, 2, 1, 3)
    fitted = sum(
        all_basis[j][None, None, :, None] * new_consensus[:, j][:, :, None, :]
        for j in range(NPOLY)
    )
    new_dual = lifted - fitted
    return (new_gains, new_consensus, new_dual, residuals)


def solution(mesh):
    split = Mesh(
        mesh.devices.reshape(4, 2, 4, 2, 2), ("bl_0", "bl_1", "freq_0", "freq_1", "freq_2")
    )
    in_specs = (
        P(None, None, FREQ, BL),
        P(None, FREQ, BL),
        P(None, BL),
        P(None, None, BL),
        P(),
        P(None, FREQ),
        P(FREQ),
        P(None, None, FREQ, None),
        P(None, None, FREQ, None),
        P(),
        P(),
    )
    out_specs = (P(None, None, FREQ, None), P(), P(None, None, FREQ, None), P(None, None, FREQ, BL))
    return jax.shard_map(body, mesh=split, in_specs=in_specs, out_specs=out_specs, check_vma=False)
```

```python
import functools

import jax
import jax.numpy as jnp
from jax import lax
from jax.experimental import pallas as pl
from jax.experimental.pallas import tpu as pltpu
from jax.sharding import Mesh
from jax.sharding import PartitionSpec as P

NPOLY = 3
ITERS = 3
BL = ("bl_0", "bl_1")
FREQ = ("freq_0", "freq_1", "freq_2")
ALL = BL + FREQ

STATIONS = 512
DIRS = 8
TIMES = 2
BASELINES = 16384
PARTS = 8
FEW = 2
LOCAL = BASELINES // PARTS
SUB = 256
MODEL_RUNS = 8
NORMAL_RUNS = 4

robust_dof = 2.0
small_term = 1e-06

SIN_TERMS = (
    3.1415926401307086,
    -5.167710083507905,
    2.5500775232148403,
    -0.5982912856219295,
    0.07765766030867731,
)
COS_TERMS = (
    0.9999999997799046,
    -4.934802137078821,
    4.058709159556128,
    -1.3352120030477381,
    0.23493731380150681,
    -0.024396324323359975,
)

F32 = jnp.float32
PER_US = 4.0e6


def lasts(microseconds):
    return pl.CostEstimate(
        flops=int(microseconds * PER_US), transcendentals=0, bytes_accessed=1 << 20
    )


BF16 = jnp.bfloat16


def legendre(ratios):
    scaled = (ratios - 1.05) / 0.35
    values = [jnp.ones_like(scaled), scaled]
    values.append((3 * scaled * values[1] - 1 * values[0]) / 2)
    return values[:NPOLY]


def horner(terms, w):
    value = jnp.full_like(w, terms[-1])
    for term in terms[-2::-1]:
        value = value * w + term
    return value


def turn_parts(turns):
    f = turns - jnp.floor(turns + 0.5)
    w = f * f
    half_sin = f * horner(SIN_TERMS, w)
    half_cos = horner(COS_TERMS, w)
    twice = half_sin + half_sin
    return 1.0 - twice * half_sin, twice * half_cos


def two_parts(value):
    high = value.astype(BF16)
    low = (value - high.astype(F32)).astype(BF16)
    return high, low


def wide_kernel(
    gains_ref,
    vis_ref,
    flag_ref,
    pair_ref,
    coord_ref,
    dirs_ref,
    flux_ref,
    ratio_ref,
    *rest,
    residual_out,
    channels,
    block,
):
    outs, rest = rest[:1], rest[1:]
    high_ref, low_ref, left_ref, right_ref, column_ref, held_ref = rest
    step = pl.program_id(0)

    @pl.when(step == 0)
    def _():
        own = lax.broadcasted_iota(jnp.int32, (channels, channels), 0)
        own = own == lax.broadcasted_iota(jnp.int32, (channels, channels), 1)
        for k in range(DIRS + 1):
            row = flux_ref[k : k + 1, :] if k < DIRS else ratio_ref[...]
            column = jnp.where(own, jnp.broadcast_to(row, (channels, channels)), 0.0)
            column_ref[k * channels : (k + 1) * channels, :] = jnp.broadcast_to(
                jnp.sum(column, axis=1, keepdims=True), (channels, 128)
            )
        high, low = two_parts(gains_ref[...])
        high_ref[...] = high
        low_ref[...] = low

    stations = lax.broadcasted_iota(jnp.int32, (STATIONS, block), 0)
    for row, target in ((0, left_ref), (1, right_ref)):
        hot = (stations == pair_ref[row : row + 1, :]).astype(F32).astype(BF16)
        target[...] = jnp.dot(high_ref[...], hot, preferred_element_type=F32) + jnp.dot(
            low_ref[...], hot, preferred_element_type=F32
        )
    ratio = column_ref[DIRS * channels :, :1]
    total = [[None, None] for _ in range(TIMES)]
    for k in range(DIRS):
        re = pl.ds(k * channels, channels)
        im = pl.ds((DIRS + k) * channels, channels)
        left_re, left_im = left_ref[re, :], left_ref[im, :]
        right_re, right_im = right_ref[re, :], right_ref[im, :]
        flux = column_ref[re, :1]
        pair_re = (left_re * right_re + left_im * right_im) * flux
        pair_im = (left_im * right_re - left_re * right_im) * flux
        for t in range(TIMES):
            project = (
                dirs_ref[0, k] * coord_ref[0, t : t + 1, :]
                + dirs_ref[1, k] * coord_ref[1, t : t + 1, :]
            )
            sky_re, sky_im = turn_parts(project * ratio)
            model_re = pair_re * sky_re - pair_im * sky_im
            model_im = pair_re * sky_im + pair_im * sky_re
            if k == 0:
                total[t] = [model_re, model_im]
            else:
                total[t] = [total[t][0] + model_re, total[t][1] + model_im]
    if residual_out:
        (residual_ref,) = outs
        for t in range(TIMES):
            residual_ref[0, t] = vis_ref[0, t] - total[t][0]
            residual_ref[1, t] = vis_ref[1, t] - total[t][1]
    else:
        (sums_ref,) = outs
        misfit = jnp.zeros((8, 128), F32)
        count = jnp.zeros((8, 128), F32)
        for t in range(TIMES):
            error_re = vis_ref[0, t] - total[t][0]
            error_im = vis_ref[1, t] - total[t][1]
            flagged = flag_ref[t].astype(F32)
            part = flagged * (error_re * error_re + error_im * error_im)
            for r in range(0, channels, 8):
                for c in range(0, block, 128):
                    misfit += part[r : r + 8, c : c + 128]
                    count += flagged[r : r + 8, c : c + 128]
        step_sums = jnp.concatenate([misfit, count], axis=0)

        @pl.when(step == 0)
        def _():
            held_ref[...] = step_sums

        @pl.when(step > 0)
        def _():
            held_ref[...] += step_sums

        @pl.when(step == pl.num_programs(0) - 1)
        def _():
            full = lambda x: jnp.sum(jnp.sum(x, axis=0, keepdims=True), axis=1, keepdims=True)
            basis = legendre(ratio_ref[...])
            entries = [full(held_ref[0:8, :]), full(held_ref[8:16, :])]
            entries += [full(basis[i] * basis[j]) for i in range(NPOLY) for j in range(i + 1)]
            lane = lax.broadcasted_iota(jnp.int32, (8, 128), 1)
            row = jnp.zeros((8, 128), F32)
            for i, entry in enumerate(entries):
                row = jnp.where(lane == i, jnp.broadcast_to(entry, (8, 128)), row)
            sums_ref[...] = jnp.broadcast_to(row[0:1], sums_ref.shape)


def wide_model(gains, vis, flags, pairs, coords, directions, flux, ratio, residual_out, devices=None):
    channels = vis.shape[2]
    count = vis.shape[3]
    block = SUB
    rows = 2 * DIRS * channels
    whole = lambda shape: pl.BlockSpec(shape, lambda i: (0,) * len(shape))
    vis_spec = pl.BlockSpec((2, TIMES, channels, block), lambda i: (0, 0, 0, i))
    if residual_out:
        out_shape = jax.ShapeDtypeStruct(vis.shape, F32)
        out_spec = vis_spec
    else:
        out_shape = jax.ShapeDtypeStruct((devices, 128), F32)
        out_spec = whole((devices, 128))
    return pl.pallas_call(
        functools.partial(
            wide_kernel, residual_out=residual_out, channels=channels, block=block
        ),
        grid=(count // block,),
        in_specs=[
            whole((rows, STATIONS)),
            vis_spec,
            pl.BlockSpec((TIMES, channels, block), lambda i: (0, 0, i)),
            pl.BlockSpec((2, block), lambda i: (0, i)),
            pl.BlockSpec((2, TIMES, block), lambda i: (0, 0, i)),
            pl.BlockSpec(memory_space=pltpu.SMEM),
            whole((DIRS, channels)),
            whole((1, channels)),
        ],
        out_specs=out_spec,
        out_shape=out_shape,
        scratch_shapes=[
            pltpu.VMEM((rows, STATIONS), BF16),
            pltpu.VMEM((rows, STATIONS), BF16),
            pltpu.VMEM((rows, block), F32),
            pltpu.VMEM((rows, block), F32),
            pltpu.VMEM(((DIRS + 1) * channels, 128), F32),
            pltpu.VMEM((16, 128), F32),
        ],
        cost_estimate=lasts(8),
        name="wide_residual" if residual_out else "wide_misfit",
    )(gains, vis, flags, pairs, coords, directions, flux, ratio.reshape(1, -1))


def swap_sum(rows):
    place = lax.broadcasted_iota(jnp.int32, rows[0].shape, 0)
    for bit in (4, 2, 1):
        mine = (place & bit) == 0
        merged = []
        for i in range(len(rows) // 2):
            a, b = rows[i], rows[i + len(rows) // 2]
            low = a + pltpu.roll(a, 8 - bit, axis=0)
            high = b + pltpu.roll(b, bit, axis=0)
            merged.append(jnp.where(mine, low, high))
        rows = merged
    return rows[0]


def one_hot(places, count):
    row = jnp.concatenate([places, places], axis=0).astype(BF16)
    lanes = places.shape[1]
    base = lax.broadcasted_iota(jnp.int32, (16, lanes), 0).astype(F32)
    one = jnp.ones((16, lanes), BF16)
    none = jnp.zeros((16, lanes), BF16)
    return jnp.concatenate(
        [jnp.where(row == (base + float(i)).astype(BF16), one, none) for i in range(0, count, 16)],
        axis=0,
    )


def model_block(part, at, data_ref, table_ref, sky_ref, outs, misfit, geo):
    left_out, right_out, error_out = outs
    lanes = pl.ds(at, SUB)
    picked = []
    for side in range(2):
        station = jnp.broadcast_to(data_ref[part, 16 + side : 17 + side, lanes], (8, SUB))
        quarter = jnp.floor(station * (1.0 / 128.0))
        hot = one_hot(station - 128.0 * quarter, 128)
        got = jnp.dot(
            table_ref[...], jnp.concatenate([hot, hot], axis=0), preferred_element_type=F32
        )
        first, second, lower = quarter == 0.0, quarter == 2.0, quarter < 2.0
        picked.append(
            jnp.concatenate(
                [
                    jnp.where(
                        lower,
                        jnp.where(first, got[i : i + 8], got[32 + i : 40 + i]),
                        jnp.where(second, got[64 + i : 72 + i], got[96 + i : 104 + i]),
                    )
                    for i in range(0, 32, 8)
                ],
                axis=0,
            )
        )
    left, right = picked
    left_out[part, :, lanes] = left
    right_out[part, :, lanes] = right
    pieces = [None] * 8
    for f in range(FEW):
        lr, li = left[16 * f : 16 * f + 8], left[16 * f + 8 : 16 * f + 16]
        rr, ri = right[16 * f : 16 * f + 8], right[16 * f + 8 : 16 * f + 16]
        pair_re = lr * rr + li * ri
        pair_im = li * rr - lr * ri
        for t in range(TIMES):
            if geo is not None:
                dirs, flux, ratio = geo
                project = dirs[0] * data_ref[part, 12 + t : 13 + t, lanes] + dirs[
                    1
                ] * data_ref[part, 14 + t : 15 + t, lanes]
                sky_re, sky_im = turn_parts(project * ratio[f])
                sky_re = sky_re * flux[f]
                sky_im = sky_im * flux[f]
                sky_ref[part, t, f, 0, :, lanes] = sky_re
                sky_ref[part, t, f, 1, :, lanes] = sky_im
            else:
                sky_re = sky_ref[part, t, f, 0, :, lanes]
                sky_im = sky_ref[part, t, f, 1, :, lanes]
            pieces[2 * t + f] = pair_re * sky_re - pair_im * sky_im
            pieces[4 + 2 * t + f] = pair_re * sky_im + pair_im * sky_re
    error = data_ref[part, 0:8, lanes] - swap_sum(pieces)
    error_out[part, :, lanes] = error
    flagged = data_ref[part, 8:12, lanes]
    return misfit + jnp.concatenate([flagged, flagged], axis=0) * (error * error)


def model_runs(data_ref, table_ref, sky_ref, outs, geo):
    steps = LOCAL // SUB // MODEL_RUNS

    def run(i, misfit):
        part, first = i // steps, (i % steps) * MODEL_RUNS
        for j in range(MODEL_RUNS):
            at = pl.multiple_of((first + j) * SUB, SUB)
            misfit = model_block(
                part, at, data_ref, table_ref, sky_ref, outs, misfit, geo
            )
        return misfit

    return lax.fori_loop(0, PARTS * steps, run, jnp.zeros((8, SUB), F32))


def build_table(table_ref, gains):
    for p, part in enumerate(two_parts(gains)):
        for q in range(4):
            table_ref[32 * q : 32 * q + 32, 128 * p : 128 * p + 128] = part[
                :, 128 * q : 128 * q + 128
            ]


def normal_block(part, at, data_ref, left_ref, right_ref, error_ref, sky_ref, inverse):
    lanes = pl.ds(at, SUB)
    error = error_ref[part, :, lanes]
    square = error * error
    square = square + pltpu.roll(square, 4, axis=0)
    flagged = data_ref[part, 8:12, lanes]
    flagged = jnp.concatenate([flagged, flagged], axis=0)
    weight = flagged * (robust_dof + 1.0) / (robust_dof + square * inverse)
    scaled = weight * error
    left = left_ref[part, :, lanes]
    right = right_ref[part, :, lanes]
    first, second = [], []
    wide = lambda row: jnp.broadcast_to(row, (DIRS, SUB))
    for f in range(FEW):
        z_re, z_im = None, None
        for t in range(TIMES):
            i = 2 * t + f
            y_re, y_im = wide(scaled[i : i + 1]), wide(scaled[4 + i : 5 + i])
            sky_re = sky_ref[part, t, f, 0, :, lanes]
            sky_im = sky_ref[part, t, f, 1, :, lanes]
            a = sky_re * y_re + sky_im * y_im
            b = sky_re * y_im - sky_im * y_re
            z_re, z_im = (a, b) if t == 0 else (z_re + a, z_im + b)
        power = wide(weight[f : f + 1] + weight[2 + f : 3 + f])
        lr, li = left[16 * f : 16 * f + 8], left[16 * f + 8 : 16 * f + 16]
        rr, ri = right[16 * f : 16 * f + 8], right[16 * f + 8 : 16 * f + 16]
        first += [rr * z_re - ri * z_im, rr * z_im + ri * z_re, (rr * rr + ri * ri) * power]
        second += [lr * z_re + li * z_im, li * z_re - lr * z_im, (lr * lr + li * li) * power]
    made = []
    for side, pieces in ((0, first), (1, second)):
        station = jnp.broadcast_to(data_ref[part, 16 + side : 17 + side, lanes], (8, SUB))
        half = jnp.where(station >= 256.0, 1.0, 0.0)
        high = jnp.concatenate([half, half], axis=0).astype(BF16)
        parts = two_parts(jnp.concatenate(pieces, axis=0))
        upper = [p[i : i + 16] * high for p in parts for i in (0, 16, 32)]
        hot = one_hot(station - 256.0 * half, 256)
        made.append((jnp.concatenate(list(parts) + upper, axis=0), hot))
    return made


def normal_runs(data_ref, left_ref, right_ref, error_ref, sky_ref, total_ref, buffers, inverse):
    steps = LOCAL // SUB // NORMAL_RUNS
    width = 2 * SUB * NORMAL_RUNS

    def fill(i, into):
        part, first = i // steps, (i % steps) * NORMAL_RUNS
        values_ref, hots_ref = into
        for j in range(NORMAL_RUNS):
            at = pl.multiple_of((first + j) * SUB, SUB)
            made = normal_block(
                part, at, data_ref, left_ref, right_ref, error_ref, sky_ref, inverse
            )
            for side in range(2):
                where = slice((2 * j + side) * SUB, (2 * j + side + 1) * SUB)
                values_ref[:, where] = made[side][0]
                hots_ref[:, where] = made[side][1]

    def add(into):
        values_ref, hots_ref = into
        return lax.dot_general(
            values_ref[...],
            hots_ref[...],
            (((1,), (1,)), ((), ())),
            preferred_element_type=F32,
        )

    fill(0, buffers[0])
    total_ref[...] = jnp.zeros_like(total_ref)

    def run(i, carry):
        one = add(buffers[0])
        fill(2 * i + 1, buffers[1])
        two = add(buffers[1])
        fill(jnp.minimum(2 * i + 2, PARTS * steps - 1), buffers[0])
        total_ref[...] += one + two
        return carry

    lax.fori_loop(0, PARTS * steps // 2, run, 0)


def renew_gains(gains, anchor, total, columns):
    both, upper = total[0:48] + total[48:96], total[96:144] + total[144:192]
    sums = jnp.concatenate([both - upper, upper], axis=1)
    rows = []
    for f in range(FEW):
        flux = columns[:, 2 + f : 3 + f]
        rho = columns[:, 6:7]
        norm = sums[24 * f + 16 : 24 * f + 24] * (flux * flux)
        divisor = norm + rho
        for c in range(2):
            g = gains[16 * f + 8 * c : 16 * f + 8 * c + 8]
            a = anchor[16 * f + 8 * c : 16 * f + 8 * c + 8]
            n = sums[24 * f + 8 * c : 24 * f + 8 * c + 8] + g * norm
            rows.append(0.5 * (g + (n + rho * a) / divisor))
    return jnp.concatenate(rows, axis=0)


def inverse_of(squares_ref, count_ref):
    squares = jnp.sum(squares_ref[...], axis=0, keepdims=True)
    count = jnp.sum(count_ref[...], axis=0, keepdims=True)
    lane = lax.broadcasted_iota(jnp.int32, (1, 128), 1)
    pick = lambda row, i: jnp.sum(jnp.where(lane == i, row, 0.0), axis=1, keepdims=True)
    return 1.0 / (pick(squares, 0) / (pick(count, 1) + 1.0) + small_term)


def renewed(
    squares_ref, count_ref, data_ref, held, gains_ref, anchor_ref, geo_ref, total_ref, buffers
):
    normal_runs(
        data_ref, *held, total_ref, buffers, inverse_of(squares_ref, count_ref)
    )
    return renew_gains(gains_ref[...], anchor_ref[...], total_ref[...], geo_ref[...])


def next_model(gains, data_ref, sky_ref, outs, misfit_out, table_ref):
    build_table(table_ref, gains)
    misfit = model_runs(data_ref, table_ref, sky_ref, outs, None)
    misfit = jnp.sum(misfit[:, :128] + misfit[:, 128:], axis=0, keepdims=True)
    misfit = jnp.sum(misfit, axis=1, keepdims=True)
    misfit_out[...] = jnp.broadcast_to(misfit, misfit_out.shape)


def first_kernel(
    data_ref, gains_ref, geo_ref, left_out, right_out, error_out, sky_out, table_ref
):
    build_table(table_ref, gains_ref[...])
    col = lambda i: geo_ref[:, i : i + 1]
    geo = ((col(0), col(1)), (col(2), col(3)), (col(4), col(5)))
    model_runs(data_ref, table_ref, sky_out, (left_out, right_out, error_out), geo)


def middle_kernel(
    squares_ref,
    count_ref,
    data_ref,
    left_ref,
    right_ref,
    error_ref,
    sky_ref,
    gains_ref,
    anchor_ref,
    geo_ref,
    gains_out,
    left_out,
    right_out,
    error_out,
    misfit_out,
    table_ref,
    total_ref,
    *flat,
):
    buffers = (flat[0:2], flat[2:4])
    held = (left_ref, right_ref, error_ref, sky_ref)
    gains = renewed(
        squares_ref, count_ref, data_ref, held, gains_ref, anchor_ref, geo_ref, total_ref, buffers
    )
    gains_out[...] = gains
    next_model(
        gains, data_ref, sky_ref, (left_out, right_out, error_out), misfit_out, table_ref
    )


def last_kernel(
    squares_ref,
    count_ref,
    data_ref,
    left_ref,
    right_ref,
    error_ref,
    sky_ref,
    gains_ref,
    anchor_ref,
    geo_ref,
    gains_out,
    total_ref,
    *flat,
):
    buffers = (flat[0:2], flat[2:4])
    held = (left_ref, right_ref, error_ref, sky_ref)
    gains = renewed(
        squares_ref, count_ref, data_ref, held, gains_ref, anchor_ref, geo_ref, total_ref, buffers
    )
    gains_out[...] = jnp.broadcast_to(gains[None], gains_out.shape)


ROWS = 18
GAIN_ROWS = 2 * FEW * DIRS
SKY = (TIMES, FEW, 2, DIRS)
GRANT = pltpu.CompilerParams(vmem_limit_bytes=8 * 1024 * 1024)
ON_CHIP = pl.BlockSpec(memory_space=pltpu.VMEM)


def shapes_of(rows):
    return jax.ShapeDtypeStruct((PARTS, rows, LOCAL), F32)


def held_shapes():
    return [
        shapes_of(GAIN_ROWS),
        shapes_of(GAIN_ROWS),
        shapes_of(8),
        jax.ShapeDtypeStruct((PARTS,) + SKY + (LOCAL,), F32),
    ]


def first_call(data, gains, geo):
    return pl.pallas_call(
        first_kernel,
        in_specs=[ON_CHIP] * 3,
        out_specs=[ON_CHIP] * 4,
        out_shape=held_shapes(),
        scratch_shapes=[pltpu.VMEM((128, 256), BF16)],
        compiler_params=GRANT,
        cost_estimate=lasts(6),
        name="first_model",
    )(data, gains, geo)


def run_buffers():
    width = 2 * SUB * NORMAL_RUNS
    return [pltpu.VMEM((192, width), BF16), pltpu.VMEM((256, width), BF16)] * 2


def middle_call(squares, count, data, held, gains, anchor, geo, devices):
    return pl.pallas_call(
        middle_kernel,
        in_specs=[ON_CHIP] * 10,
        out_specs=[ON_CHIP] * 5,
        out_shape=[
            jax.ShapeDtypeStruct((GAIN_ROWS, STATIONS), F32),
            shapes_of(GAIN_ROWS),
            shapes_of(GAIN_ROWS),
            shapes_of(8),
            jax.ShapeDtypeStruct((devices, 128), F32),
        ],
        scratch_shapes=[pltpu.VMEM((128, 256), BF16), pltpu.VMEM((192, 256), F32), *run_buffers()],
        compiler_params=GRANT,
        cost_estimate=lasts(14),
        name="normal_and_model",
    )(squares, count, data, *held, gains, anchor, geo)


def last_call(squares, count, data, held, gains, anchor, geo):
    return pl.pallas_call(
        last_kernel,
        in_specs=[ON_CHIP] * 10,
        out_specs=ON_CHIP,
        out_shape=jax.ShapeDtypeStruct((PARTS, GAIN_ROWS, STATIONS), F32),
        scratch_shapes=[pltpu.VMEM((192, 256), F32), *run_buffers()],
        compiler_params=GRANT,
        cost_estimate=lasts(8),
        name="normal_last",
    )(squares, count, data, *held, gains, anchor, geo)


def finish_kernel(solved_ref, gains_ref, dual_ref, ratio_ref, consensus_out, dual_out):
    channels = ratio_ref.shape[1]
    own = lax.broadcasted_iota(jnp.int32, (channels, channels), 0)
    own = own == lax.broadcasted_iota(jnp.int32, (channels, channels), 1)
    columns = [
        jnp.sum(
            jnp.where(own, jnp.broadcast_to(row, (channels, channels)), 0.0),
            axis=1,
            keepdims=True,
        )
        for row in legendre(ratio_ref[...])
    ]
    for c in range(2):
        for k in range(DIRS):
            g = DIRS * c + k
            rows = [solved_ref[g, j : j + 1, :] for j in range(NPOLY)]
            for j in range(NPOLY):
                consensus_out[c, j, k : k + 1, :] = rows[j]
            fitted = sum(columns[j] * rows[j] for j in range(NPOLY))
            dual_out[c, k] = dual_ref[c, k] + gains_ref[c, k] - fitted


def finish_call(solved, gains, dual, ratio):
    return pl.pallas_call(
        finish_kernel,
        in_specs=[ON_CHIP] * 4,
        out_specs=[ON_CHIP] * 2,
        out_shape=[
            jax.ShapeDtypeStruct((2, NPOLY, DIRS, STATIONS), F32),
            jax.ShapeDtypeStruct(dual.shape, F32),
        ],
        compiler_params=GRANT,
        cost_estimate=lasts(1),
        name="finish",
    )(solved, gains, dual, ratio.reshape(1, -1))


def sent_to_all(array, axes):
    count = lax.axis_size(axes)
    return lax.all_to_all(
        jnp.broadcast_to(array[None], (count, *array.shape)), axes, 0, 0, tiled=True
    )


def cholesky_solve(gram, rhs):
    order = len(rhs)
    factor = [[None] * order for _ in range(order)]
    for i in range(order):
        for j in range(i + 1):
            value = gram[i][j]
            for m in range(j):
                value = value - factor[i][m] * factor[j][m]
            factor[i][j] = jnp.sqrt(value) if i == j else value / factor[j][j]
    forward = []
    for i in range(order):
        running = rhs[i]
        for j in range(i):
            running = running - factor[i][j] * forward[j]
        forward.append(running / factor[i][i])
    backward = [None] * order
    for i in reversed(range(order)):
        running = forward[i]
        for j in range(i + 1, order):
            running = running - factor[j][i] * backward[j]
        backward[i] = running / factor[i][i]
    return backward


def own_channels(array, axis, own):
    return lax.dynamic_slice_in_dim(array, own * FEW, FEW, axis)


def packed(vis, flags, pairs, coords):
    vis = vis.reshape(4, PARTS, FEW, LOCAL).transpose(1, 0, 2, 3).reshape(PARTS, 8, LOCAL)
    flags = flags.astype(F32).reshape(TIMES, PARTS, FEW, LOCAL).transpose(1, 0, 2, 3)
    flags = flags.reshape(PARTS, 4, LOCAL)
    coords = jnp.broadcast_to(coords.reshape(1, 4, LOCAL), (PARTS, 4, LOCAL))
    pairs = jnp.broadcast_to(pairs.astype(F32)[None], (PARTS, 2, LOCAL))
    return jnp.concatenate([vis, flags, coords, pairs], axis=1)


def body(
    visibilities,
    sample_flag_weight,
    baseline_station_pair,
    baseline_spatial_coords,
    directions,
    source_flux,
    channel_ratio,
    jones_gains,
    scaled_dual,
    consensus,
    penalty,
):
    devices = lax.axis_size(ALL)
    own = lax.axis_index(BL)
    channels = channel_ratio.shape[0]
    rho = penalty * (2.0 * BASELINES * TIMES / STATIONS)

    wide = functools.partial(
        wide_model,
        vis=visibilities,
        flags=sample_flag_weight,
        pairs=baseline_station_pair,
        coords=baseline_spatial_coords,
        directions=directions,
        flux=source_flux,
        ratio=channel_ratio,
    )
    payload = wide(jones_gains.reshape(-1, STATIONS), residual_out=False, devices=devices)
    send = packed(
        visibilities, sample_flag_weight, baseline_station_pair, baseline_spatial_coords
    )
    send = send.reshape(PARTS, ROWS * LOCAL // 128, 128)
    data = lax.all_to_all(send, BL, 0, 0, tiled=True).reshape(PARTS, ROWS, LOCAL)

    ratio = own_channels(channel_ratio, 0, own)
    flux = own_channels(source_flux, 1, own)
    basis = legendre(ratio)
    def rows_of(array):
        part = own_channels(array, 2, own)
        return part.transpose(2, 0, 1, 3)

    dual = rows_of(scaled_dual)
    anchor = (
        sum(
            basis[j][:, None, None, None] * consensus[:, j][None] for j in range(NPOLY)
        )
        - dual
    ).reshape(GAIN_ROWS, STATIONS)
    gains = rows_of(jones_gains).reshape(GAIN_ROWS, STATIONS)
    geo = jnp.concatenate(
        [
            directions.T,
            flux,
            jnp.broadcast_to(ratio[None], (DIRS, FEW)),
            rho[:, None],
            jnp.zeros((DIRS, 1), F32),
        ],
        axis=1,
    )

    left, right, error, sky = first_call(data, gains, geo)
    payload, error, anchor = lax.optimization_barrier((payload, error, anchor))
    arrived = lax.all_to_all(payload[:, None], ALL, 0, 0, tiled=True)[:, 0]
    squares = arrived
    for iteration in range(ITERS - 1):
        gains, left, right, error, misfit = middle_call(
            squares, arrived, data, (left, right, error, sky), gains, anchor, geo, devices
        )
        squares = lax.all_to_all(misfit[:, None], ALL, 0, 0, tiled=True)[:, 0]
    gains = last_call(squares, arrived, data, (left, right, error, sky), gains, anchor, geo)

    gathered = lax.all_to_all(gains, BL, 0, 0, tiled=True)
    new_gains = (
        gathered.reshape(PARTS * FEW, 2, DIRS, STATIONS).transpose(1, 2, 0, 3)
    )
    new_gains = lax.optimization_barrier(new_gains)
    residuals = wide(new_gains.reshape(-1, STATIONS), residual_out=True)

    all_basis = legendre(channel_ratio)
    lifted = new_gains + scaled_dual
    rhs = jnp.stack(
        [
            (all_basis[j][None, None, :, None] * lifted).sum(axis=2).reshape(-1, STATIONS)
            for j in range(NPOLY)
        ],
        axis=1,
    )
    rhs = lax.all_to_all(rhs, FREQ, 0, 0, tiled=True)
    rhs, residuals = lax.optimization_barrier((rhs, residuals))
    rhs = rhs.sum(axis=0)
    sums = arrived.sum(axis=0) / lax.axis_size(BL)
    gram = [[sums[2 + i * (i + 1) // 2 + j] for j in range(i + 1)] for i in range(NPOLY)]
    solved = jnp.stack(cholesky_solve(gram, [rhs[j] for j in range(NPOLY)]))
    everyone = sent_to_all(solved, FREQ)
    new_consensus, new_dual = finish_call(everyone, new_gains, scaled_dual, channel_ratio)
    return (new_gains, new_consensus, new_dual, residuals)


def solution(mesh):
    split = Mesh(
        mesh.devices.reshape(4, 2, 4, 2, 2), ("bl_0", "bl_1", "freq_0", "freq_1", "freq_2")
    )
    in_specs = (
        P(None, None, FREQ, BL),
        P(None, FREQ, BL),
        P(None, BL),
        P(None, None, BL),
        P(),
        P(None, FREQ),
        P(FREQ),
        P(None, None, FREQ, None),
        P(None, None, FREQ, None),
        P(),
        P(),
    )
    out_specs = (P(None, None, FREQ, None), P(), P(None, None, FREQ, None), P(None, None, FREQ, BL))
    return jax.shard_map(body, mesh=split, in_specs=in_specs, out_specs=out_specs, check_vma=False)
```

```python
import functools

import jax
import jax.numpy as jnp
from jax import lax
from jax.experimental import pallas as pl
from jax.experimental.pallas import tpu as pltpu
from jax.sharding import Mesh
from jax.sharding import PartitionSpec as P

NPOLY = 3
ITERS = 3
BL = ("bl_0", "bl_1")
FREQ = ("freq_0", "freq_1", "freq_2")
ALL = BL + FREQ

STATIONS = 512
DIRS = 8
TIMES = 2
BASELINES = 16384
PARTS = 8
FEW = 2
LOCAL = BASELINES // PARTS
SUB = 256
MODEL_RUNS = 8
NORMAL_RUNS = 4

robust_dof = 2.0
small_term = 1e-06

SIN_TERMS = (
    3.1415926401307086,
    -5.167710083507905,
    2.5500775232148403,
    -0.5982912856219295,
    0.07765766030867731,
)
COS_TERMS = (
    0.9999999997799046,
    -4.934802137078821,
    4.058709159556128,
    -1.3352120030477381,
    0.23493731380150681,
    -0.024396324323359975,
)

F32 = jnp.float32
PER_US = 4.0e6


def lasts(microseconds):
    return pl.CostEstimate(
        flops=int(microseconds * PER_US), transcendentals=0, bytes_accessed=1 << 20
    )


BF16 = jnp.bfloat16


def legendre(ratios):
    scaled = (ratios - 1.05) / 0.35
    values = [jnp.ones_like(scaled), scaled]
    values.append((3 * scaled * values[1] - 1 * values[0]) / 2)
    return values[:NPOLY]


def horner(terms, w):
    value = jnp.full_like(w, terms[-1])
    for term in terms[-2::-1]:
        value = value * w + term
    return value


def turn_parts(turns):
    f = turns - jnp.floor(turns + 0.5)
    w = f * f
    half_sin = f * horner(SIN_TERMS, w)
    half_cos = horner(COS_TERMS, w)
    twice = half_sin + half_sin
    return 1.0 - twice * half_sin, twice * half_cos


def two_parts(value):
    high = value.astype(BF16)
    low = (value - high.astype(F32)).astype(BF16)
    return high, low


def wide_kernel(
    gains_ref,
    vis_ref,
    flag_ref,
    pair_ref,
    coord_ref,
    dirs_ref,
    flux_ref,
    ratio_ref,
    *rest,
    residual_out,
    channels,
    block,
):
    outs, rest = rest[:1], rest[1:]
    high_ref, low_ref, left_ref, right_ref, column_ref, held_ref = rest
    step = pl.program_id(0)

    @pl.when(step == 0)
    def _():
        own = lax.broadcasted_iota(jnp.int32, (channels, channels), 0)
        own = own == lax.broadcasted_iota(jnp.int32, (channels, channels), 1)
        for k in range(DIRS + 1):
            row = flux_ref[k : k + 1, :] if k < DIRS else ratio_ref[...]
            column = jnp.where(own, jnp.broadcast_to(row, (channels, channels)), 0.0)
            column_ref[k * channels : (k + 1) * channels, :] = jnp.broadcast_to(
                jnp.sum(column, axis=1, keepdims=True), (channels, 128)
            )
        high, low = two_parts(gains_ref[...])
        high_ref[...] = high
        low_ref[...] = low

    stations = lax.broadcasted_iota(jnp.int32, (STATIONS, block), 0)
    for row, target in ((0, left_ref), (1, right_ref)):
        hot = (stations == pair_ref[row : row + 1, :]).astype(F32).astype(BF16)
        target[...] = jnp.dot(high_ref[...], hot, preferred_element_type=F32) + jnp.dot(
            low_ref[...], hot, preferred_element_type=F32
        )
    ratio = column_ref[DIRS * channels :, :1]
    total = [[None, None] for _ in range(TIMES)]
    for k in range(DIRS):
        re = pl.ds(k * channels, channels)
        im = pl.ds((DIRS + k) * channels, channels)
        left_re, left_im = left_ref[re, :], left_ref[im, :]
        right_re, right_im = right_ref[re, :], right_ref[im, :]
        flux = column_ref[re, :1]
        pair_re = (left_re * right_re + left_im * right_im) * flux
        pair_im = (left_im * right_re - left_re * right_im) * flux
        for t in range(TIMES):
            project = (
                dirs_ref[0, k] * coord_ref[0, t : t + 1, :]
                + dirs_ref[1, k] * coord_ref[1, t : t + 1, :]
            )
            sky_re, sky_im = turn_parts(project * ratio)
            model_re = pair_re * sky_re - pair_im * sky_im
            model_im = pair_re * sky_im + pair_im * sky_re
            if k == 0:
                total[t] = [model_re, model_im]
            else:
                total[t] = [total[t][0] + model_re, total[t][1] + model_im]
    if residual_out:
        (residual_ref,) = outs
        for t in range(TIMES):
            residual_ref[0, t] = vis_ref[0, t] - total[t][0]
            residual_ref[1, t] = vis_ref[1, t] - total[t][1]
    else:
        (sums_ref,) = outs
        misfit = jnp.zeros((8, 128), F32)
        count = jnp.zeros((8, 128), F32)
        for t in range(TIMES):
            error_re = vis_ref[0, t] - total[t][0]
            error_im = vis_ref[1, t] - total[t][1]
            flagged = flag_ref[t].astype(F32)
            part = flagged * (error_re * error_re + error_im * error_im)
            for r in range(0, channels, 8):
                for c in range(0, block, 128):
                    misfit += part[r : r + 8, c : c + 128]
                    count += flagged[r : r + 8, c : c + 128]
        step_sums = jnp.concatenate([misfit, count], axis=0)

        @pl.when(step == 0)
        def _():
            held_ref[...] = step_sums

        @pl.when(step > 0)
        def _():
            held_ref[...] += step_sums

        @pl.when(step == pl.num_programs(0) - 1)
        def _():
            full = lambda x: jnp.sum(jnp.sum(x, axis=0, keepdims=True), axis=1, keepdims=True)
            basis = legendre(ratio_ref[...])
            entries = [full(held_ref[0:8, :]), full(held_ref[8:16, :])]
            entries += [full(basis[i] * basis[j]) for i in range(NPOLY) for j in range(i + 1)]
            lane = lax.broadcasted_iota(jnp.int32, (8, 128), 1)
            row = jnp.zeros((8, 128), F32)
            for i, entry in enumerate(entries):
                row = jnp.where(lane == i, jnp.broadcast_to(entry, (8, 128)), row)
            sums_ref[...] = jnp.broadcast_to(row[0:1], sums_ref.shape)


def wide_model(gains, vis, flags, pairs, coords, directions, flux, ratio, residual_out, devices=None):
    channels = vis.shape[2]
    count = vis.shape[3]
    block = SUB
    rows = 2 * DIRS * channels
    whole = lambda shape: pl.BlockSpec(shape, lambda i: (0,) * len(shape))
    vis_spec = pl.BlockSpec((2, TIMES, channels, block), lambda i: (0, 0, 0, i))
    if residual_out:
        out_shape = jax.ShapeDtypeStruct(vis.shape, F32)
        out_spec = vis_spec
    else:
        out_shape = jax.ShapeDtypeStruct((devices, 128), F32)
        out_spec = whole((devices, 128))
    return pl.pallas_call(
        functools.partial(
            wide_kernel, residual_out=residual_out, channels=channels, block=block
        ),
        grid=(count // block,),
        in_specs=[
            whole((rows, STATIONS)),
            vis_spec,
            pl.BlockSpec((TIMES, channels, block), lambda i: (0, 0, i)),
            pl.BlockSpec((2, block), lambda i: (0, i)),
            pl.BlockSpec((2, TIMES, block), lambda i: (0, 0, i)),
            pl.BlockSpec(memory_space=pltpu.SMEM),
            whole((DIRS, channels)),
            whole((1, channels)),
        ],
        out_specs=out_spec,
        out_shape=out_shape,
        scratch_shapes=[
            pltpu.VMEM((rows, STATIONS), BF16),
            pltpu.VMEM((rows, STATIONS), BF16),
            pltpu.VMEM((rows, block), F32),
            pltpu.VMEM((rows, block), F32),
            pltpu.VMEM(((DIRS + 1) * channels, 128), F32),
            pltpu.VMEM((16, 128), F32),
        ],
        cost_estimate=lasts(8),
        name="wide_residual" if residual_out else "wide_misfit",
    )(gains, vis, flags, pairs, coords, directions, flux, ratio.reshape(1, -1))


def swap_sum(rows):
    place = lax.broadcasted_iota(jnp.int32, rows[0].shape, 0)
    for bit in (4, 2, 1):
        mine = (place & bit) == 0
        merged = []
        for i in range(len(rows) // 2):
            a, b = rows[i], rows[i + len(rows) // 2]
            low = a + pltpu.roll(a, 8 - bit, axis=0)
            high = b + pltpu.roll(b, bit, axis=0)
            merged.append(jnp.where(mine, low, high))
        rows = merged
    return rows[0]


def one_hot(places, count):
    row = jnp.concatenate([places, places], axis=0).astype(BF16)
    lanes = places.shape[1]
    base = lax.broadcasted_iota(jnp.int32, (16, lanes), 0).astype(F32)
    one = jnp.ones((16, lanes), BF16)
    none = jnp.zeros((16, lanes), BF16)
    return jnp.concatenate(
        [jnp.where(row == (base + float(i)).astype(BF16), one, none) for i in range(0, count, 16)],
        axis=0,
    )


def model_block(part, at, data_ref, table_ref, sky_ref, outs, misfit, geo):
    left_out, right_out, error_out = outs
    lanes = pl.ds(at, SUB)
    picked = []
    for side in range(2):
        station = jnp.broadcast_to(data_ref[part, 16 + side : 17 + side, lanes], (8, SUB))
        quarter = jnp.floor(station * (1.0 / 128.0))
        hot = one_hot(station - 128.0 * quarter, 128)
        got = jnp.dot(
            table_ref[...], jnp.concatenate([hot, hot], axis=0), preferred_element_type=F32
        )
        first, second, lower = quarter == 0.0, quarter == 2.0, quarter < 2.0
        picked.append(
            jnp.concatenate(
                [
                    jnp.where(
                        lower,
                        jnp.where(first, got[i : i + 8], got[32 + i : 40 + i]),
                        jnp.where(second, got[64 + i : 72 + i], got[96 + i : 104 + i]),
                    )
                    for i in range(0, 32, 8)
                ],
                axis=0,
            )
        )
    left, right = picked
    left_out[part, :, lanes] = left
    right_out[part, :, lanes] = right
    pieces = [None] * 8
    for f in range(FEW):
        lr, li = left[16 * f : 16 * f + 8], left[16 * f + 8 : 16 * f + 16]
        rr, ri = right[16 * f : 16 * f + 8], right[16 * f + 8 : 16 * f + 16]
        pair_re = lr * rr + li * ri
        pair_im = li * rr - lr * ri
        for t in range(TIMES):
            if geo is not None:
                dirs, flux, ratio = geo
                project = dirs[0] * data_ref[part, 12 + t : 13 + t, lanes] + dirs[
                    1
                ] * data_ref[part, 14 + t : 15 + t, lanes]
                sky_re, sky_im = turn_parts(project * ratio[f])
                sky_re = sky_re * flux[f]
                sky_im = sky_im * flux[f]
                sky_ref[part, t, f, 0, :, lanes] = sky_re
                sky_ref[part, t, f, 1, :, lanes] = sky_im
            else:
                sky_re = sky_ref[part, t, f, 0, :, lanes]
                sky_im = sky_ref[part, t, f, 1, :, lanes]
            pieces[2 * t + f] = pair_re * sky_re - pair_im * sky_im
            pieces[4 + 2 * t + f] = pair_re * sky_im + pair_im * sky_re
    error = data_ref[part, 0:8, lanes] - swap_sum(pieces)
    error_out[part, :, lanes] = error
    flagged = data_ref[part, 8:12, lanes]
    return misfit + jnp.concatenate([flagged, flagged], axis=0) * (error * error)


def model_runs(data_ref, table_ref, sky_ref, outs, geo):
    steps = LOCAL // SUB // MODEL_RUNS

    def run(i, misfit):
        part, first = i // steps, (i % steps) * MODEL_RUNS
        for j in range(MODEL_RUNS):
            at = pl.multiple_of((first + j) * SUB, SUB)
            misfit = model_block(
                part, at, data_ref, table_ref, sky_ref, outs, misfit, geo
            )
        return misfit

    return lax.fori_loop(0, PARTS * steps, run, jnp.zeros((8, SUB), F32))


def build_table(table_ref, gains):
    for p, part in enumerate(two_parts(gains)):
        for q in range(4):
            table_ref[32 * q : 32 * q + 32, 128 * p : 128 * p + 128] = part[
                :, 128 * q : 128 * q + 128
            ]


def normal_block(part, at, data_ref, left_ref, right_ref, error_ref, sky_ref, inverse):
    lanes = pl.ds(at, SUB)
    error = error_ref[part, :, lanes]
    square = error * error
    square = square + pltpu.roll(square, 4, axis=0)
    flagged = data_ref[part, 8:12, lanes]
    flagged = jnp.concatenate([flagged, flagged], axis=0)
    weight = flagged * (robust_dof + 1.0) / (robust_dof + square * inverse)
    scaled = weight * error
    left = left_ref[part, :, lanes]
    right = right_ref[part, :, lanes]
    first, second = [], []
    wide = lambda row: jnp.broadcast_to(row, (DIRS, SUB))
    for f in range(FEW):
        z_re, z_im = None, None
        for t in range(TIMES):
            i = 2 * t + f
            y_re, y_im = wide(scaled[i : i + 1]), wide(scaled[4 + i : 5 + i])
            sky_re = sky_ref[part, t, f, 0, :, lanes]
            sky_im = sky_ref[part, t, f, 1, :, lanes]
            a = sky_re * y_re + sky_im * y_im
            b = sky_re * y_im - sky_im * y_re
            z_re, z_im = (a, b) if t == 0 else (z_re + a, z_im + b)
        power = wide(weight[f : f + 1] + weight[2 + f : 3 + f])
        lr, li = left[16 * f : 16 * f + 8], left[16 * f + 8 : 16 * f + 16]
        rr, ri = right[16 * f : 16 * f + 8], right[16 * f + 8 : 16 * f + 16]
        first += [rr * z_re - ri * z_im, rr * z_im + ri * z_re, (rr * rr + ri * ri) * power]
        second += [lr * z_re + li * z_im, li * z_re - lr * z_im, (lr * lr + li * li) * power]
    made = []
    for side, pieces in ((0, first), (1, second)):
        station = jnp.broadcast_to(data_ref[part, 16 + side : 17 + side, lanes], (8, SUB))
        half = jnp.where(station >= 256.0, 1.0, 0.0)
        high = jnp.concatenate([half, half], axis=0).astype(BF16)
        parts = two_parts(jnp.concatenate(pieces, axis=0))
        upper = [p[i : i + 16] * high for p in parts for i in (0, 16, 32)]
        hot = one_hot(station - 256.0 * half, 256)
        made.append((jnp.concatenate(list(parts) + upper, axis=0), hot))
    return made


def normal_runs(data_ref, left_ref, right_ref, error_ref, sky_ref, total_ref, buffers, inverse):
    steps = LOCAL // SUB // NORMAL_RUNS
    width = 2 * SUB * NORMAL_RUNS

    def fill(i, into):
        part, first = i // steps, (i % steps) * NORMAL_RUNS
        values_ref, hots_ref = into
        for j in range(NORMAL_RUNS):
            at = pl.multiple_of((first + j) * SUB, SUB)
            made = normal_block(
                part, at, data_ref, left_ref, right_ref, error_ref, sky_ref, inverse
            )
            for side in range(2):
                where = slice((2 * j + side) * SUB, (2 * j + side + 1) * SUB)
                values_ref[:, where] = made[side][0]
                hots_ref[:, where] = made[side][1]

    def add(into):
        values_ref, hots_ref = into
        return lax.dot_general(
            values_ref[...],
            hots_ref[...],
            (((1,), (1,)), ((), ())),
            preferred_element_type=F32,
        )

    fill(0, buffers[0])
    total_ref[...] = jnp.zeros_like(total_ref)

    def run(i, carry):
        one = add(buffers[0])
        fill(2 * i + 1, buffers[1])
        two = add(buffers[1])
        fill(jnp.minimum(2 * i + 2, PARTS * steps - 1), buffers[0])
        total_ref[...] += one + two
        return carry

    lax.fori_loop(0, PARTS * steps // 2, run, 0)


def renew_gains(gains, anchor, total, columns):
    both, upper = total[0:48] + total[48:96], total[96:144] + total[144:192]
    sums = jnp.concatenate([both - upper, upper], axis=1)
    rows = []
    for f in range(FEW):
        flux = columns[:, 2 + f : 3 + f]
        rho = columns[:, 6:7]
        norm = sums[24 * f + 16 : 24 * f + 24] * (flux * flux)
        divisor = norm + rho
        for c in range(2):
            g = gains[16 * f + 8 * c : 16 * f + 8 * c + 8]
            a = anchor[16 * f + 8 * c : 16 * f + 8 * c + 8]
            n = sums[24 * f + 8 * c : 24 * f + 8 * c + 8] + g * norm
            rows.append(0.5 * (g + (n + rho * a) / divisor))
    return jnp.concatenate(rows, axis=0)


def inverse_of(squares_ref, count_ref):
    squares = jnp.sum(squares_ref[...], axis=0, keepdims=True)
    count = jnp.sum(count_ref[...], axis=0, keepdims=True)
    lane = lax.broadcasted_iota(jnp.int32, (1, 128), 1)
    pick = lambda row, i: jnp.sum(jnp.where(lane == i, row, 0.0), axis=1, keepdims=True)
    return 1.0 / (pick(squares, 0) / (pick(count, 1) + 1.0) + small_term)


def renewed(
    squares_ref, count_ref, data_ref, held, gains_ref, anchor_ref, geo_ref, total_ref, buffers
):
    normal_runs(
        data_ref, *held, total_ref, buffers, inverse_of(squares_ref, count_ref)
    )
    return renew_gains(gains_ref[...], anchor_ref[...], total_ref[...], geo_ref[...])


def next_model(gains, data_ref, sky_ref, outs, misfit_out, table_ref):
    build_table(table_ref, gains)
    misfit = model_runs(data_ref, table_ref, sky_ref, outs, None)
    misfit = jnp.sum(misfit[:, :128] + misfit[:, 128:], axis=0, keepdims=True)
    misfit = jnp.sum(misfit, axis=1, keepdims=True)
    misfit_out[...] = jnp.broadcast_to(misfit, misfit_out.shape)


def first_kernel(
    data_ref, gains_ref, geo_ref, left_out, right_out, error_out, sky_out, table_ref
):
    build_table(table_ref, gains_ref[...])
    col = lambda i: geo_ref[:, i : i + 1]
    geo = ((col(0), col(1)), (col(2), col(3)), (col(4), col(5)))
    model_runs(data_ref, table_ref, sky_out, (left_out, right_out, error_out), geo)


def middle_kernel(
    squares_ref,
    count_ref,
    data_ref,
    left_ref,
    right_ref,
    error_ref,
    sky_ref,
    gains_ref,
    anchor_ref,
    geo_ref,
    gains_out,
    left_out,
    right_out,
    error_out,
    misfit_out,
    table_ref,
    total_ref,
    *flat,
):
    buffers = (flat[0:2], flat[2:4])
    held = (left_ref, right_ref, error_ref, sky_ref)
    gains = renewed(
        squares_ref, count_ref, data_ref, held, gains_ref, anchor_ref, geo_ref, total_ref, buffers
    )
    gains_out[...] = gains
    next_model(
        gains, data_ref, sky_ref, (left_out, right_out, error_out), misfit_out, table_ref
    )


def last_kernel(
    squares_ref,
    count_ref,
    data_ref,
    left_ref,
    right_ref,
    error_ref,
    sky_ref,
    gains_ref,
    anchor_ref,
    geo_ref,
    gains_out,
    total_ref,
    *flat,
):
    buffers = (flat[0:2], flat[2:4])
    held = (left_ref, right_ref, error_ref, sky_ref)
    gains = renewed(
        squares_ref, count_ref, data_ref, held, gains_ref, anchor_ref, geo_ref, total_ref, buffers
    )
    gains_out[...] = jnp.broadcast_to(gains[None], gains_out.shape)


ROWS = 18
GAIN_ROWS = 2 * FEW * DIRS
SKY = (TIMES, FEW, 2, DIRS)
GRANT = pltpu.CompilerParams(vmem_limit_bytes=8 * 1024 * 1024)
ON_CHIP = pl.BlockSpec(memory_space=pltpu.VMEM)


def shapes_of(rows):
    return jax.ShapeDtypeStruct((PARTS, rows, LOCAL), F32)


def held_shapes():
    return [
        shapes_of(GAIN_ROWS),
        shapes_of(GAIN_ROWS),
        shapes_of(8),
        jax.ShapeDtypeStruct((PARTS,) + SKY + (LOCAL,), F32),
    ]


def first_call(data, gains, geo):
    return pl.pallas_call(
        first_kernel,
        in_specs=[ON_CHIP] * 3,
        out_specs=[ON_CHIP] * 4,
        out_shape=held_shapes(),
        scratch_shapes=[pltpu.VMEM((128, 256), BF16)],
        compiler_params=GRANT,
        cost_estimate=lasts(6),
        name="first_model",
    )(data, gains, geo)


def run_buffers():
    width = 2 * SUB * NORMAL_RUNS
    return [pltpu.VMEM((192, width), BF16), pltpu.VMEM((256, width), BF16)] * 2


def middle_call(squares, count, data, held, gains, anchor, geo, devices):
    return pl.pallas_call(
        middle_kernel,
        in_specs=[ON_CHIP] * 10,
        out_specs=[ON_CHIP] * 5,
        out_shape=[
            jax.ShapeDtypeStruct((GAIN_ROWS, STATIONS), F32),
            shapes_of(GAIN_ROWS),
            shapes_of(GAIN_ROWS),
            shapes_of(8),
            jax.ShapeDtypeStruct((devices, 128), F32),
        ],
        scratch_shapes=[pltpu.VMEM((128, 256), BF16), pltpu.VMEM((192, 256), F32), *run_buffers()],
        compiler_params=GRANT,
        cost_estimate=lasts(14),
        name="normal_and_model",
    )(squares, count, data, *held, gains, anchor, geo)


def last_call(squares, count, data, held, gains, anchor, geo):
    return pl.pallas_call(
        last_kernel,
        in_specs=[ON_CHIP] * 10,
        out_specs=ON_CHIP,
        out_shape=jax.ShapeDtypeStruct((PARTS, GAIN_ROWS, STATIONS), F32),
        scratch_shapes=[pltpu.VMEM((192, 256), F32), *run_buffers()],
        compiler_params=GRANT,
        cost_estimate=lasts(8),
        name="normal_last",
    )(squares, count, data, *held, gains, anchor, geo)


def cholesky_solve(gram, rhs):
    order = len(rhs)
    factor = [[None] * order for _ in range(order)]
    for i in range(order):
        for j in range(i + 1):
            value = gram[i][j]
            for m in range(j):
                value = value - factor[i][m] * factor[j][m]
            factor[i][j] = jnp.sqrt(value) if i == j else value / factor[j][j]
    forward = []
    for i in range(order):
        running = rhs[i]
        for j in range(i):
            running = running - factor[i][j] * forward[j]
        forward.append(running / factor[i][i])
    backward = [None] * order
    for i in reversed(range(order)):
        running = forward[i]
        for j in range(i + 1, order):
            running = running - factor[j][i] * backward[j]
        backward[i] = running / factor[i][i]
    return backward


def consensus_kernel(rhs_ref, arrived_ref, out_ref, *, copies):
    rhs = rhs_ref[0]
    for i in range(1, rhs_ref.shape[0]):
        rhs = rhs + rhs_ref[i]
    sums = jnp.sum(arrived_ref[...], axis=0, keepdims=True) * (1.0 / copies)
    lane = lax.broadcasted_iota(jnp.int32, (1, 128), 1)
    pick = lambda i: jnp.sum(jnp.where(lane == i, sums, 0.0), axis=1, keepdims=True)
    gram = [[pick(2 + i * (i + 1) // 2 + j) for j in range(i + 1)] for i in range(NPOLY)]
    solved = cholesky_solve(gram, [rhs[j : j + 1] for j in range(NPOLY)])
    out_ref[...] = jnp.broadcast_to(jnp.concatenate(solved, axis=0)[None], out_ref.shape)


def consensus_call(rhs, arrived, copies):
    return pl.pallas_call(
        functools.partial(consensus_kernel, copies=copies),
        in_specs=[ON_CHIP] * 2,
        out_specs=ON_CHIP,
        out_shape=jax.ShapeDtypeStruct(rhs.shape, F32),
        compiler_params=GRANT,
        cost_estimate=lasts(1),
        name="consensus",
    )(rhs, arrived)


def finish_kernel(solved_ref, gains_ref, dual_ref, ratio_ref, consensus_out, dual_out):
    channels = ratio_ref.shape[1]
    own = lax.broadcasted_iota(jnp.int32, (channels, channels), 0)
    own = own == lax.broadcasted_iota(jnp.int32, (channels, channels), 1)
    columns = [
        jnp.sum(
            jnp.where(own, jnp.broadcast_to(row, (channels, channels)), 0.0),
            axis=1,
            keepdims=True,
        )
        for row in legendre(ratio_ref[...])
    ]
    for k in range(DIRS):
        rows = [solved_ref[k, j : j + 1, :] for j in range(NPOLY)]
        for j in range(NPOLY):
            consensus_out[0, j, k : k + 1, :] = rows[j]
        fitted = sum(columns[j] * rows[j] for j in range(NPOLY))
        dual_out[0, k] = dual_ref[0, k] + gains_ref[0, k] - fitted


def finish_call(solved, gains, dual, ratio):
    channels = ratio.shape[0]
    big = pl.BlockSpec((1, DIRS, channels, STATIONS), lambda c: (c, 0, 0, 0))
    return pl.pallas_call(
        finish_kernel,
        grid=(2,),
        in_specs=[
            pl.BlockSpec((DIRS, NPOLY, STATIONS), lambda c: (c, 0, 0)),
            big,
            big,
            pl.BlockSpec((1, channels), lambda c: (0, 0)),
        ],
        out_specs=[pl.BlockSpec((1, NPOLY, DIRS, STATIONS), lambda c: (c, 0, 0, 0)), big],
        out_shape=[
            jax.ShapeDtypeStruct((2, NPOLY, DIRS, STATIONS), F32),
            jax.ShapeDtypeStruct(dual.shape, F32),
        ],
        cost_estimate=lasts(1),
        name="finish",
    )(solved, gains, dual, ratio.reshape(1, -1))


def own_channels(array, axis, own):
    return lax.dynamic_slice_in_dim(array, own * FEW, FEW, axis)


def pack_kernel(vis_ref, flag_ref, pair_ref, coord_ref, out_ref):
    def run(j, carry):
        lanes = pl.ds(pl.multiple_of(j * 128, 128), 128)
        to = pl.ds(j, 1)
        for c in range(2):
            for t in range(TIMES):
                rows = vis_ref[c, t, :, lanes]
                for f in range(PARTS * FEW):
                    out_ref[f // FEW, (2 * c + t) * FEW + f % FEW, to, :] = rows[f : f + 1]
                rows = coord_ref[c, t : t + 1, lanes]
                for d in range(PARTS):
                    out_ref[d, 12 + 2 * c + t, to, :] = rows
        for t in range(TIMES):
            rows = flag_ref[t, :, lanes].astype(F32)
            for f in range(PARTS * FEW):
                out_ref[f // FEW, 8 + t * FEW + f % FEW, to, :] = rows[f : f + 1]
        for side in range(2):
            rows = pair_ref[side : side + 1, lanes].astype(F32)
            for d in range(PARTS):
                out_ref[d, 16 + side, to, :] = rows
        return carry

    lax.fori_loop(0, out_ref.shape[2], run, 0)


def packed(vis, flags, pairs, coords):
    half = LOCAL // 2
    channels = vis.shape[2]
    return pl.pallas_call(
        pack_kernel,
        grid=(2,),
        in_specs=[
            pl.BlockSpec((2, TIMES, channels, half), lambda i: (0, 0, 0, i)),
            pl.BlockSpec((TIMES, channels, half), lambda i: (0, 0, i)),
            pl.BlockSpec((2, half), lambda i: (0, i)),
            pl.BlockSpec((2, TIMES, half), lambda i: (0, 0, i)),
        ],
        out_specs=pl.BlockSpec((PARTS, ROWS, half // 128, 128), lambda i: (0, 0, i, 0)),
        out_shape=jax.ShapeDtypeStruct((PARTS, ROWS, LOCAL // 128, 128), F32),
        cost_estimate=lasts(2),
        name="pack",
    )(vis, flags, pairs, coords)


def body(
    visibilities,
    sample_flag_weight,
    baseline_station_pair,
    baseline_spatial_coords,
    directions,
    source_flux,
    channel_ratio,
    jones_gains,
    scaled_dual,
    consensus,
    penalty,
):
    devices = lax.axis_size(ALL)
    own = lax.axis_index(BL)
    channels = channel_ratio.shape[0]
    rho = penalty * (2.0 * BASELINES * TIMES / STATIONS)

    wide = functools.partial(
        wide_model,
        vis=visibilities,
        flags=sample_flag_weight,
        pairs=baseline_station_pair,
        coords=baseline_spatial_coords,
        directions=directions,
        flux=source_flux,
        ratio=channel_ratio,
    )
    payload = wide(jones_gains.reshape(-1, STATIONS), residual_out=False, devices=devices)
    send = packed(
        visibilities, sample_flag_weight, baseline_station_pair, baseline_spatial_coords
    )
    send = send.reshape(PARTS, ROWS * LOCAL // 128, 128)
    data = lax.all_to_all(send, BL, 0, 0, tiled=True).reshape(PARTS, ROWS, LOCAL)

    ratio = own_channels(channel_ratio, 0, own)
    flux = own_channels(source_flux, 1, own)
    basis = legendre(ratio)
    def rows_of(array):
        part = own_channels(array, 2, own)
        return part.transpose(2, 0, 1, 3)

    dual = rows_of(scaled_dual)
    anchor = (
        sum(
            basis[j][:, None, None, None] * consensus[:, j][None] for j in range(NPOLY)
        )
        - dual
    ).reshape(GAIN_ROWS, STATIONS)
    gains = rows_of(jones_gains).reshape(GAIN_ROWS, STATIONS)
    geo = jnp.concatenate(
        [
            directions.T,
            flux,
            jnp.broadcast_to(ratio[None], (DIRS, FEW)),
            rho[:, None],
            jnp.zeros((DIRS, 1), F32),
        ],
        axis=1,
    )

    left, right, error, sky = first_call(data, gains, geo)
    payload, error, anchor = lax.optimization_barrier((payload, error, anchor))
    arrived = lax.all_to_all(payload[:, None], ALL, 0, 0, tiled=True)[:, 0]
    squares = arrived
    for iteration in range(ITERS - 1):
        gains, left, right, error, misfit = middle_call(
            squares, arrived, data, (left, right, error, sky), gains, anchor, geo, devices
        )
        squares = lax.all_to_all(misfit[:, None], ALL, 0, 0, tiled=True)[:, 0]
    gains = last_call(squares, arrived, data, (left, right, error, sky), gains, anchor, geo)

    gathered = lax.all_to_all(gains, BL, 0, 0, tiled=True)
    new_gains = (
        gathered.reshape(PARTS * FEW, 2, DIRS, STATIONS).transpose(1, 2, 0, 3)
    )
    new_gains = lax.optimization_barrier(new_gains)
    residuals = wide(new_gains.reshape(-1, STATIONS), residual_out=True)

    all_basis = legendre(channel_ratio)
    lifted = new_gains + scaled_dual
    rhs = jnp.stack(
        [
            (all_basis[j][None, None, :, None] * lifted).sum(axis=2).reshape(-1, STATIONS)
            for j in range(NPOLY)
        ],
        axis=1,
    )
    rhs = lax.all_to_all(rhs, FREQ, 0, 0, tiled=True)
    rhs, residuals = lax.optimization_barrier((rhs, residuals))
    solved = consensus_call(rhs, arrived, lax.axis_size(BL))
    everyone = lax.all_to_all(solved, FREQ, 0, 0, tiled=True)
    new_consensus, new_dual = finish_call(everyone, new_gains, scaled_dual, channel_ratio)
    return (new_gains, new_consensus, new_dual, residuals)


def solution(mesh):
    split = Mesh(
        mesh.devices.reshape(4, 2, 4, 2, 2), ("bl_0", "bl_1", "freq_0", "freq_1", "freq_2")
    )
    in_specs = (
        P(None, None, FREQ, BL),
        P(None, FREQ, BL),
        P(None, BL),
        P(None, None, BL),
        P(),
        P(None, FREQ),
        P(FREQ),
        P(None, None, FREQ, None),
        P(None, None, FREQ, None),
        P(),
        P(),
    )
    out_specs = (P(None, None, FREQ, None), P(), P(None, None, FREQ, None), P(None, None, FREQ, BL))
    return jax.shard_map(body, mesh=split, in_specs=in_specs, out_specs=out_specs, check_vma=False)
```

```python
import functools

import jax
import jax.numpy as jnp
from jax import lax
from jax.experimental import pallas as pl
from jax.experimental.pallas import tpu as pltpu
from jax.sharding import Mesh
from jax.sharding import PartitionSpec as P

NPOLY = 3
ITERS = 3
BL = ("bl_0", "bl_1")
FREQ = ("freq_0", "freq_1", "freq_2")
ALL = BL + FREQ

STATIONS = 512
DIRS = 8
TIMES = 2
BASELINES = 16384
PARTS = 8
FEW = 2
LOCAL = BASELINES // PARTS
SUB = 256
MODEL_RUNS = 8
NORMAL_RUNS = 8

robust_dof = 2.0
small_term = 1e-06

SIN_TERMS = (
    3.1415926401307086,
    -5.167710083507905,
    2.5500775232148403,
    -0.5982912856219295,
    0.07765766030867731,
)
COS_TERMS = (
    0.9999999997799046,
    -4.934802137078821,
    4.058709159556128,
    -1.3352120030477381,
    0.23493731380150681,
    -0.024396324323359975,
)

F32 = jnp.float32
PER_US = 4.0e6


def lasts(microseconds):
    return pl.CostEstimate(
        flops=int(microseconds * PER_US), transcendentals=0, bytes_accessed=1 << 20
    )


BF16 = jnp.bfloat16


def legendre(ratios):
    scaled = (ratios - 1.05) / 0.35
    values = [jnp.ones_like(scaled), scaled]
    values.append((3 * scaled * values[1] - 1 * values[0]) / 2)
    return values[:NPOLY]


def horner(terms, w):
    value = jnp.full_like(w, terms[-1])
    for term in terms[-2::-1]:
        value = value * w + term
    return value


def turn_parts(turns):
    f = turns - jnp.floor(turns + 0.5)
    w = f * f
    half_sin = f * horner(SIN_TERMS, w)
    half_cos = horner(COS_TERMS, w)
    twice = half_sin + half_sin
    return 1.0 - twice * half_sin, twice * half_cos


def two_parts(value):
    high = value.astype(BF16)
    low = (value - high.astype(F32)).astype(BF16)
    return high, low


def wide_kernel(
    gains_ref,
    vis_ref,
    flag_ref,
    pair_ref,
    coord_ref,
    dirs_ref,
    flux_ref,
    ratio_ref,
    *rest,
    residual_out,
    channels,
    block,
):
    outs, rest = rest[:1], rest[1:]
    high_ref, low_ref, left_ref, right_ref, column_ref, held_ref = rest
    step = pl.program_id(0)

    @pl.when(step == 0)
    def _():
        own = lax.broadcasted_iota(jnp.int32, (channels, channels), 0)
        own = own == lax.broadcasted_iota(jnp.int32, (channels, channels), 1)
        for k in range(DIRS + 1):
            row = flux_ref[k : k + 1, :] if k < DIRS else ratio_ref[...]
            column = jnp.where(own, jnp.broadcast_to(row, (channels, channels)), 0.0)
            column_ref[k * channels : (k + 1) * channels, :] = jnp.broadcast_to(
                jnp.sum(column, axis=1, keepdims=True), (channels, 128)
            )
        high, low = two_parts(gains_ref[...])
        high_ref[...] = high
        low_ref[...] = low

    stations = lax.broadcasted_iota(jnp.int32, (STATIONS, block), 0)
    for row, target in ((0, left_ref), (1, right_ref)):
        hot = (stations == pair_ref[row : row + 1, :]).astype(F32).astype(BF16)
        target[...] = jnp.dot(high_ref[...], hot, preferred_element_type=F32) + jnp.dot(
            low_ref[...], hot, preferred_element_type=F32
        )
    ratio = column_ref[DIRS * channels :, :1]
    total = [[None, None] for _ in range(TIMES)]
    for k in range(DIRS):
        re = pl.ds(k * channels, channels)
        im = pl.ds((DIRS + k) * channels, channels)
        left_re, left_im = left_ref[re, :], left_ref[im, :]
        right_re, right_im = right_ref[re, :], right_ref[im, :]
        flux = column_ref[re, :1]
        pair_re = (left_re * right_re + left_im * right_im) * flux
        pair_im = (left_im * right_re - left_re * right_im) * flux
        for t in range(TIMES):
            project = (
                dirs_ref[0, k] * coord_ref[0, t : t + 1, :]
                + dirs_ref[1, k] * coord_ref[1, t : t + 1, :]
            )
            sky_re, sky_im = turn_parts(project * ratio)
            model_re = pair_re * sky_re - pair_im * sky_im
            model_im = pair_re * sky_im + pair_im * sky_re
            if k == 0:
                total[t] = [model_re, model_im]
            else:
                total[t] = [total[t][0] + model_re, total[t][1] + model_im]
    if residual_out:
        (residual_ref,) = outs
        for t in range(TIMES):
            residual_ref[0, t] = vis_ref[0, t] - total[t][0]
            residual_ref[1, t] = vis_ref[1, t] - total[t][1]
    else:
        (sums_ref,) = outs
        misfit = jnp.zeros((8, 128), F32)
        count = jnp.zeros((8, 128), F32)
        for t in range(TIMES):
            error_re = vis_ref[0, t] - total[t][0]
            error_im = vis_ref[1, t] - total[t][1]
            flagged = flag_ref[t].astype(F32)
            part = flagged * (error_re * error_re + error_im * error_im)
            for r in range(0, channels, 8):
                for c in range(0, block, 128):
                    misfit += part[r : r + 8, c : c + 128]
                    count += flagged[r : r + 8, c : c + 128]
        step_sums = jnp.concatenate([misfit, count], axis=0)

        @pl.when(step == 0)
        def _():
            held_ref[...] = step_sums

        @pl.when(step > 0)
        def _():
            held_ref[...] += step_sums

        @pl.when(step == pl.num_programs(0) - 1)
        def _():
            full = lambda x: jnp.sum(jnp.sum(x, axis=0, keepdims=True), axis=1, keepdims=True)
            basis = legendre(ratio_ref[...])
            entries = [full(held_ref[0:8, :]), full(held_ref[8:16, :])]
            entries += [full(basis[i] * basis[j]) for i in range(NPOLY) for j in range(i + 1)]
            lane = lax.broadcasted_iota(jnp.int32, (8, 128), 1)
            row = jnp.zeros((8, 128), F32)
            for i, entry in enumerate(entries):
                row = jnp.where(lane == i, jnp.broadcast_to(entry, (8, 128)), row)
            sums_ref[...] = jnp.broadcast_to(row[0:1], sums_ref.shape)


def wide_model(gains, vis, flags, pairs, coords, directions, flux, ratio, residual_out, devices=None):
    channels = vis.shape[2]
    count = vis.shape[3]
    block = SUB
    rows = 2 * DIRS * channels
    whole = lambda shape: pl.BlockSpec(shape, lambda i: (0,) * len(shape))
    vis_spec = pl.BlockSpec((2, TIMES, channels, block), lambda i: (0, 0, 0, i))
    if residual_out:
        out_shape = jax.ShapeDtypeStruct(vis.shape, F32)
        out_spec = vis_spec
    else:
        out_shape = jax.ShapeDtypeStruct((devices, 128), F32)
        out_spec = whole((devices, 128))
    return pl.pallas_call(
        functools.partial(
            wide_kernel, residual_out=residual_out, channels=channels, block=block
        ),
        grid=(count // block,),
        in_specs=[
            whole((rows, STATIONS)),
            vis_spec,
            pl.BlockSpec((TIMES, channels, block), lambda i: (0, 0, i)),
            pl.BlockSpec((2, block), lambda i: (0, i)),
            pl.BlockSpec((2, TIMES, block), lambda i: (0, 0, i)),
            pl.BlockSpec(memory_space=pltpu.SMEM),
            whole((DIRS, channels)),
            whole((1, channels)),
        ],
        out_specs=out_spec,
        out_shape=out_shape,
        scratch_shapes=[
            pltpu.VMEM((rows, STATIONS), BF16),
            pltpu.VMEM((rows, STATIONS), BF16),
            pltpu.VMEM((rows, block), F32),
            pltpu.VMEM((rows, block), F32),
            pltpu.VMEM(((DIRS + 1) * channels, 128), F32),
            pltpu.VMEM((16, 128), F32),
        ],
        cost_estimate=lasts(8),
        name="wide_residual" if residual_out else "wide_misfit",
    )(gains, vis, flags, pairs, coords, directions, flux, ratio.reshape(1, -1))


def swap_sum(rows):
    place = lax.broadcasted_iota(jnp.int32, rows[0].shape, 0)
    for bit in (4, 2, 1):
        mine = (place & bit) == 0
        merged = []
        for i in range(len(rows) // 2):
            a, b = rows[i], rows[i + len(rows) // 2]
            low = a + pltpu.roll(a, 8 - bit, axis=0)
            high = b + pltpu.roll(b, bit, axis=0)
            merged.append(jnp.where(mine, low, high))
        rows = merged
    return rows[0]


def one_hot(places, count):
    row = jnp.concatenate([places, places], axis=0).astype(BF16)
    lanes = places.shape[1]
    base = lax.broadcasted_iota(jnp.int32, (16, lanes), 0).astype(F32)
    one = jnp.ones((16, lanes), BF16)
    none = jnp.zeros((16, lanes), BF16)
    return jnp.concatenate(
        [jnp.where(row == (base + float(i)).astype(BF16), one, none) for i in range(0, count, 16)],
        axis=0,
    )


def model_block(part, at, data_ref, table_ref, sky_ref, outs, misfit, geo):
    left_out, right_out, error_out = outs
    lanes = pl.ds(at, SUB)
    picked = []
    for side in range(2):
        station = jnp.broadcast_to(data_ref[part, 16 + side : 17 + side, lanes], (8, SUB))
        quarter = jnp.floor(station * (1.0 / 128.0))
        hot = one_hot(station - 128.0 * quarter, 128)
        got = jnp.dot(
            table_ref[...], jnp.concatenate([hot, hot], axis=0), preferred_element_type=F32
        )
        first, second, lower = quarter == 0.0, quarter == 2.0, quarter < 2.0
        picked.append(
            jnp.concatenate(
                [
                    jnp.where(
                        lower,
                        jnp.where(first, got[i : i + 8], got[32 + i : 40 + i]),
                        jnp.where(second, got[64 + i : 72 + i], got[96 + i : 104 + i]),
                    )
                    for i in range(0, 32, 8)
                ],
                axis=0,
            )
        )
    left, right = picked
    left_out[part, :, lanes] = left
    right_out[part, :, lanes] = right
    pieces = [None] * 8
    for f in range(FEW):
        lr, li = left[16 * f : 16 * f + 8], left[16 * f + 8 : 16 * f + 16]
        rr, ri = right[16 * f : 16 * f + 8], right[16 * f + 8 : 16 * f + 16]
        pair_re = lr * rr + li * ri
        pair_im = li * rr - lr * ri
        for t in range(TIMES):
            if geo is not None:
                dirs, flux, ratio = geo
                project = dirs[0] * data_ref[part, 12 + t : 13 + t, lanes] + dirs[
                    1
                ] * data_ref[part, 14 + t : 15 + t, lanes]
                sky_re, sky_im = turn_parts(project * ratio[f])
                sky_re = sky_re * flux[f]
                sky_im = sky_im * flux[f]
                sky_ref[part, t, f, 0, :, lanes] = sky_re
                sky_ref[part, t, f, 1, :, lanes] = sky_im
            else:
                sky_re = sky_ref[part, t, f, 0, :, lanes]
                sky_im = sky_ref[part, t, f, 1, :, lanes]
            pieces[2 * t + f] = pair_re * sky_re - pair_im * sky_im
            pieces[4 + 2 * t + f] = pair_re * sky_im + pair_im * sky_re
    error = data_ref[part, 0:8, lanes] - swap_sum(pieces)
    error_out[part, :, lanes] = error
    flagged = data_ref[part, 8:12, lanes]
    return misfit + jnp.concatenate([flagged, flagged], axis=0) * (error * error)


def model_runs(data_ref, table_ref, sky_ref, outs, geo):
    steps = LOCAL // SUB // MODEL_RUNS

    def run(i, misfit):
        part, first = i // steps, (i % steps) * MODEL_RUNS
        for j in range(MODEL_RUNS):
            at = pl.multiple_of((first + j) * SUB, SUB)
            misfit = model_block(
                part, at, data_ref, table_ref, sky_ref, outs, misfit, geo
            )
        return misfit

    return lax.fori_loop(0, PARTS * steps, run, jnp.zeros((8, SUB), F32))


def build_table(table_ref, gains):
    for p, part in enumerate(two_parts(gains)):
        for q in range(4):
            table_ref[32 * q : 32 * q + 32, 128 * p : 128 * p + 128] = part[
                :, 128 * q : 128 * q + 128
            ]


def normal_block(part, at, data_ref, left_ref, right_ref, error_ref, sky_ref, inverse):
    lanes = pl.ds(at, SUB)
    error = error_ref[part, :, lanes]
    square = error * error
    square = square + pltpu.roll(square, 4, axis=0)
    flagged = data_ref[part, 8:12, lanes]
    flagged = jnp.concatenate([flagged, flagged], axis=0)
    weight = flagged * (robust_dof + 1.0) / (robust_dof + square * inverse)
    scaled = weight * error
    left = left_ref[part, :, lanes]
    right = right_ref[part, :, lanes]
    first, second = [], []
    wide = lambda row: jnp.broadcast_to(row, (DIRS, SUB))
    for f in range(FEW):
        z_re, z_im = None, None
        for t in range(TIMES):
            i = 2 * t + f
            y_re, y_im = wide(scaled[i : i + 1]), wide(scaled[4 + i : 5 + i])
            sky_re = sky_ref[part, t, f, 0, :, lanes]
            sky_im = sky_ref[part, t, f, 1, :, lanes]
            a = sky_re * y_re + sky_im * y_im
            b = sky_re * y_im - sky_im * y_re
            z_re, z_im = (a, b) if t == 0 else (z_re + a, z_im + b)
        power = wide(weight[f : f + 1] + weight[2 + f : 3 + f])
        lr, li = left[16 * f : 16 * f + 8], left[16 * f + 8 : 16 * f + 16]
        rr, ri = right[16 * f : 16 * f + 8], right[16 * f + 8 : 16 * f + 16]
        first += [rr * z_re - ri * z_im, rr * z_im + ri * z_re, (rr * rr + ri * ri) * power]
        second += [lr * z_re + li * z_im, li * z_re - lr * z_im, (lr * lr + li * li) * power]
    made = []
    for side, pieces in ((0, first), (1, second)):
        station = jnp.broadcast_to(data_ref[part, 16 + side : 17 + side, lanes], (8, SUB))
        half = jnp.where(station >= 256.0, 1.0, 0.0)
        high = jnp.concatenate([half, half], axis=0).astype(BF16)
        parts = two_parts(jnp.concatenate(pieces, axis=0))
        upper = [p[i : i + 16] * high for p in parts for i in (0, 16, 32)]
        hot = one_hot(station - 256.0 * half, 256)
        made.append((jnp.concatenate(list(parts) + upper, axis=0), hot))
    return made


def normal_runs(data_ref, left_ref, right_ref, error_ref, sky_ref, total_ref, buffers, inverse):
    steps = LOCAL // SUB // NORMAL_RUNS
    width = 2 * SUB * NORMAL_RUNS

    def fill(i, into):
        part, first = i // steps, (i % steps) * NORMAL_RUNS
        values_ref, hots_ref = into
        for j in range(NORMAL_RUNS):
            at = pl.multiple_of((first + j) * SUB, SUB)
            made = normal_block(
                part, at, data_ref, left_ref, right_ref, error_ref, sky_ref, inverse
            )
            for side in range(2):
                where = slice((2 * j + side) * SUB, (2 * j + side + 1) * SUB)
                values_ref[:, where] = made[side][0]
                hots_ref[:, where] = made[side][1]

    def add(into):
        values_ref, hots_ref = into
        return lax.dot_general(
            values_ref[...],
            hots_ref[...],
            (((1,), (1,)), ((), ())),
            preferred_element_type=F32,
        )

    fill(0, buffers[0])
    total_ref[...] = jnp.zeros_like(total_ref)

    def run(i, carry):
        one = add(buffers[0])
        fill(2 * i + 1, buffers[1])
        two = add(buffers[1])
        fill(jnp.minimum(2 * i + 2, PARTS * steps - 1), buffers[0])
        total_ref[...] += one + two
        return carry

    lax.fori_loop(0, PARTS * steps // 2, run, 0)


def renew_gains(gains, anchor, total, columns):
    both, upper = total[0:48] + total[48:96], total[96:144] + total[144:192]
    sums = jnp.concatenate([both - upper, upper], axis=1)
    rows = []
    for f in range(FEW):
        flux = columns[:, 2 + f : 3 + f]
        rho = columns[:, 6:7]
        norm = sums[24 * f + 16 : 24 * f + 24] * (flux * flux)
        divisor = norm + rho
        for c in range(2):
            g = gains[16 * f + 8 * c : 16 * f + 8 * c + 8]
            a = anchor[16 * f + 8 * c : 16 * f + 8 * c + 8]
            n = sums[24 * f + 8 * c : 24 * f + 8 * c + 8] + g * norm
            rows.append(0.5 * (g + (n + rho * a) / divisor))
    return jnp.concatenate(rows, axis=0)


def inverse_of(squares_ref, count_ref):
    squares = jnp.sum(squares_ref[...], axis=0, keepdims=True)
    count = jnp.sum(count_ref[...], axis=0, keepdims=True)
    lane = lax.broadcasted_iota(jnp.int32, (1, 128), 1)
    pick = lambda row, i: jnp.sum(jnp.where(lane == i, row, 0.0), axis=1, keepdims=True)
    return 1.0 / (pick(squares, 0) / (pick(count, 1) + 1.0) + small_term)


def renewed(
    squares_ref, count_ref, data_ref, held, gains_ref, anchor_ref, geo_ref, total_ref, buffers
):
    normal_runs(
        data_ref, *held, total_ref, buffers, inverse_of(squares_ref, count_ref)
    )
    return renew_gains(gains_ref[...], anchor_ref[...], total_ref[...], geo_ref[...])


def next_model(gains, data_ref, sky_ref, outs, misfit_out, table_ref):
    build_table(table_ref, gains)
    misfit = model_runs(data_ref, table_ref, sky_ref, outs, None)
    misfit = jnp.sum(misfit[:, :128] + misfit[:, 128:], axis=0, keepdims=True)
    misfit = jnp.sum(misfit, axis=1, keepdims=True)
    misfit_out[...] = jnp.broadcast_to(misfit, misfit_out.shape)


def first_kernel(
    data_ref, gains_ref, geo_ref, left_out, right_out, error_out, sky_out, table_ref
):
    build_table(table_ref, gains_ref[...])
    col = lambda i: geo_ref[:, i : i + 1]
    geo = ((col(0), col(1)), (col(2), col(3)), (col(4), col(5)))
    model_runs(data_ref, table_ref, sky_out, (left_out, right_out, error_out), geo)


def middle_kernel(
    squares_ref,
    count_ref,
    data_ref,
    left_ref,
    right_ref,
    error_ref,
    sky_ref,
    gains_ref,
    anchor_ref,
    geo_ref,
    gains_out,
    left_out,
    right_out,
    error_out,
    misfit_out,
    table_ref,
    total_ref,
    *flat,
):
    buffers = (flat[0:2], flat[2:4])
    held = (left_ref, right_ref, error_ref, sky_ref)
    gains = renewed(
        squares_ref, count_ref, data_ref, held, gains_ref, anchor_ref, geo_ref, total_ref, buffers
    )
    gains_out[...] = gains
    next_model(
        gains, data_ref, sky_ref, (left_out, right_out, error_out), misfit_out, table_ref
    )


def last_kernel(
    squares_ref,
    count_ref,
    data_ref,
    left_ref,
    right_ref,
    error_ref,
    sky_ref,
    gains_ref,
    anchor_ref,
    geo_ref,
    gains_out,
    total_ref,
    *flat,
):
    buffers = (flat[0:2], flat[2:4])
    held = (left_ref, right_ref, error_ref, sky_ref)
    gains = renewed(
        squares_ref, count_ref, data_ref, held, gains_ref, anchor_ref, geo_ref, total_ref, buffers
    )
    gains_out[...] = jnp.broadcast_to(gains[None], gains_out.shape)


ROWS = 18
GAIN_ROWS = 2 * FEW * DIRS
SKY = (TIMES, FEW, 2, DIRS)
GRANT = pltpu.CompilerParams(vmem_limit_bytes=8 * 1024 * 1024)
ON_CHIP = pl.BlockSpec(memory_space=pltpu.VMEM)


def shapes_of(rows):
    return jax.ShapeDtypeStruct((PARTS, rows, LOCAL), F32)


def held_shapes():
    return [
        shapes_of(GAIN_ROWS),
        shapes_of(GAIN_ROWS),
        shapes_of(8),
        jax.ShapeDtypeStruct((PARTS,) + SKY + (LOCAL,), F32),
    ]


def first_call(data, gains, geo):
    return pl.pallas_call(
        first_kernel,
        in_specs=[ON_CHIP] * 3,
        out_specs=[ON_CHIP] * 4,
        out_shape=held_shapes(),
        scratch_shapes=[pltpu.VMEM((128, 256), BF16)],
        compiler_params=GRANT,
        cost_estimate=lasts(6),
        name="first_model",
    )(data, gains, geo)


def run_buffers():
    width = 2 * SUB * NORMAL_RUNS
    return [pltpu.VMEM((192, width), BF16), pltpu.VMEM((256, width), BF16)] * 2


def middle_call(squares, count, data, held, gains, anchor, geo, devices):
    return pl.pallas_call(
        middle_kernel,
        in_specs=[ON_CHIP] * 10,
        out_specs=[ON_CHIP] * 5,
        out_shape=[
            jax.ShapeDtypeStruct((GAIN_ROWS, STATIONS), F32),
            shapes_of(GAIN_ROWS),
            shapes_of(GAIN_ROWS),
            shapes_of(8),
            jax.ShapeDtypeStruct((devices, 128), F32),
        ],
        scratch_shapes=[pltpu.VMEM((128, 256), BF16), pltpu.VMEM((192, 256), F32), *run_buffers()],
        compiler_params=GRANT,
        cost_estimate=lasts(14),
        name="normal_and_model",
    )(squares, count, data, *held, gains, anchor, geo)


def last_call(squares, count, data, held, gains, anchor, geo):
    return pl.pallas_call(
        last_kernel,
        in_specs=[ON_CHIP] * 10,
        out_specs=ON_CHIP,
        out_shape=jax.ShapeDtypeStruct((PARTS, GAIN_ROWS, STATIONS), F32),
        scratch_shapes=[pltpu.VMEM((192, 256), F32), *run_buffers()],
        compiler_params=GRANT,
        cost_estimate=lasts(8),
        name="normal_last",
    )(squares, count, data, *held, gains, anchor, geo)


def cholesky_solve(gram, rhs):
    order = len(rhs)
    factor = [[None] * order for _ in range(order)]
    for i in range(order):
        for j in range(i + 1):
            value = gram[i][j]
            for m in range(j):
                value = value - factor[i][m] * factor[j][m]
            factor[i][j] = jnp.sqrt(value) if i == j else value / factor[j][j]
    forward = []
    for i in range(order):
        running = rhs[i]
        for j in range(i):
            running = running - factor[i][j] * forward[j]
        forward.append(running / factor[i][i])
    backward = [None] * order
    for i in reversed(range(order)):
        running = forward[i]
        for j in range(i + 1, order):
            running = running - factor[j][i] * backward[j]
        backward[i] = running / factor[i][i]
    return backward


def consensus_kernel(rhs_ref, arrived_ref, out_ref, *, copies):
    rhs = rhs_ref[0]
    for i in range(1, rhs_ref.shape[0]):
        rhs = rhs + rhs_ref[i]
    sums = jnp.sum(arrived_ref[...], axis=0, keepdims=True) * (1.0 / copies)
    lane = lax.broadcasted_iota(jnp.int32, (1, 128), 1)
    pick = lambda i: jnp.sum(jnp.where(lane == i, sums, 0.0), axis=1, keepdims=True)
    gram = [[pick(2 + i * (i + 1) // 2 + j) for j in range(i + 1)] for i in range(NPOLY)]
    solved = cholesky_solve(gram, [rhs[j : j + 1] for j in range(NPOLY)])
    out_ref[...] = jnp.broadcast_to(jnp.concatenate(solved, axis=0)[None], out_ref.shape)


def consensus_call(rhs, arrived, copies):
    return pl.pallas_call(
        functools.partial(consensus_kernel, copies=copies),
        in_specs=[ON_CHIP] * 2,
        out_specs=ON_CHIP,
        out_shape=jax.ShapeDtypeStruct(rhs.shape, F32),
        compiler_params=GRANT,
        cost_estimate=lasts(1),
        name="consensus",
    )(rhs, arrived)


def finish_kernel(solved_ref, gains_ref, dual_ref, ratio_ref, consensus_out, dual_out):
    channels = ratio_ref.shape[1]
    own = lax.broadcasted_iota(jnp.int32, (channels, channels), 0)
    own = own == lax.broadcasted_iota(jnp.int32, (channels, channels), 1)
    columns = [
        jnp.sum(
            jnp.where(own, jnp.broadcast_to(row, (channels, channels)), 0.0),
            axis=1,
            keepdims=True,
        )
        for row in legendre(ratio_ref[...])
    ]
    for k in range(DIRS):
        rows = [solved_ref[k, j : j + 1, :] for j in range(NPOLY)]
        for j in range(NPOLY):
            consensus_out[0, j, k : k + 1, :] = rows[j]
        fitted = sum(columns[j] * rows[j] for j in range(NPOLY))
        dual_out[0, k] = dual_ref[0, k] + gains_ref[0, k] - fitted


def finish_call(solved, gains, dual, ratio):
    channels = ratio.shape[0]
    big = pl.BlockSpec((1, DIRS, channels, STATIONS), lambda c: (c, 0, 0, 0))
    return pl.pallas_call(
        finish_kernel,
        grid=(2,),
        in_specs=[
            pl.BlockSpec((DIRS, NPOLY, STATIONS), lambda c: (c, 0, 0)),
            big,
            big,
            pl.BlockSpec((1, channels), lambda c: (0, 0)),
        ],
        out_specs=[pl.BlockSpec((1, NPOLY, DIRS, STATIONS), lambda c: (c, 0, 0, 0)), big],
        out_shape=[
            jax.ShapeDtypeStruct((2, NPOLY, DIRS, STATIONS), F32),
            jax.ShapeDtypeStruct(dual.shape, F32),
        ],
        cost_estimate=lasts(1),
        name="finish",
    )(solved, gains, dual, ratio.reshape(1, -1))


def own_channels(array, axis, own):
    return lax.dynamic_slice_in_dim(array, own * FEW, FEW, axis)


def pack_kernel(vis_ref, flag_ref, pair_ref, coord_ref, out_ref):
    def run(j, carry):
        lanes = pl.ds(pl.multiple_of(j * 128, 128), 128)
        to = pl.ds(j, 1)
        for c in range(2):
            for t in range(TIMES):
                rows = vis_ref[c, t, :, lanes]
                for f in range(PARTS * FEW):
                    out_ref[f // FEW, (2 * c + t) * FEW + f % FEW, to, :] = rows[f : f + 1]
                rows = coord_ref[c, t : t + 1, lanes]
                for d in range(PARTS):
                    out_ref[d, 12 + 2 * c + t, to, :] = rows
        for t in range(TIMES):
            rows = flag_ref[t, :, lanes].astype(F32)
            for f in range(PARTS * FEW):
                out_ref[f // FEW, 8 + t * FEW + f % FEW, to, :] = rows[f : f + 1]
        for side in range(2):
            rows = pair_ref[side : side + 1, lanes].astype(F32)
            for d in range(PARTS):
                out_ref[d, 16 + side, to, :] = rows
        return carry

    lax.fori_loop(0, out_ref.shape[2], run, 0)


def packed(vis, flags, pairs, coords):
    half = LOCAL // 2
    channels = vis.shape[2]
    return pl.pallas_call(
        pack_kernel,
        grid=(2,),
        in_specs=[
            pl.BlockSpec((2, TIMES, channels, half), lambda i: (0, 0, 0, i)),
            pl.BlockSpec((TIMES, channels, half), lambda i: (0, 0, i)),
            pl.BlockSpec((2, half), lambda i: (0, i)),
            pl.BlockSpec((2, TIMES, half), lambda i: (0, 0, i)),
        ],
        out_specs=pl.BlockSpec((PARTS, ROWS, half // 128, 128), lambda i: (0, 0, i, 0)),
        out_shape=jax.ShapeDtypeStruct((PARTS, ROWS, LOCAL // 128, 128), F32),
        cost_estimate=lasts(2),
        name="pack",
    )(vis, flags, pairs, coords)


def body(
    visibilities,
    sample_flag_weight,
    baseline_station_pair,
    baseline_spatial_coords,
    directions,
    source_flux,
    channel_ratio,
    jones_gains,
    scaled_dual,
    consensus,
    penalty,
):
    devices = lax.axis_size(ALL)
    own = lax.axis_index(BL)
    channels = channel_ratio.shape[0]
    rho = penalty * (2.0 * BASELINES * TIMES / STATIONS)

    wide = functools.partial(
        wide_model,
        vis=visibilities,
        flags=sample_flag_weight,
        pairs=baseline_station_pair,
        coords=baseline_spatial_coords,
        directions=directions,
        flux=source_flux,
        ratio=channel_ratio,
    )
    payload = wide(jones_gains.reshape(-1, STATIONS), residual_out=False, devices=devices)
    send = packed(
        visibilities, sample_flag_weight, baseline_station_pair, baseline_spatial_coords
    )
    send = send.reshape(PARTS, ROWS * LOCAL // 128, 128)
    data = lax.all_to_all(send, BL, 0, 0, tiled=True).reshape(PARTS, ROWS, LOCAL)

    ratio = own_channels(channel_ratio, 0, own)
    flux = own_channels(source_flux, 1, own)
    basis = legendre(ratio)
    def rows_of(array):
        part = own_channels(array, 2, own)
        return part.transpose(2, 0, 1, 3)

    dual = rows_of(scaled_dual)
    anchor = (
        sum(
            basis[j][:, None, None, None] * consensus[:, j][None] for j in range(NPOLY)
        )
        - dual
    ).reshape(GAIN_ROWS, STATIONS)
    gains = rows_of(jones_gains).reshape(GAIN_ROWS, STATIONS)
    geo = jnp.concatenate(
        [
            directions.T,
            flux,
            jnp.broadcast_to(ratio[None], (DIRS, FEW)),
            rho[:, None],
            jnp.zeros((DIRS, 1), F32),
        ],
        axis=1,
    )

    left, right, error, sky = first_call(data, gains, geo)
    all_basis = legendre(channel_ratio)
    payload, error, anchor, *all_basis = lax.optimization_barrier(
        (payload, error, anchor, *all_basis)
    )
    arrived = lax.all_to_all(payload[:, None], ALL, 0, 0, tiled=True)[:, 0]
    squares = arrived
    for iteration in range(ITERS - 1):
        gains, left, right, error, misfit = middle_call(
            squares, arrived, data, (left, right, error, sky), gains, anchor, geo, devices
        )
        squares = lax.all_to_all(misfit[:, None], ALL, 0, 0, tiled=True)[:, 0]
    gains = last_call(squares, arrived, data, (left, right, error, sky), gains, anchor, geo)

    gains, *all_basis = lax.optimization_barrier((gains, *all_basis))
    gathered = lax.all_to_all(gains, BL, 0, 0, tiled=True)
    new_gains = (
        gathered.reshape(PARTS * FEW, 2, DIRS, STATIONS).transpose(1, 2, 0, 3)
    )
    new_gains = lax.optimization_barrier(new_gains)
    residuals = wide(new_gains.reshape(-1, STATIONS), residual_out=True)

    lifted = new_gains + scaled_dual
    rhs = jnp.stack(
        [
            (all_basis[j][None, None, :, None] * lifted).sum(axis=2).reshape(-1, STATIONS)
            for j in range(NPOLY)
        ],
        axis=1,
    )
    rhs = lax.all_to_all(rhs, FREQ, 0, 0, tiled=True)
    rhs, residuals = lax.optimization_barrier((rhs, residuals))
    solved = consensus_call(rhs, arrived, lax.axis_size(BL))
    everyone = lax.all_to_all(solved, FREQ, 0, 0, tiled=True)
    new_consensus, new_dual = finish_call(everyone, new_gains, scaled_dual, channel_ratio)
    return (new_gains, new_consensus, new_dual, residuals)


def solution(mesh):
    split = Mesh(
        mesh.devices.reshape(4, 2, 4, 2, 2), ("bl_0", "bl_1", "freq_0", "freq_1", "freq_2")
    )
    in_specs = (
        P(None, None, FREQ, BL),
        P(None, FREQ, BL),
        P(None, BL),
        P(None, None, BL),
        P(),
        P(None, FREQ),
        P(FREQ),
        P(None, None, FREQ, None),
        P(None, None, FREQ, None),
        P(),
        P(),
    )
    out_specs = (P(None, None, FREQ, None), P(), P(None, None, FREQ, None), P(None, None, FREQ, BL))
    return jax.shard_map(body, mesh=split, in_specs=in_specs, out_specs=out_specs, check_vma=False)
```

```python
import functools

import jax
import jax.numpy as jnp
from jax import lax
from jax.experimental import pallas as pl
from jax.experimental.pallas import tpu as pltpu
from jax.sharding import Mesh
from jax.sharding import PartitionSpec as P

NPOLY = 3
ITERS = 3
BL = ("bl_0", "bl_1")
FREQ = ("freq_0", "freq_1", "freq_2")
ALL = BL + FREQ

STATIONS = 512
DIRS = 8
TIMES = 2
BASELINES = 16384
PARTS = 8
FEW = 2
LOCAL = BASELINES // PARTS
SUB = 256
MODEL_RUNS = 8
NORMAL_RUNS = 8

robust_dof = 2.0
small_term = 1e-06

SIN_TERMS = (
    3.1415926401307086,
    -5.167710083507905,
    2.5500775232148403,
    -0.5982912856219295,
    0.07765766030867731,
)
COS_TERMS = (
    0.9999999997799046,
    -4.934802137078821,
    4.058709159556128,
    -1.3352120030477381,
    0.23493731380150681,
    -0.024396324323359975,
)

F32 = jnp.float32
PER_US = 4.0e6


def lasts(microseconds):
    return pl.CostEstimate(
        flops=int(microseconds * PER_US), transcendentals=0, bytes_accessed=1 << 20
    )


BF16 = jnp.bfloat16


def legendre(ratios):
    scaled = (ratios - 1.05) / 0.35
    values = [jnp.ones_like(scaled), scaled]
    values.append((3 * scaled * values[1] - 1 * values[0]) / 2)
    return values[:NPOLY]


def horner(terms, w):
    value = jnp.full_like(w, terms[-1])
    for term in terms[-2::-1]:
        value = value * w + term
    return value


def turn_parts(turns):
    f = turns - jnp.floor(turns + 0.5)
    w = f * f
    half_sin = f * horner(SIN_TERMS, w)
    half_cos = horner(COS_TERMS, w)
    twice = half_sin + half_sin
    return 1.0 - twice * half_sin, twice * half_cos


def two_parts(value):
    high = value.astype(BF16)
    low = (value - high.astype(F32)).astype(BF16)
    return high, low


def wide_kernel(
    gains_ref,
    vis_ref,
    flag_ref,
    pair_ref,
    coord_ref,
    dirs_ref,
    flux_ref,
    ratio_ref,
    *rest,
    residual_out,
    channels,
    block,
):
    outs, rest = rest[:1], rest[1:]
    high_ref, low_ref, left_ref, right_ref, column_ref, held_ref = rest
    step = pl.program_id(0)

    @pl.when(step == 0)
    def _():
        own = lax.broadcasted_iota(jnp.int32, (channels, channels), 0)
        own = own == lax.broadcasted_iota(jnp.int32, (channels, channels), 1)
        for k in range(DIRS + 1):
            row = flux_ref[k : k + 1, :] if k < DIRS else ratio_ref[...]
            column = jnp.where(own, jnp.broadcast_to(row, (channels, channels)), 0.0)
            column_ref[k * channels : (k + 1) * channels, :] = jnp.broadcast_to(
                jnp.sum(column, axis=1, keepdims=True), (channels, 128)
            )
        high, low = two_parts(gains_ref[...])
        high_ref[...] = high
        low_ref[...] = low

    stations = lax.broadcasted_iota(jnp.int32, (STATIONS, block), 0)
    for row, target in ((0, left_ref), (1, right_ref)):
        hot = (stations == pair_ref[row : row + 1, :]).astype(F32).astype(BF16)
        target[...] = jnp.dot(high_ref[...], hot, preferred_element_type=F32) + jnp.dot(
            low_ref[...], hot, preferred_element_type=F32
        )
    ratio = column_ref[DIRS * channels :, :1]
    total = [[None, None] for _ in range(TIMES)]
    for k in range(DIRS):
        re = pl.ds(k * channels, channels)
        im = pl.ds((DIRS + k) * channels, channels)
        left_re, left_im = left_ref[re, :], left_ref[im, :]
        right_re, right_im = right_ref[re, :], right_ref[im, :]
        flux = column_ref[re, :1]
        pair_re = (left_re * right_re + left_im * right_im) * flux
        pair_im = (left_im * right_re - left_re * right_im) * flux
        for t in range(TIMES):
            project = (
                dirs_ref[0, k] * coord_ref[0, t : t + 1, :]
                + dirs_ref[1, k] * coord_ref[1, t : t + 1, :]
            )
            sky_re, sky_im = turn_parts(project * ratio)
            model_re = pair_re * sky_re - pair_im * sky_im
            model_im = pair_re * sky_im + pair_im * sky_re
            if k == 0:
                total[t] = [model_re, model_im]
            else:
                total[t] = [total[t][0] + model_re, total[t][1] + model_im]
    if residual_out:
        (residual_ref,) = outs
        for t in range(TIMES):
            residual_ref[0, t] = vis_ref[0, t] - total[t][0]
            residual_ref[1, t] = vis_ref[1, t] - total[t][1]
    else:
        (sums_ref,) = outs
        misfit = jnp.zeros((8, 128), F32)
        count = jnp.zeros((8, 128), F32)
        for t in range(TIMES):
            error_re = vis_ref[0, t] - total[t][0]
            error_im = vis_ref[1, t] - total[t][1]
            flagged = flag_ref[t].astype(F32)
            part = flagged * (error_re * error_re + error_im * error_im)
            for r in range(0, channels, 8):
                for c in range(0, block, 128):
                    misfit += part[r : r + 8, c : c + 128]
                    count += flagged[r : r + 8, c : c + 128]
        step_sums = jnp.concatenate([misfit, count], axis=0)

        @pl.when(step == 0)
        def _():
            held_ref[...] = step_sums

        @pl.when(step > 0)
        def _():
            held_ref[...] += step_sums

        @pl.when(step == pl.num_programs(0) - 1)
        def _():
            full = lambda x: jnp.sum(jnp.sum(x, axis=0, keepdims=True), axis=1, keepdims=True)
            basis = legendre(ratio_ref[...])
            entries = [full(held_ref[0:8, :]), full(held_ref[8:16, :])]
            entries += [full(basis[i] * basis[j]) for i in range(NPOLY) for j in range(i + 1)]
            lane = lax.broadcasted_iota(jnp.int32, (8, 128), 1)
            row = jnp.zeros((8, 128), F32)
            for i, entry in enumerate(entries):
                row = jnp.where(lane == i, jnp.broadcast_to(entry, (8, 128)), row)
            sums_ref[...] = jnp.broadcast_to(row[0:1], sums_ref.shape)


def wide_model(gains, vis, flags, pairs, coords, directions, flux, ratio, residual_out, devices=None):
    channels = vis.shape[2]
    count = vis.shape[3]
    block = SUB
    rows = 2 * DIRS * channels
    whole = lambda shape: pl.BlockSpec(shape, lambda i: (0,) * len(shape))
    vis_spec = pl.BlockSpec((2, TIMES, channels, block), lambda i: (0, 0, 0, i))
    if residual_out:
        out_shape = jax.ShapeDtypeStruct(vis.shape, F32)
        out_spec = vis_spec
    else:
        out_shape = jax.ShapeDtypeStruct((devices, 128), F32)
        out_spec = whole((devices, 128))
    return pl.pallas_call(
        functools.partial(
            wide_kernel, residual_out=residual_out, channels=channels, block=block
        ),
        grid=(count // block,),
        in_specs=[
            whole((rows, STATIONS)),
            vis_spec,
            pl.BlockSpec((TIMES, channels, block), lambda i: (0, 0, i)),
            pl.BlockSpec((2, block), lambda i: (0, i)),
            pl.BlockSpec((2, TIMES, block), lambda i: (0, 0, i)),
            pl.BlockSpec(memory_space=pltpu.SMEM),
            whole((DIRS, channels)),
            whole((1, channels)),
        ],
        out_specs=out_spec,
        out_shape=out_shape,
        scratch_shapes=[
            pltpu.VMEM((rows, STATIONS), BF16),
            pltpu.VMEM((rows, STATIONS), BF16),
            pltpu.VMEM((rows, block), F32),
            pltpu.VMEM((rows, block), F32),
            pltpu.VMEM(((DIRS + 1) * channels, 128), F32),
            pltpu.VMEM((16, 128), F32),
        ],
        cost_estimate=lasts(8),
        name="wide_residual" if residual_out else "wide_misfit",
    )(gains, vis, flags, pairs, coords, directions, flux, ratio.reshape(1, -1))


def swap_sum(rows):
    place = lax.broadcasted_iota(jnp.int32, rows[0].shape, 0)
    for bit in (4, 2, 1):
        mine = (place & bit) == 0
        merged = []
        for i in range(len(rows) // 2):
            a, b = rows[i], rows[i + len(rows) // 2]
            low = a + pltpu.roll(a, 8 - bit, axis=0)
            high = b + pltpu.roll(b, bit, axis=0)
            merged.append(jnp.where(mine, low, high))
        rows = merged
    return rows[0]


def one_hot(places, count):
    row = jnp.concatenate([places, places], axis=0).astype(BF16)
    lanes = places.shape[1]
    base = lax.broadcasted_iota(jnp.int32, (16, lanes), 0).astype(F32)
    one = jnp.ones((16, lanes), BF16)
    none = jnp.zeros((16, lanes), BF16)
    return jnp.concatenate(
        [jnp.where(row == (base + float(i)).astype(BF16), one, none) for i in range(0, count, 16)],
        axis=0,
    )


def model_block(part, at, data_ref, table_ref, sky_ref, outs, misfit, geo):
    left_out, right_out, error_out = outs
    lanes = pl.ds(at, SUB)
    picked = []
    for side in range(2):
        station = jnp.broadcast_to(data_ref[part, 16 + side : 17 + side, lanes], (8, SUB))
        quarter = jnp.floor(station * (1.0 / 128.0))
        hot = one_hot(station - 128.0 * quarter, 128)
        got = jnp.dot(
            table_ref[...], jnp.concatenate([hot, hot], axis=0), preferred_element_type=F32
        )
        first, second, lower = quarter == 0.0, quarter == 2.0, quarter < 2.0
        picked.append(
            jnp.concatenate(
                [
                    jnp.where(
                        lower,
                        jnp.where(first, got[i : i + 8], got[32 + i : 40 + i]),
                        jnp.where(second, got[64 + i : 72 + i], got[96 + i : 104 + i]),
                    )
                    for i in range(0, 32, 8)
                ],
                axis=0,
            )
        )
    left, right = picked
    left_out[part, :, lanes] = left
    right_out[part, :, lanes] = right
    pieces = [None] * 8
    for f in range(FEW):
        lr, li = left[16 * f : 16 * f + 8], left[16 * f + 8 : 16 * f + 16]
        rr, ri = right[16 * f : 16 * f + 8], right[16 * f + 8 : 16 * f + 16]
        pair_re = lr * rr + li * ri
        pair_im = li * rr - lr * ri
        for t in range(TIMES):
            if geo is not None:
                dirs, flux, ratio = geo
                project = dirs[0] * data_ref[part, 12 + t : 13 + t, lanes] + dirs[
                    1
                ] * data_ref[part, 14 + t : 15 + t, lanes]
                sky_re, sky_im = turn_parts(project * ratio[f])
                sky_re = sky_re * flux[f]
                sky_im = sky_im * flux[f]
                sky_ref[part, t, f, 0, :, lanes] = sky_re
                sky_ref[part, t, f, 1, :, lanes] = sky_im
            else:
                sky_re = sky_ref[part, t, f, 0, :, lanes]
                sky_im = sky_ref[part, t, f, 1, :, lanes]
            pieces[2 * t + f] = pair_re * sky_re - pair_im * sky_im
            pieces[4 + 2 * t + f] = pair_re * sky_im + pair_im * sky_re
    error = data_ref[part, 0:8, lanes] - swap_sum(pieces)
    error_out[part, :, lanes] = error
    flagged = data_ref[part, 8:12, lanes]
    return misfit + jnp.concatenate([flagged, flagged], axis=0) * (error * error)


def model_runs(data_ref, table_ref, sky_ref, outs, geo):
    steps = LOCAL // SUB // MODEL_RUNS

    def run(i, misfit):
        part, first = i // steps, (i % steps) * MODEL_RUNS
        for j in range(MODEL_RUNS):
            at = pl.multiple_of((first + j) * SUB, SUB)
            misfit = model_block(
                part, at, data_ref, table_ref, sky_ref, outs, misfit, geo
            )
        return misfit

    return lax.fori_loop(0, PARTS * steps, run, jnp.zeros((8, SUB), F32))


def build_table(table_ref, gains):
    for p, part in enumerate(two_parts(gains)):
        for q in range(4):
            table_ref[32 * q : 32 * q + 32, 128 * p : 128 * p + 128] = part[
                :, 128 * q : 128 * q + 128
            ]


def normal_block(part, at, data_ref, left_ref, right_ref, error_ref, sky_ref, inverse):
    lanes = pl.ds(at, SUB)
    error = error_ref[part, :, lanes]
    square = error * error
    square = square + pltpu.roll(square, 4, axis=0)
    flagged = data_ref[part, 8:12, lanes]
    flagged = jnp.concatenate([flagged, flagged], axis=0)
    weight = flagged * (robust_dof + 1.0) / (robust_dof + square * inverse)
    scaled = weight * error
    left = left_ref[part, :, lanes]
    right = right_ref[part, :, lanes]
    first, second = [], []
    wide = lambda row: jnp.broadcast_to(row, (DIRS, SUB))
    for f in range(FEW):
        z_re, z_im = None, None
        for t in range(TIMES):
            i = 2 * t + f
            y_re, y_im = wide(scaled[i : i + 1]), wide(scaled[4 + i : 5 + i])
            sky_re = sky_ref[part, t, f, 0, :, lanes]
            sky_im = sky_ref[part, t, f, 1, :, lanes]
            a = sky_re * y_re + sky_im * y_im
            b = sky_re * y_im - sky_im * y_re
            z_re, z_im = (a, b) if t == 0 else (z_re + a, z_im + b)
        power = wide(weight[f : f + 1] + weight[2 + f : 3 + f])
        lr, li = left[16 * f : 16 * f + 8], left[16 * f + 8 : 16 * f + 16]
        rr, ri = right[16 * f : 16 * f + 8], right[16 * f + 8 : 16 * f + 16]
        first += [rr * z_re - ri * z_im, rr * z_im + ri * z_re, (rr * rr + ri * ri) * power]
        second += [lr * z_re + li * z_im, li * z_re - lr * z_im, (lr * lr + li * li) * power]
    made = []
    for side, pieces in ((0, first), (1, second)):
        station = jnp.broadcast_to(data_ref[part, 16 + side : 17 + side, lanes], (8, SUB))
        half = jnp.where(station >= 256.0, 1.0, 0.0)
        high = jnp.concatenate([half, half], axis=0).astype(BF16)
        parts = two_parts(jnp.concatenate(pieces, axis=0))
        upper = [p[i : i + 16] * high for p in parts for i in (0, 16, 32)]
        hot = one_hot(station - 256.0 * half, 256)
        made.append((jnp.concatenate(list(parts) + upper, axis=0), hot))
    return made


def normal_runs(data_ref, left_ref, right_ref, error_ref, sky_ref, total_ref, buffers, inverse):
    steps = LOCAL // SUB // NORMAL_RUNS
    width = 2 * SUB * NORMAL_RUNS

    def fill(i, into):
        part, first = i // steps, (i % steps) * NORMAL_RUNS
        values_ref, hots_ref = into
        for j in range(NORMAL_RUNS):
            at = pl.multiple_of((first + j) * SUB, SUB)
            made = normal_block(
                part, at, data_ref, left_ref, right_ref, error_ref, sky_ref, inverse
            )
            for side in range(2):
                where = slice((2 * j + side) * SUB, (2 * j + side + 1) * SUB)
                values_ref[:, where] = made[side][0]
                hots_ref[:, where] = made[side][1]

    def add(into):
        values_ref, hots_ref = into
        return lax.dot_general(
            values_ref[...],
            hots_ref[...],
            (((1,), (1,)), ((), ())),
            preferred_element_type=F32,
        )

    fill(0, buffers[0])
    total_ref[...] = jnp.zeros_like(total_ref)

    def run(i, carry):
        one = add(buffers[0])
        fill(2 * i + 1, buffers[1])
        two = add(buffers[1])
        fill(jnp.minimum(2 * i + 2, PARTS * steps - 1), buffers[0])
        total_ref[...] += one + two
        return carry

    lax.fori_loop(0, PARTS * steps // 2, run, 0)


def renew_gains(gains, anchor, total, columns):
    both, upper = total[0:48] + total[48:96], total[96:144] + total[144:192]
    sums = jnp.concatenate([both - upper, upper], axis=1)
    rows = []
    for f in range(FEW):
        flux = columns[:, 2 + f : 3 + f]
        rho = columns[:, 6:7]
        norm = sums[24 * f + 16 : 24 * f + 24] * (flux * flux)
        divisor = norm + rho
        for c in range(2):
            g = gains[16 * f + 8 * c : 16 * f + 8 * c + 8]
            a = anchor[16 * f + 8 * c : 16 * f + 8 * c + 8]
            n = sums[24 * f + 8 * c : 24 * f + 8 * c + 8] + g * norm
            rows.append(0.5 * (g + (n + rho * a) / divisor))
    return jnp.concatenate(rows, axis=0)


def inverse_of(squares_ref, count_ref):
    squares = jnp.sum(squares_ref[...], axis=0, keepdims=True)
    count = jnp.sum(count_ref[...], axis=0, keepdims=True)
    lane = lax.broadcasted_iota(jnp.int32, (1, 128), 1)
    pick = lambda row, i: jnp.sum(jnp.where(lane == i, row, 0.0), axis=1, keepdims=True)
    return 1.0 / (pick(squares, 0) / (pick(count, 1) + 1.0) + small_term)


def renewed(
    squares_ref, count_ref, data_ref, held, gains_ref, anchor_ref, geo_ref, total_ref, buffers
):
    normal_runs(
        data_ref, *held, total_ref, buffers, inverse_of(squares_ref, count_ref)
    )
    return renew_gains(gains_ref[...], anchor_ref[...], total_ref[...], geo_ref[...])


def next_model(gains, data_ref, sky_ref, outs, misfit_out, table_ref):
    build_table(table_ref, gains)
    misfit = model_runs(data_ref, table_ref, sky_ref, outs, None)
    misfit = jnp.sum(misfit[:, :128] + misfit[:, 128:], axis=0, keepdims=True)
    misfit = jnp.sum(misfit, axis=1, keepdims=True)
    misfit_out[...] = jnp.broadcast_to(misfit, misfit_out.shape)


def first_kernel(
    data_ref, gains_ref, geo_ref, left_out, right_out, error_out, sky_out, table_ref
):
    build_table(table_ref, gains_ref[...])
    col = lambda i: geo_ref[:, i : i + 1]
    geo = ((col(0), col(1)), (col(2), col(3)), (col(4), col(5)))
    model_runs(data_ref, table_ref, sky_out, (left_out, right_out, error_out), geo)


def middle_kernel(
    squares_ref,
    count_ref,
    data_ref,
    left_ref,
    right_ref,
    error_ref,
    sky_ref,
    gains_ref,
    anchor_ref,
    geo_ref,
    gains_out,
    left_out,
    right_out,
    error_out,
    misfit_out,
    table_ref,
    total_ref,
    *flat,
):
    buffers = (flat[0:2], flat[2:4])
    held = (left_ref, right_ref, error_ref, sky_ref)
    gains = renewed(
        squares_ref, count_ref, data_ref, held, gains_ref, anchor_ref, geo_ref, total_ref, buffers
    )
    gains_out[...] = gains
    next_model(
        gains, data_ref, sky_ref, (left_out, right_out, error_out), misfit_out, table_ref
    )


def last_kernel(
    squares_ref,
    count_ref,
    data_ref,
    left_ref,
    right_ref,
    error_ref,
    sky_ref,
    gains_ref,
    anchor_ref,
    geo_ref,
    gains_out,
    total_ref,
    *flat,
):
    buffers = (flat[0:2], flat[2:4])
    held = (left_ref, right_ref, error_ref, sky_ref)
    gains = renewed(
        squares_ref, count_ref, data_ref, held, gains_ref, anchor_ref, geo_ref, total_ref, buffers
    )
    gains_out[...] = jnp.broadcast_to(gains[None], gains_out.shape)


ROWS = 18
GAIN_ROWS = 2 * FEW * DIRS
SKY = (TIMES, FEW, 2, DIRS)
GRANT = pltpu.CompilerParams(vmem_limit_bytes=8 * 1024 * 1024)
ON_CHIP = pl.BlockSpec(memory_space=pltpu.VMEM)


def shapes_of(rows):
    return jax.ShapeDtypeStruct((PARTS, rows, LOCAL), F32)


def held_shapes():
    return [
        shapes_of(GAIN_ROWS),
        shapes_of(GAIN_ROWS),
        shapes_of(8),
        jax.ShapeDtypeStruct((PARTS,) + SKY + (LOCAL,), F32),
    ]


def first_call(data, gains, geo):
    return pl.pallas_call(
        first_kernel,
        in_specs=[ON_CHIP] * 3,
        out_specs=[ON_CHIP] * 4,
        out_shape=held_shapes(),
        scratch_shapes=[pltpu.VMEM((128, 256), BF16)],
        compiler_params=GRANT,
        cost_estimate=lasts(6),
        name="first_model",
    )(data, gains, geo)


def run_buffers():
    width = 2 * SUB * NORMAL_RUNS
    return [pltpu.VMEM((192, width), BF16), pltpu.VMEM((256, width), BF16)] * 2


def middle_call(squares, count, data, held, gains, anchor, geo, devices):
    return pl.pallas_call(
        middle_kernel,
        in_specs=[ON_CHIP] * 10,
        out_specs=[ON_CHIP] * 5,
        out_shape=[
            jax.ShapeDtypeStruct((GAIN_ROWS, STATIONS), F32),
            shapes_of(GAIN_ROWS),
            shapes_of(GAIN_ROWS),
            shapes_of(8),
            jax.ShapeDtypeStruct((devices, 128), F32),
        ],
        scratch_shapes=[pltpu.VMEM((128, 256), BF16), pltpu.VMEM((192, 256), F32), *run_buffers()],
        compiler_params=GRANT,
        cost_estimate=lasts(14),
        name="normal_and_model",
    )(squares, count, data, *held, gains, anchor, geo)


def last_call(squares, count, data, held, gains, anchor, geo):
    return pl.pallas_call(
        last_kernel,
        in_specs=[ON_CHIP] * 10,
        out_specs=ON_CHIP,
        out_shape=jax.ShapeDtypeStruct((PARTS, GAIN_ROWS, STATIONS), F32),
        scratch_shapes=[pltpu.VMEM((192, 256), F32), *run_buffers()],
        compiler_params=GRANT,
        cost_estimate=lasts(8),
        name="normal_last",
    )(squares, count, data, *held, gains, anchor, geo)


def cholesky_solve(gram, rhs):
    order = len(rhs)
    factor = [[None] * order for _ in range(order)]
    for i in range(order):
        for j in range(i + 1):
            value = gram[i][j]
            for m in range(j):
                value = value - factor[i][m] * factor[j][m]
            factor[i][j] = jnp.sqrt(value) if i == j else value / factor[j][j]
    forward = []
    for i in range(order):
        running = rhs[i]
        for j in range(i):
            running = running - factor[i][j] * forward[j]
        forward.append(running / factor[i][i])
    backward = [None] * order
    for i in reversed(range(order)):
        running = forward[i]
        for j in range(i + 1, order):
            running = running - factor[j][i] * backward[j]
        backward[i] = running / factor[i][i]
    return backward


def consensus_kernel(rhs_ref, arrived_ref, out_ref, *, copies):
    rhs = rhs_ref[0]
    for i in range(1, rhs_ref.shape[0]):
        rhs = rhs + rhs_ref[i]
    sums = jnp.sum(arrived_ref[...], axis=0, keepdims=True) * (1.0 / copies)
    lane = lax.broadcasted_iota(jnp.int32, (1, 128), 1)
    pick = lambda i: jnp.sum(jnp.where(lane == i, sums, 0.0), axis=1, keepdims=True)
    gram = [[pick(2 + i * (i + 1) // 2 + j) for j in range(i + 1)] for i in range(NPOLY)]
    solved = cholesky_solve(gram, [rhs[j : j + 1] for j in range(NPOLY)])
    out_ref[...] = jnp.broadcast_to(jnp.concatenate(solved, axis=0)[None], out_ref.shape)


def consensus_call(rhs, arrived, copies):
    return pl.pallas_call(
        functools.partial(consensus_kernel, copies=copies),
        in_specs=[ON_CHIP] * 2,
        out_specs=ON_CHIP,
        out_shape=jax.ShapeDtypeStruct(rhs.shape, F32),
        compiler_params=GRANT,
        cost_estimate=lasts(1),
        name="consensus",
    )(rhs, arrived)


def finish_kernel(solved_ref, gains_ref, dual_ref, ratio_ref, consensus_out, dual_out):
    channels = ratio_ref.shape[1]
    own = lax.broadcasted_iota(jnp.int32, (channels, channels), 0)
    own = own == lax.broadcasted_iota(jnp.int32, (channels, channels), 1)
    columns = [
        jnp.sum(
            jnp.where(own, jnp.broadcast_to(row, (channels, channels)), 0.0),
            axis=1,
            keepdims=True,
        )
        for row in legendre(ratio_ref[...])
    ]
    for k in range(DIRS):
        rows = [solved_ref[k, j : j + 1, :] for j in range(NPOLY)]
        for j in range(NPOLY):
            consensus_out[0, j, k : k + 1, :] = rows[j]
        fitted = sum(columns[j] * rows[j] for j in range(NPOLY))
        dual_out[0, k] = dual_ref[0, k] + gains_ref[0, k] - fitted


def finish_call(solved, gains, dual, ratio):
    channels = ratio.shape[0]
    big = pl.BlockSpec((1, DIRS, channels, STATIONS), lambda c: (c, 0, 0, 0))
    return pl.pallas_call(
        finish_kernel,
        grid=(2,),
        in_specs=[
            pl.BlockSpec((DIRS, NPOLY, STATIONS), lambda c: (c, 0, 0)),
            big,
            big,
            pl.BlockSpec((1, channels), lambda c: (0, 0)),
        ],
        out_specs=[pl.BlockSpec((1, NPOLY, DIRS, STATIONS), lambda c: (c, 0, 0, 0)), big],
        out_shape=[
            jax.ShapeDtypeStruct((2, NPOLY, DIRS, STATIONS), F32),
            jax.ShapeDtypeStruct(dual.shape, F32),
        ],
        cost_estimate=lasts(1),
        name="finish",
    )(solved, gains, dual, ratio.reshape(1, -1))


def own_channels(array, axis, own):
    return lax.dynamic_slice_in_dim(array, own * FEW, FEW, axis)


def pack_kernel(vis_ref, flag_ref, pair_ref, coord_ref, out_ref):
    def run(j, carry):
        lanes = pl.ds(pl.multiple_of(j * 128, 128), 128)
        to = pl.ds(j, 1)
        for c in range(2):
            for t in range(TIMES):
                rows = vis_ref[c, t, :, lanes]
                for f in range(PARTS * FEW):
                    out_ref[f // FEW, (2 * c + t) * FEW + f % FEW, to, :] = rows[f : f + 1]
                rows = coord_ref[c, t : t + 1, lanes]
                for d in range(PARTS):
                    out_ref[d, 12 + 2 * c + t, to, :] = rows
        for t in range(TIMES):
            rows = flag_ref[t, :, lanes].astype(F32)
            for f in range(PARTS * FEW):
                out_ref[f // FEW, 8 + t * FEW + f % FEW, to, :] = rows[f : f + 1]
        for side in range(2):
            rows = pair_ref[side : side + 1, lanes].astype(F32)
            for d in range(PARTS):
                out_ref[d, 16 + side, to, :] = rows
        return carry

    lax.fori_loop(0, out_ref.shape[2], run, 0)


def packed(vis, flags, pairs, coords):
    half = LOCAL // 2
    channels = vis.shape[2]
    return pl.pallas_call(
        pack_kernel,
        grid=(2,),
        in_specs=[
            pl.BlockSpec((2, TIMES, channels, half), lambda i: (0, 0, 0, i)),
            pl.BlockSpec((TIMES, channels, half), lambda i: (0, 0, i)),
            pl.BlockSpec((2, half), lambda i: (0, i)),
            pl.BlockSpec((2, TIMES, half), lambda i: (0, 0, i)),
        ],
        out_specs=pl.BlockSpec((PARTS, ROWS, half // 128, 128), lambda i: (0, 0, i, 0)),
        out_shape=jax.ShapeDtypeStruct((PARTS, ROWS, LOCAL // 128, 128), F32),
        cost_estimate=lasts(2),
        name="pack",
    )(vis, flags, pairs, coords)


def body(
    visibilities,
    sample_flag_weight,
    baseline_station_pair,
    baseline_spatial_coords,
    directions,
    source_flux,
    channel_ratio,
    jones_gains,
    scaled_dual,
    consensus,
    penalty,
):
    devices = lax.axis_size(ALL)
    own = lax.axis_index(BL)
    channels = channel_ratio.shape[0]
    rho = penalty * (2.0 * BASELINES * TIMES / STATIONS)

    wide = functools.partial(
        wide_model,
        vis=visibilities,
        flags=sample_flag_weight,
        pairs=baseline_station_pair,
        coords=baseline_spatial_coords,
        directions=directions,
        flux=source_flux,
        ratio=channel_ratio,
    )
    payload = wide(jones_gains.reshape(-1, STATIONS), residual_out=False, devices=devices)
    send = packed(
        visibilities, sample_flag_weight, baseline_station_pair, baseline_spatial_coords
    )
    send = send.reshape(PARTS, ROWS * LOCAL // 128, 128)
    data = lax.all_to_all(send, BL, 0, 0, tiled=True).reshape(PARTS, ROWS, LOCAL)

    ratio = own_channels(channel_ratio, 0, own)
    flux = own_channels(source_flux, 1, own)
    basis = legendre(ratio)
    def rows_of(array):
        part = own_channels(array, 2, own)
        return part.transpose(2, 0, 1, 3)

    dual = rows_of(scaled_dual)
    anchor = (
        sum(
            basis[j][:, None, None, None] * consensus[:, j][None] for j in range(NPOLY)
        )
        - dual
    ).reshape(GAIN_ROWS, STATIONS)
    gains = rows_of(jones_gains).reshape(GAIN_ROWS, STATIONS)
    geo = jnp.concatenate(
        [
            directions.T,
            flux,
            jnp.broadcast_to(ratio[None], (DIRS, FEW)),
            rho[:, None],
            jnp.zeros((DIRS, 1), F32),
        ],
        axis=1,
    )

    left, right, error, sky = first_call(data, gains, geo)
    all_basis = [jnp.stack(legendre(channel_ratio))]
    payload, error, anchor, *all_basis = lax.optimization_barrier(
        (payload, error, anchor, *all_basis)
    )
    arrived = lax.all_to_all(payload[:, None], ALL, 0, 0, tiled=True)[:, 0]
    squares = arrived
    for iteration in range(ITERS - 1):
        gains, left, right, error, misfit = middle_call(
            squares, arrived, data, (left, right, error, sky), gains, anchor, geo, devices
        )
        squares = lax.all_to_all(misfit[:, None], ALL, 0, 0, tiled=True)[:, 0]
    gains = last_call(squares, arrived, data, (left, right, error, sky), gains, anchor, geo)

    gains, *all_basis = lax.optimization_barrier((gains, *all_basis))
    gathered = lax.all_to_all(gains, BL, 0, 0, tiled=True)
    new_gains = (
        gathered.reshape(PARTS * FEW, 2, DIRS, STATIONS).transpose(1, 2, 0, 3)
    )
    new_gains = lax.optimization_barrier(new_gains)
    residuals = wide(new_gains.reshape(-1, STATIONS), residual_out=True)

    lifted = new_gains + scaled_dual
    wide_basis = all_basis[0][None, :, :, None]
    rhs = (wide_basis * lifted.reshape(-1, 1, *lifted.shape[2:])).sum(axis=2)
    rhs = lax.all_to_all(rhs, FREQ, 0, 0, tiled=True)
    rhs, residuals = lax.optimization_barrier((rhs, residuals))
    solved = consensus_call(rhs, arrived, lax.axis_size(BL))
    everyone = lax.all_to_all(solved, FREQ, 0, 0, tiled=True)
    new_consensus, new_dual = finish_call(everyone, new_gains, scaled_dual, channel_ratio)
    return (new_gains, new_consensus, new_dual, residuals)


def solution(mesh):
    split = Mesh(
        mesh.devices.reshape(4, 2, 4, 2, 2), ("bl_0", "bl_1", "freq_0", "freq_1", "freq_2")
    )
    in_specs = (
        P(None, None, FREQ, BL),
        P(None, FREQ, BL),
        P(None, BL),
        P(None, None, BL),
        P(),
        P(None, FREQ),
        P(FREQ),
        P(None, None, FREQ, None),
        P(None, None, FREQ, None),
        P(),
        P(),
    )
    out_specs = (P(None, None, FREQ, None), P(), P(None, None, FREQ, None), P(None, None, FREQ, BL))
    return jax.shard_map(body, mesh=split, in_specs=in_specs, out_specs=out_specs, check_vma=False)
```
